32 devices in a mesh: batch: 4 (over z), ctx: 4 (over x, core), tensor: 2 (over y).
Axes of the slice: x: 2, y: 2, z: 4, core: 2. Of those that a mesh axis runs over, the one named last changes fastest.
Arguments:
- tokens: bfloat16 [1032, 16, 1024], P(('ctx', 'tensor'), 'batch'), may hold values from -6 to 6
- positions: int32 [2, 1032, 16], P(None, 'ctx', 'batch'), may hold values from 0 to 31
- key_mask: int32 [1032, 16], P(None, 'batch'), may hold values from 0 to 1, as said below
- norm1_gain: float32 [1024], replicated, may hold values from 0.25 to 1.75
- norm1_bias: float32 [1024], replicated, may hold values from -3 to 3
- qkv_weight: float32 [1024, 3, 1024], P(('batch', 'ctx'), None, 'tensor'), may hold values from -0.1875 to 0.1875
- qv_bias: float32 [2, 1024], replicated, may hold values from -3 to 3
- out_weight: float32 [1024, 1024], P('tensor', ('batch', 'ctx')), may hold values from -3.5 to 3.5
- out_bias: float32 [1024], replicated, may hold values from -3 to 3
- norm2_gain: float32 [1024], replicated, may hold values from 0.25 to 1.75
- norm2_bias: float32 [1024], replicated, may hold values from -3 to 3
- gate_up_weight: float32 [1024, 2, 2730], P(('batch', 'ctx'), None, 'tensor'), may hold values from -0.1875 to 0.1875
- gate_up_bias: float32 [2, 2730], replicated, may hold values from -3 to 3
- inner_gain: float32 [2730], replicated, may hold values from 0.25 to 1.75
- inner_bias: float32 [2730], replicated, may hold values from -3 to 3
- down_weight: float32 [2730, 1024], P('tensor', ('batch', 'ctx')), may hold values from -0.109375 to 0.109375
- down_bias: float32 [1024], replicated, may hold values from -3 to 3
- cotangent: bfloat16 [1032, 16, 1024], P('ctx', 'batch'), may hold values from -6 to 6
Outputs:
- mixed: bfloat16 [1032, 16, 1024], P(('ctx', 'tensor'), 'batch')
- tokens_grad: bfloat16 [1032, 16, 1024], P(('ctx', 'tensor'), 'batch')
- norm1_gain_grad: float32 [1024], replicated
- norm1_bias_grad: float32 [1024], replicated
- qkv_weight_grad: float32 [1024, 3, 1024], P(('batch', 'ctx'), None, 'tensor')
- qv_bias_grad: float32 [2, 1024], replicated
- out_weight_grad: float32 [1024, 1024], P('tensor', ('batch', 'ctx'))
- out_bias_grad: float32 [1024], replicated
- norm2_gain_grad: float32 [1024], replicated
- norm2_bias_grad: float32 [1024], replicated
- gate_up_weight_grad: float32 [1024, 2, 2730], P(('batch', 'ctx'), None, 'tensor')
- gate_up_bias_grad: float32 [2, 2730], replicated
- inner_gain_grad: float32 [2730], replicated
- inner_bias_grad: float32 [2730], replicated
- down_weight_grad: float32 [2730, 1024], P('tensor', ('batch', 'ctx'))
- down_bias_grad: float32 [1024], replicated
The draws below stay inside these ranges and needn't reach their ends.
Inputs may be any that keep to these rules, and one draw needn't show every extreme that they name: `key_mask`: in each image the live tokens come first and the padded ones after; every image has at least one live token.
All inputs are finite; a program needn't handle non-finite values.
Results may differ from the reference program's by a relative error of at most 0.017.
Values may be sent and summed in bfloat16 or wider, within the bound.
A program may use at most 256 MiB of HBM per device.

```python
import math
import jax
import jax.numpy as jnp
from jax import lax

D = 1024
HEADS = 16
HEAD_DIM = 64
FF = 2730
SEQ = 1032
GRID = 32
IMAGES = 16


def draw_key_mask(key, part):
    live_length = jax.random.randint(key, (1, IMAGES), SEQ // 2, SEQ - 6)
    return (jnp.arange(SEQ)[:, None] < live_length).astype(jnp.int32)


def place_ends(array, stream_key, low, largest):
    extent = array.shape
    index_at = [jax.random.randint(jax.random.fold_in(stream_key, axis), (), 0, extent[axis]) for axis in range(len(extent))]
    array = array.at[tuple(index_at)].set(low)
    longest = extent.index(max(extent))
    index_at[longest] = (index_at[longest] + 1) % extent[longest]
    return array.at[tuple(index_at)].set(largest)


def raised(array, own_key, source, target, shards_of, factor):
    owner, partner = [(jnp.arange(array.shape[axis_at]) // (array.shape[axis_at] // shards_of)).reshape([-1 if axis == axis_at else 1 for axis in range(array.ndim)]) for axis_at in (source, target)]
    chosen = jax.random.permutation(own_key, shards_of)[partner]
    strong = (owner == chosen) | (owner == (partner + shards_of // 2) % shards_of)
    return jnp.where(strong, factor * array, array)


def shard_levels(stream_key, extent, shards, smallest, largest):
    level, own = 1.0, jax.random.fold_in(stream_key, 6)
    for dim, shards_of in shards:
        heights = jnp.exp(jax.random.uniform(jax.random.fold_in(own, dim), (shards_of,), jnp.float32, smallest / len(shards), largest / len(shards)))
        level = level * jnp.repeat(heights, extent[dim] // shards_of).reshape([-1 if axis == dim else 1 for axis in range(len(extent))])
    return level


def scatter_about(own_key, shape, deviation, limit, cuts=(), dtype=jnp.bfloat16):
    entries = jax.random.normal(own_key, shape, jnp.float32) * deviation
    if len(cuts) > 0:
        entries = shard_levels(own_key, shape, cuts, -0.22, 0.18) * entries
    return jnp.clip(entries, min=-limit, max=limit).astype(dtype)


def gaussian_with(rng, extent, scale, bound, shards, heavy, kind=jnp.bfloat16):
    entries = scale * jax.random.normal(rng, extent, jnp.float32)
    if shards:
        entries = entries * shard_levels(rng, extent, shards, -0.22, 0.18)
    return jnp.clip(raised(entries, jax.random.fold_in(rng, 3), *heavy), -bound, bound).astype(kind)


def setup_inputs(seed: int = 0) -> dict:
    seeds = jax.random.split(jax.random.key(seed), 19)
    return {
        "tokens": scatter_about(seeds[0], (SEQ, IMAGES, D), 1.0, 6.0, ((0, 8), (1, 4))),
        "positions": place_ends(jax.random.randint(seeds[1], (2, SEQ, IMAGES), 0, GRID), jax.random.fold_in(seeds[1], 1), 0, GRID - 1).astype(jnp.int32),
        "key_mask": draw_key_mask(jax.random.fold_in(seeds[18], 71), 0),
        "norm1_gain": jnp.clip(1.0 + 0.15 * jax.random.normal(seeds[3], (D,), jnp.float32), 0.25, 1.75),
        "norm1_bias": scatter_about(seeds[4], (D,), 0.3, 3.0, (), jnp.float32),
        "qkv_weight": scatter_about(seeds[5], (D, 3, D), D ** -0.5, 0.1875, ((0, 16), (2, 2)), jnp.float32),
        "qv_bias": scatter_about(seeds[6], (2, D), 0.5, 3.0, (), jnp.float32),
        "out_weight": scatter_about(seeds[7], (D, D), (max(D * 4 // SEQ, 1)) ** -0.5, 3.5, ((0, 2), (1, 16)), jnp.float32),
        "out_bias": scatter_about(seeds[8], (D,), 0.3, 3.0, (), jnp.float32),
        "norm2_gain": jnp.clip(1.0 + 0.15 * jax.random.normal(seeds[9], (D,), jnp.float32), 0.25, 1.75),
        "norm2_bias": scatter_about(seeds[10], (D,), 0.3, 3.0, (), jnp.float32),
        "gate_up_weight": scatter_about(seeds[11], (D, 2, FF), D ** -0.5, 0.1875, ((0, 16), (2, 2)), jnp.float32),
        "gate_up_bias": scatter_about(seeds[12], (2, FF), 0.5, 3.0, (), jnp.float32),
        "inner_gain": jnp.clip(1.0 + 0.15 * jax.random.normal(seeds[13], (FF,), jnp.float32), 0.25, 1.75),
        "inner_bias": scatter_about(seeds[14], (FF,), 0.3, 3.0, (), jnp.float32),
        "down_weight": scatter_about(seeds[15], (FF, D), FF ** -0.5, 0.109375, ((0, 2), (1, 16)), jnp.float32),
        "down_bias": scatter_about(seeds[16], (D,), 0.3, 3.0, (), jnp.float32),
        "cotangent": gaussian_with(seeds[17], (SEQ, IMAGES, D), 1.0, 6.0, ((0, 4), (1, 4)), (1, 2, 4, 2.0)),
    }


@jax.custom_vjp
def low(v):
    return lax.optimization_barrier(v.astype(jnp.bfloat16)).astype(jnp.float32)

@jax.custom_vjp
def low_back(v):
    return v

def low_keep(v):
    return (low(v), None)

def low_pass(kept, grad):
    return (grad,)

def back_keep(v):
    return (v, None)

def back_low(kept, grad):
    return (low(grad),)
low.defvjp(low_keep, low_pass)
low_back.defvjp(back_keep, back_low)
highest = lax.Precision.HIGHEST
epsilon = 1e-06
masked_score = -1e+30

def layer_norm(values, gain, shift):
    centre = lax.optimization_barrier(jnp.mean(values, axis=-1, keepdims=True))
    spread = lax.optimization_barrier(jnp.mean(jnp.square(values - centre), axis=-1, keepdims=True))
    return (values - centre) * lax.rsqrt(spread + epsilon) * gain + shift

def rotary_tables(grid):
    quarter = HEAD_DIM // 4
    freqs = 10000.0 ** (-jnp.arange(quarter).astype(jnp.float32) / quarter)
    angles = grid.astype(jnp.float32)[..., None] * freqs
    angles = jnp.moveaxis(angles, 0, 2)[:, :, None]
    return (jnp.cos(angles), jnp.sin(angles))

def rotate_heads(values, cosine, sine):
    quarter = HEAD_DIM // 4
    shaped = values.reshape(values.shape[:-1] + (values.shape[-1] // HEAD_DIM, 2, 2, quarter))
    first = shaped[..., 0, :]
    second = shaped[..., 1, :]
    turned = jnp.stack([first * cosine - second * sine, second * cosine + first * sine], axis=-2)
    return turned.reshape(values.shape)

def attend_image(inputs_image):
    query, keys, values, live = inputs_image
    query_heads = query.reshape(SEQ, HEADS, HEAD_DIM)
    key_heads = keys.reshape(SEQ, HEADS, HEAD_DIM)
    value_heads = values.reshape(SEQ, HEADS, HEAD_DIM)
    scores = jnp.einsum('qhe,khe->hqk', query_heads, key_heads, precision=highest) * HEAD_DIM ** (-0.5)
    scores = low_back(scores)
    scores = jnp.where(live[None, None, :] > 0, scores, masked_score)
    probs = jax.nn.softmax(scores, axis=-1)
    attended = jnp.einsum('hqk,khe->qhe', low(probs), value_heads, precision=highest)
    return low_back(low(attended.reshape(SEQ, HEADS * HEAD_DIM)))

def block(inputs_f, weights, cosine, sine, live):
    norm1_gain, norm1_bias, qkv_weight, qv_bias, out_weight, out_bias, norm2_gain, norm2_bias, gate_up_weight, gate_up_bias, inner_gain, inner_bias, down_weight, down_bias = weights
    first_normed = low(layer_norm(inputs_f, norm1_gain, norm1_bias))
    projected = jnp.einsum('sid,dtf->sitf', first_normed, low(qkv_weight), precision=highest)
    bias_rows = jnp.stack([qv_bias[0], jnp.zeros_like(qv_bias[0]), qv_bias[1]])
    projected = low_back(projected + bias_rows)
    query = low(rotate_heads(projected[:, :, 0], cosine, sine))
    keys = low(rotate_heads(projected[:, :, 1], cosine, sine))
    values = low(projected[:, :, 2])
    attended = lax.map(jax.checkpoint(attend_image), (jnp.moveaxis(query, 1, 0), jnp.moveaxis(keys, 1, 0), jnp.moveaxis(values, 1, 0), jnp.moveaxis(live, 1, 0)))
    attended = jnp.moveaxis(attended, 0, 1)
    attn_branch = low_back(jnp.einsum('sie,ed->sid', attended, low(out_weight), precision=highest) + out_bias)
    resid = inputs_f + attn_branch
    second_normed = low(layer_norm(resid, norm2_gain, norm2_bias))
    gate_up = jnp.einsum('sid,dtf->sitf', second_normed, low(gate_up_weight), precision=highest)
    gate_up = low_back(gate_up + gate_up_bias)
    activated = jax.nn.silu(gate_up[:, :, 0]) * gate_up[:, :, 1]
    inner = low(layer_norm(activated, inner_gain, inner_bias))
    ffn_branch = low_back(jnp.einsum('sif,fd->sid', inner, low(down_weight), precision=highest) + down_bias)
    return resid + ffn_branch

def reference(tokens, positions, key_mask, norm1_gain, norm1_bias, qkv_weight, qv_bias, out_weight, out_bias, norm2_gain, norm2_bias, gate_up_weight, gate_up_bias, inner_gain, inner_bias, down_weight, down_bias, cotangent):
    group = math.gcd(IMAGES, 4)
    count = IMAGES // group
    params = (norm1_gain, norm1_bias, qkv_weight, qv_bias, out_weight, out_bias, norm2_gain, norm2_bias, gate_up_weight, gate_up_bias, inner_gain, inner_bias, down_weight, down_bias)
    inputs_all = jnp.moveaxis(tokens.astype(jnp.float32).reshape(SEQ, count, group, D), 1, 0)
    grads_all = jnp.moveaxis(cotangent.astype(jnp.float32).reshape(SEQ, count, group, D), 1, 0)
    grids_all = jnp.moveaxis(positions.reshape(2, SEQ, count, group), 2, 0)
    lives_all = jnp.moveaxis(key_mask.reshape(SEQ, count, group), 1, 0)

    def one_group(totals, items):
        inputs_g, grid_g, live_g, upstream_g = items
        cosine, sine = rotary_tables(grid_g)

        def forward(inputs_f, weights):
            return block(inputs_f, weights, cosine, sine, live_g)
        output_g, pull_back = jax.vjp(forward, inputs_g, params)
        input_grad, weight_grads = pull_back(upstream_g)
        totals = jax.tree.map(lambda total, extra: total + extra, totals, weight_grads)
        return (totals, (output_g.astype(jnp.bfloat16), input_grad.astype(jnp.bfloat16)))
    zeros_init = jax.tree.map(jnp.zeros_like, params)
    totals, outputs = lax.scan(one_group, zeros_init, (inputs_all, grids_all, lives_all, grads_all))
    mixed = jnp.moveaxis(outputs[0], 0, 1).reshape(SEQ, IMAGES, D)
    tokens_grad = jnp.moveaxis(outputs[1], 0, 1).reshape(SEQ, IMAGES, D)
    return (mixed, tokens_grad, totals[0], totals[1], totals[2], totals[3], totals[4], totals[5], totals[6], totals[7], totals[8], totals[9], totals[10], totals[11], totals[12], totals[13])
```

```python
import functools

import jax
import jax.numpy as jnp
from jax import lax
from jax.experimental import pallas as pl
from jax.experimental.pallas import tpu as pltpu

from jax.sharding import PartitionSpec as P
MESH = pl.DeviceIdType.MESH
FAR = ("batch", "x", "core", "tensor")


def place(b, x, c, y):
    return {"batch": b, "x": x, "core": c, "tensor": y}


def ring_offsets(count):
    order = [0]
    for step in range(1, count // 2 + 1):
        for off in (step, count - step):
            if off not in order:
                order.append(off)
    return order


def greet(count, corner=False):
    b, x, c, y = (lax.axis_index(a) for a in FAR)
    barrier = pltpu.get_barrier_semaphore()
    for off in range(1, count):
        pl.semaphore_signal(
            barrier, inc=1, device_id=place(lax.rem(b + off, count), x, c, y), device_id_type=MESH
        )
    near = [place(b, 1 - x, c, y), place(b, x, c, 1 - y), place(b, x, 1 - c, y)]
    if corner:
        near.append(place(b, 1 - x, c, 1 - y))
    for there in near:
        pl.semaphore_signal(barrier, inc=1, device_id=there, device_id_type=MESH)
    pl.semaphore_wait(barrier, count - 1 + len(near))


def gather_kernel(count, groups, *refs):
    own = refs[:groups]
    moved = refs[groups : groups + 3]
    full = refs[groups + 3 : 2 * groups + 3]
    landed = refs[2 * groups + 3 : 2 * groups + 6]
    zs, zr, xs, xr, ys, yr, xds, yds, dr, cs, cr, ls, ts, tr = refs[2 * groups + 6 :]
    b, x, c, y = (lax.axis_index(a) for a in FAR)
    xn, yn, cn = place(b, 1 - x, c, y), place(b, x, c, 1 - y), place(b, x, 1 - c, y)
    offsets = ring_offsets(count)
    tokens, spots, cot = moved
    greet(count, corner=True)

    def send(src, dst, s, r, there):
        pltpu.make_async_remote_copy(
            src_ref=src, dst_ref=dst, send_sem=s, recv_sem=r, device_id=there, device_id_type=MESH
        ).start()

    def arrived(dst, sem):
        pltpu.make_async_copy(dst, dst, sem).wait()

    mine = 2 * x + y
    for n, (ox, oy) in enumerate(((1, 0), (0, 1), (1, 1))):
        px = 1 - x if ox else x
        py = 1 - y if oy else y
        send(
            tokens.at[2 * px + py], landed[0].at[mine], ts.at[n], tr.at[n], place(b, px, c, py)
        )
    far = 2 * (1 - x) + y
    send(spots.at[far], landed[1].at[x], ts.at[3], tr.at[3], xn)

    def block(g, yy, item, xx, cc):
        bb = lax.rem(b + offsets[item], count)
        return full[g].at[yy, bb, xx, cc]

    def shard(g, item):
        return own[g] if item == 0 else block(g, y, item, x, c)

    items = [(g, j) for g in range(groups) for j in range(count)]
    for g in range(groups):
        home = full[g].at[y, b, x, c]
        for j in range(1, count):
            there = place(lax.rem(b + count - offsets[j], count), x, c, y)
            send(own[g], home, zs.at[g], zr.at[g, j], there)
        if g == 0:
            send(cot.at[far], landed[2].at[x], ts.at[4], tr.at[4], xn)

    def stage_column(g, j):
        if j > 0:
            arrived(block(g, y, j, x, c), zr.at[g, j])
        src, dst = shard(g, j), block(g, y, j, x, c)
        send(src, dst, xs.at[g], xr.at[g, j], xn)
        send(src, dst, ys.at[g], yr.at[g, j], yn)
        send(src, dst, cs.at[g], cr.at[g], cn)

    def stage_plane(g, j):
        from_x, from_y = block(g, y, j, 1 - x, c), block(g, 1 - y, j, x, c)
        arrived(from_x, xr.at[g, j])
        if j % 2 == 0:
            send(from_x, from_x, yds.at[g], dr.at[g, j], yn)
        send(from_x, from_x, cs.at[g], cr.at[g], cn)
        arrived(from_y, yr.at[g, j])
        if j % 2 == 1:
            send(from_y, from_y, xds.at[g], dr.at[g, j], xn)
        send(from_y, from_y, cs.at[g], cr.at[g], cn)

    def stage_corner(g, j):
        corner = block(g, 1 - y, j, 1 - x, c)
        arrived(corner, dr.at[g, j])
        send(corner, corner, cs.at[g], cr.at[g], cn)

    homes = []
    for g in range(groups):
        copy = pltpu.make_async_copy(own[g], full[g].at[y, b, x, c], ls.at[g])
        copy.start()
        homes.append(copy)
    for t in range(len(items) + 2):
        if t < len(items):
            stage_column(*items[t])
        if 1 <= t <= len(items):
            stage_plane(*items[t - 1])
        if t >= 2:
            stage_corner(*items[t - 2])
    for copy in homes:
        copy.wait()
    for n, (ox, oy) in enumerate(((1, 0), (0, 1), (1, 1))):
        px = 1 - x if ox else x
        py = 1 - y if oy else y
        arrived(landed[0].at[2 * px + py], tr.at[n])
        arrived(tokens.at[0], ts.at[n])
    arrived(landed[1].at[1 - x], tr.at[3])
    arrived(spots.at[0], ts.at[3])
    arrived(landed[2].at[1 - x], tr.at[4])
    arrived(cot.at[0], ts.at[4])
    for g in range(groups):
        arrived(full[g].at[:, :, :, 1 - c], cr.at[g])
        arrived(full[g].at[:, :, :, 0], cs.at[g])
        arrived(full[g].at[0, : count - 1, 0, 0], zs.at[g])
        arrived(full[g].at[0, :, 0, 0], xs.at[g])
        arrived(full[g].at[0, :, 0, 0], ys.at[g])
        arrived(full[g].at[0, : count // 2, 0, 0], xds.at[g])
        arrived(full[g].at[0, : (count + 1) // 2, 0, 0], yds.at[g])


def gather_all(count, shards, tokens, spots, cot):
    groups = len(shards)
    any_spec = pl.BlockSpec(memory_space=pl.ANY)
    dma = pltpu.SemaphoreType.DMA
    outs = [jax.ShapeDtypeStruct((2, count, 2, 2) + s.shape, s.dtype) for s in shards]
    outs += [
        jax.ShapeDtypeStruct(tokens.shape, tokens.dtype),
        jax.ShapeDtypeStruct((2,) + spots.shape[1:], spots.dtype),
        jax.ShapeDtypeStruct((2,) + cot.shape[1:], cot.dtype),
    ]
    return pl.pallas_call(
        functools.partial(gather_kernel, count, groups),
        out_shape=outs,
        in_specs=[any_spec] * (groups + 3),
        out_specs=[any_spec] * len(outs),
        scratch_shapes=[
            dma((groups,)), dma((groups, count)), dma((groups,)), dma((groups, count)),
            dma((groups,)), dma((groups, count)), dma((groups,)), dma((groups,)),
            dma((groups, count)), dma((groups,)), dma((groups,)), dma((groups,)),
            dma((5,)), dma((5,)),
        ],
        compiler_params=pltpu.CompilerParams(collective_id=0, has_side_effects=True),
        name="gather_all",
    )(*shards, tokens, spots, cot)
def scatter_kernel(count, groups, *refs):
    parts = refs[:groups]
    outs = refs[groups : 2 * groups]
    at = 2 * groups
    held, peer, from_x, from_y, from_d, from_z = (
        refs[at + k * groups : at + (k + 1) * groups] for k in range(6)
    )
    ls, cs, cr, xs, xr, ys, yr, xds, yds, dr, zs, zr = refs[at + 6 * groups :]
    b, x, c, y = (lax.axis_index(a) for a in FAR)
    xn, yn, cn = place(b, 1 - x, c, y), place(b, x, c, 1 - y), place(b, x, 1 - c, y)
    offsets = ring_offsets(count)
    order = list(range(1, count)) + [0]
    rows = held[0].shape[3]
    chunk = min(rows, 16)
    greet(count)

    def send(src, dst, s, r, there):
        pltpu.make_async_remote_copy(
            src_ref=src, dst_ref=dst, send_sem=s, recv_sem=r, device_id=there, device_id_type=MESH
        ).start()

    def arrived(dst, sem):
        pltpu.make_async_copy(dst, dst, sem).wait()

    def add_to(target, *others):
        def body(i, carry):
            at_rows = pl.ds(pl.multiple_of(i * chunk, chunk), chunk)
            total = target[at_rows].astype(jnp.float32)
            for other in others:
                total = total + other[at_rows].astype(jnp.float32)
            target[at_rows] = total.astype(target.dtype)
            return carry

        lax.fori_loop(0, rows // chunk, body, 0)

    def where_to(j):
        return lax.rem(b + offsets[j], count)

    items = [(g, j) for g in range(groups) for j in order]
    for g, j in items:
        bb = where_to(j)
        send(parts[g].at[:, bb, :, 1 - c], peer[g].at[:, bb], cs.at[g], cr.at[g, j], cn)
        pltpu.make_async_copy(parts[g].at[:, bb, :, c], held[g].at[:, bb], ls.at[g, j]).start()

    def merge_core(g, j):
        bb = where_to(j)
        arrived(held[g].at[:, bb], ls.at[g, j])
        arrived(peer[g].at[:, bb], cr.at[g, j])
        for yy, xx in ((1 - y, 1 - x), (y, 1 - x), (1 - y, x), (y, x)):
            add_to(held[g].at[yy, bb, xx], peer[g].at[yy, bb, xx])

    def send_corner(g, j):
        src = held[g].at[1 - y, where_to(j), 1 - x]
        if j % 2 == 0:
            send(src, from_d[g].at[j], xds.at[g], dr.at[g, j], xn)
        else:
            send(src, from_d[g].at[j], yds.at[g], dr.at[g, j], yn)

    def merge_corner(g, j):
        bb = where_to(j)
        arrived(from_d[g].at[j], dr.at[g, j])
        if j % 2 == 0:
            add_to(held[g].at[1 - y, bb, x], from_d[g].at[j])
        else:
            add_to(held[g].at[y, bb, 1 - x], from_d[g].at[j])

    def send_plane(g, j):
        bb = where_to(j)
        send(held[g].at[y, bb, 1 - x], from_x[g].at[j], xs.at[g], xr.at[g, j], xn)
        send(held[g].at[1 - y, bb, x], from_y[g].at[j], ys.at[g], yr.at[g, j], yn)

    def merge_plane(g, j):
        arrived(from_x[g].at[j], xr.at[g, j])
        arrived(from_y[g].at[j], yr.at[g, j])
        add_to(held[g].at[y, where_to(j), x], from_x[g].at[j], from_y[g].at[j])

    def send_column(g, j):
        if j > 0:
            bb = where_to(j)
            send(
                held[g].at[y, bb, x], from_z[g].at[j], zs.at[g], zr.at[g, j], place(bb, x, c, y)
            )

    total = len(items)
    for t in range(total + 2):
        now = items[t] if t < total else None
        one = items[t - 1] if 1 <= t <= total else None
        two = items[t - 2] if 2 <= t else None
        if two:
            merge_plane(*two)
        if one:
            merge_corner(*one)
        if now:
            merge_core(*now)
            send_corner(*now)
        if one:
            send_plane(*one)
        if two:
            send_column(*two)
    for g in range(groups):
        for j in range(1, count):
            arrived(from_z[g].at[j], zr.at[g, j])

        def body(i, carry, g=g):
            at_rows = pl.ds(pl.multiple_of(i * chunk, chunk), chunk)
            result = held[g][y, b, x, at_rows].astype(jnp.float32)
            for j in range(1, count):
                result = result + from_z[g][j, at_rows].astype(jnp.float32)
            outs[g][at_rows] = result
            return carry

        lax.fori_loop(0, rows // chunk, body, 0)
        arrived(peer[g], cs.at[g])
        arrived(from_x[g], xs.at[g])
        arrived(from_y[g], ys.at[g])
        arrived(from_d[g].at[: (count + 1) // 2], xds.at[g])
        arrived(from_d[g].at[: count // 2], yds.at[g])
        arrived(from_z[g].at[1:], zs.at[g])


def scatter_all(count, parts, number):
    groups = len(parts)
    dma = pltpu.SemaphoreType.DMA
    shapes = [p.shape[4:] for p in parts]
    low = jnp.bfloat16
    scratch = [pltpu.VMEM((2, count, 2) + s, low) for s in shapes] * 2
    scratch += [pltpu.VMEM((count,) + s, low) for s in shapes] * 4
    many, one = dma((groups, count)), dma((groups,))
    scratch += [many, one, many, one, many, one, many, one, one, many, one, many]
    return pl.pallas_call(
        functools.partial(scatter_kernel, count, groups),
        out_shape=[jax.ShapeDtypeStruct(s, jnp.float32) for s in shapes],
        in_specs=[pl.BlockSpec(memory_space=pl.ANY)] * groups,
        out_specs=[pl.BlockSpec(memory_space=pltpu.VMEM)] * groups,
        scratch_shapes=scratch,
        compiler_params=pltpu.CompilerParams(
            collective_id=number, has_side_effects=True, vmem_limit_bytes=64000000
        ),
        name="scatter_all",
    )(*parts)


def sum_kernel(count, v_ref, o_ref, got, lane, plane, slots, ss, rs, zs, zr):
    b, x, c, y = (lax.axis_index(a) for a in FAR)
    xn, yn, cn = place(b, 1 - x, c, y), place(b, x, c, 1 - y), place(b, x, 1 - c, y)
    half = v_ref.shape[0] // 2
    mine = pl.ds(pl.multiple_of(c * half, 8), half)
    theirs = pl.ds(pl.multiple_of((1 - c) * half, 8), half)
    greet(count)

    def swap(src, dst, n, there):
        copy = pltpu.make_async_remote_copy(
            src_ref=src, dst_ref=dst, send_sem=ss.at[n], recv_sem=rs.at[n], device_id=there,
            device_id_type=MESH,
        )
        copy.start()
        copy.wait()

    swap(v_ref.at[theirs], got.at[0], 0, cn)
    lane[...] = v_ref[mine] + got[0]
    swap(lane, got.at[1], 1, xn)
    plane[...] = lane[...] + got[1]
    swap(plane, got.at[2], 2, yn)
    slots[b] = plane[...] + got[2]
    for off in range(1, count):
        pltpu.make_async_remote_copy(
            src_ref=slots.at[b], dst_ref=slots.at[b], send_sem=zs, recv_sem=zr.at[off],
            device_id=place(lax.rem(b + off, count), x, c, y), device_id_type=MESH,
        ).start()
    for off in range(1, count):
        there = slots.at[lax.rem(b + count - off, count)]
        pltpu.make_async_copy(there, there, zr.at[off]).wait()
    total = slots[0]
    for n in range(1, count):
        total = total + slots[n]
    o_ref[mine] = total
    swap(o_ref.at[mine], o_ref.at[mine], 3, cn)
    rest = slots.at[: count - 1]
    pltpu.make_async_copy(rest, rest, zs).wait()


def sum_all(count, vector, number):
    rows = vector.shape[0]
    half = (rows // 2, 128)
    dma = pltpu.SemaphoreType.DMA
    vm = pltpu.VMEM
    return pl.pallas_call(
        functools.partial(sum_kernel, count),
        out_shape=jax.ShapeDtypeStruct(vector.shape, jnp.float32),
        in_specs=[pl.BlockSpec(memory_space=pltpu.VMEM)],
        out_specs=pl.BlockSpec(memory_space=pltpu.VMEM),
        scratch_shapes=[
            vm((3,) + half, jnp.float32), vm(half, jnp.float32), vm(half, jnp.float32),
            vm((count,) + half, jnp.float32), dma((4,)), dma((4,)), dma(()), dma((count,)),
        ],
        compiler_params=pltpu.CompilerParams(collective_id=number, has_side_effects=True),
        name="sum_all",
    )(vector)

PAD = 136
WIDTH_TILE = 128
HEAD_DIM = 64
epsilon = 1e-06
masked_score = -1e30
f32, low = jnp.float32, jnp.bfloat16
VMEM_LIMIT = 60000000


def mm(a, b, dims):
    return lax.dot_general(a, b, (dims, ((), ())), preferred_element_type=f32)


NN = ((1,), (0,))
NT = ((1,), (1,))
TN = ((0,), (0,))


def normalise(values, width):
    centre = jnp.sum(values, axis=-1, keepdims=True) / width
    shifted = values - centre
    spread = jnp.sum(jnp.square(shifted), axis=-1, keepdims=True) / width
    inverse = lax.rsqrt(spread + epsilon)
    return shifted * inverse, inverse


def turn(values, cosine, sine):
    lane = lax.broadcasted_iota(jnp.int32, values.shape, 1)
    other = jnp.where((lane // 16) % 2 == 0, pltpu.roll(values, 112, 1), pltpu.roll(values, 16, 1))
    return values * cosine + other * sine


def tables(spots, freqs):
    angles = spots.astype(f32) * freqs
    lane = lax.broadcasted_iota(jnp.int32, angles.shape, 1)
    sine = jnp.sin(angles)
    return jnp.cos(angles), jnp.where((lane // 16) % 2 == 0, -sine, sine)


def project_kernel(tok, gain, shift, w, bias, spots, freqs, out, h_out, hid, cos, sin):
    y, t = pl.program_id(0), pl.program_id(1)

    @pl.when((y == 0) & (t == 0))
    def _():
        normed, _ = normalise(tok[...].astype(f32), tok.shape[1])
        hid[...] = (normed * gain[...] + shift[...]).astype(low)
        h_out[...] = hid[...]
        cosine, sine = tables(spots[...], freqs[...])
        cos[...] = cosine
        sin[...] = sine

    acc = mm(hid[...], w[0], NN) + bias[0]

    @pl.when(t < 2)
    def _():
        for n in range(acc.shape[1] // 128):
            part = acc[:, n * 128 : (n + 1) * 128]
            out[0, :, n * 128 : (n + 1) * 128] = turn(part, cos[...], sin[...]).astype(low)

    @pl.when(t == 2)
    def _():
        out[0] = acc.astype(low)


def project(tok, gain, shift, w, bias, spots, freqs):
    rows, width = tok.shape
    half = w.shape[2] // 3
    whole = lambda *s: pl.BlockSpec(s, lambda y, t: (0,) * len(s))
    return pl.pallas_call(
        project_kernel,
        grid=(2, 3),
        out_shape=(
            jax.ShapeDtypeStruct((3, rows, width), low),
            jax.ShapeDtypeStruct((rows, width), low),
        ),
        in_specs=[
            whole(rows, width), whole(1, width), whole(1, width),
            pl.BlockSpec((1, width, half), lambda y, t: (y, 0, t)),
            pl.BlockSpec((1, 1, half), lambda y, t: (t, 0, y)),
            whole(rows, 128), whole(1, 128),
        ],
        out_specs=(
            pl.BlockSpec((1, rows, half), lambda y, t: (t, 0, y)), whole(rows, width),
        ),
        scratch_shapes=[
            pltpu.VMEM((rows, width), low), pltpu.VMEM((rows, 128), f32),
            pltpu.VMEM((rows, 128), f32),
        ],
        compiler_params=pltpu.CompilerParams(vmem_limit_bytes=VMEM_LIMIT),
        cost_estimate=pl.CostEstimate(
            flops=2 * rows * width * width * 3, bytes_accessed=14000000, transcendentals=0
        ),
        name="project",
    )(tok, gain, shift, w, bias, spots, freqs)


def head_lanes(rows):
    return lax.broadcasted_iota(jnp.int32, (rows, 128), 1) // HEAD_DIM


def attend_kernel(q, k, v, kp, vp, bias, out, lse, keys, vals, *, chunk):
    pair = pl.program_id(0)
    rows = q.shape[1]
    keys[:rows], keys[rows:] = k[0], kp[0]
    vals[:rows], vals[rows:] = v[0], vp[0]
    lanes = head_lanes(chunk)
    spot = lax.broadcasted_iota(jnp.int32, (chunk, 128), 1)
    for n in range(rows // chunk):
        here = slice(n * chunk, (n + 1) * chunk)
        query = q[0, here] * low(HEAD_DIM**-0.5)
        result = None
        kept = lse[here]
        for h in range(2):
            mine = jnp.where(lanes == h, query, low(0))
            scores = mm(mine, keys[...], NT) + bias[...]
            top = jnp.max(scores, axis=-1, keepdims=True)
            weight = jnp.exp(scores - top)
            total = jnp.sum(weight, axis=-1, keepdims=True)
            probs = (weight * (1.0 / total)).astype(low)
            got = mm(probs, vals[...], NN)
            result = got if h == 0 else jnp.where(lanes == 0, result, got)
            kept = jnp.where(spot == 2 * pair + h, top + jnp.log(total), kept)
        lse[here] = kept
        out[here] = result.astype(low)


def attend(qkv, far, bias):
    _, rows, width = qkv.shape
    keys = 2 * rows
    at = lambda t: pl.BlockSpec((1, rows, 128), lambda g: (t, 0, g))
    return pl.pallas_call(
        functools.partial(attend_kernel, chunk=rows // 2),
        grid=(width // 128,),
        out_shape=(
            jax.ShapeDtypeStruct((rows, width), low), jax.ShapeDtypeStruct((rows, 128), f32),
        ),
        in_specs=[at(0), at(1), at(2), at(0), at(1), pl.BlockSpec((1, keys), lambda g: (0, 0))],
        out_specs=(
            pl.BlockSpec((rows, 128), lambda g: (0, g)),
            pl.BlockSpec((rows, 128), lambda g: (0, 0)),
        ),
        scratch_shapes=[pltpu.VMEM((keys, 128), low)] * 2,
        compiler_params=pltpu.CompilerParams(vmem_limit_bytes=VMEM_LIMIT),
        cost_estimate=pl.CostEstimate(
            flops=16 * rows * keys * width, bytes_accessed=10000000, transcendentals=0
        ),
        name="attend",
    )(qkv, qkv, qkv, far, far, bias)


def unattend_kernel(q, k, v, kp, vp, bias, lse, grad, dq, dkv, dfar, keys, vals, dk, dv, *, chunk):
    pair = pl.program_id(0)
    rows = q.shape[1]
    keys[:rows], keys[rows:] = k[0], kp[0]
    vals[:rows], vals[rows:] = v[0], vp[0]
    lanes = head_lanes(chunk)
    spot = lax.broadcasted_iota(jnp.int32, (chunk, 128), 1)
    for n in range(rows // chunk):
        here = slice(n * chunk, (n + 1) * chunk)
        query = q[0, here] * low(HEAD_DIM**-0.5)
        out_grad = grad[here]
        result = None
        for h in range(2):
            mine = jnp.where(lanes == h, query, low(0))
            mine_grad = jnp.where(lanes == h, out_grad, low(0))
            shift = jnp.sum(jnp.where(spot == 2 * pair + h, lse[here], 0.0), axis=-1, keepdims=True)
            probs = jnp.exp(mm(mine, keys[...], NT) + bias[...] - shift)
            d_probs = mm(mine_grad, vals[...], NT)
            both = probs * d_probs
            inner = jnp.sum(both, axis=-1, keepdims=True)
            d_scores = (both - probs * inner).astype(low)
            got = mm(d_scores, keys[...], NN)
            result = got if h == 0 else jnp.where(lanes == 0, result, got)
            key_part = mm(d_scores, mine, TN)
            value_part = mm(probs.astype(low), mine_grad, TN)
            if n == 0 and h == 0:
                dk[...], dv[...] = key_part, value_part
            else:
                dk[...] += key_part
                dv[...] += value_part
        dq[here] = result * HEAD_DIM**-0.5
    dkv[0], dkv[1] = dk[:rows], dv[:rows]
    dfar[0], dfar[1] = dk[rows:].astype(low), dv[rows:].astype(low)


def unattend(qkv, far, bias, lse, grad):
    _, rows, width = qkv.shape
    keys = 2 * rows
    at = lambda t: pl.BlockSpec((1, rows, 128), lambda g: (t, 0, g))
    both = pl.BlockSpec((2, rows, 128), lambda g: (0, 0, g))
    column = pl.BlockSpec((rows, 128), lambda g: (0, g))
    return pl.pallas_call(
        functools.partial(unattend_kernel, chunk=rows // 2),
        grid=(width // 128,),
        out_shape=(
            jax.ShapeDtypeStruct((rows, width), f32),
            jax.ShapeDtypeStruct((2, rows, width), f32),
            jax.ShapeDtypeStruct((2, rows, width), low),
        ),
        in_specs=[
            at(0), at(1), at(2), at(0), at(1), pl.BlockSpec((1, keys), lambda g: (0, 0)),
            pl.BlockSpec((rows, 128), lambda g: (0, 0)), column,
        ],
        out_specs=(column, both, both),
        scratch_shapes=[pltpu.VMEM((keys, 128), low)] * 2 + [pltpu.VMEM((keys, 128), f32)] * 2,
        compiler_params=pltpu.CompilerParams(vmem_limit_bytes=VMEM_LIMIT),
        cost_estimate=pl.CostEstimate(
            flops=40 * rows * keys * width, bytes_accessed=20000000, transcendentals=0
        ),
        name="unattend",
    )(qkv, qkv, qkv, far, far, bias, lse, grad)


def unproject_kernel(
    dq, dkv, got, w, spots, freqs, tok, gain, d_resid, d_proj, d_tok, sums, col, acc, cos, sin
):
    y, t = pl.program_id(0), pl.program_id(1)
    first = (y == 0) & (t == 0)

    @pl.when(first)
    def _():
        cosine, sine = tables(spots[...], freqs[...])
        cos[...] = cosine
        sin[...] = -sine

    def put(value):
        rounded = value.astype(low)
        d_proj[0] = rounded
        return rounded

    def turned(value):
        parts = [
            turn(value[:, n * 128 : (n + 1) * 128], cos[...], sin[...])
            for n in range(value.shape[1] // 128)
        ]
        return jnp.concatenate(parts, axis=1)

    @pl.when(t == 0)
    def _():
        put(turned(dq[...]))

    @pl.when(t == 1)
    def _():
        put(turned(dkv[0] + got[0].astype(f32)))

    @pl.when(t == 2)
    def _():
        put(dkv[0] + got[0].astype(f32))

    rounded = d_proj[0]
    col[0] = jnp.sum(rounded.astype(f32), axis=0, keepdims=True)
    part = mm(rounded, w[0], NT)

    @pl.when(first)
    def _():
        acc[...] = part

    @pl.when(jnp.logical_not(first))
    def _():
        acc[...] += part

    @pl.when((y == 1) & (t == 2))
    def _():
        width = tok.shape[1]
        normed, inverse = normalise(tok[...].astype(f32), width)
        up = acc[...]
        sums[0:1] = jnp.sum(up * normed, axis=0, keepdims=True)
        sums[1:2] = jnp.sum(up, axis=0, keepdims=True)
        scaled = up * gain[...]
        mean = jnp.sum(scaled, axis=-1, keepdims=True) / width
        cross = jnp.sum(scaled * normed, axis=-1, keepdims=True) / width
        d_tok[...] = (d_resid[...] + inverse * (scaled - mean - normed * cross)).astype(low)


def unproject(dq, dkv, got, w, spots, freqs, tok, gain, d_resid):
    rows, width = tok.shape
    half = w.shape[2] // 3
    whole = lambda *s: pl.BlockSpec(s, lambda y, t: (0,) * len(s))
    pick = lambda y, t: (jnp.maximum(t - 1, 0), 0, y)
    return pl.pallas_call(
        unproject_kernel,
        grid=(2, 3),
        out_shape=(
            jax.ShapeDtypeStruct((3, rows, width), low),
            jax.ShapeDtypeStruct((rows, width), low),
            jax.ShapeDtypeStruct((2, width), f32),
            jax.ShapeDtypeStruct((3, 1, width), f32),
        ),
        in_specs=[
            pl.BlockSpec((rows, half), lambda y, t: (0, y)),
            pl.BlockSpec((1, rows, half), pick), pl.BlockSpec((1, rows, half), pick),
            pl.BlockSpec((1, width, half), lambda y, t: (y, 0, t)),
            whole(rows, 128), whole(1, 128), whole(rows, width), whole(1, width),
            whole(rows, width),
        ],
        out_specs=(
            pl.BlockSpec((1, rows, half), lambda y, t: (t, 0, y)), whole(rows, width),
            whole(2, width), pl.BlockSpec((1, 1, half), lambda y, t: (t, 0, y)),
        ),
        scratch_shapes=[
            pltpu.VMEM((rows, width), f32), pltpu.VMEM((rows, 128), f32),
            pltpu.VMEM((rows, 128), f32),
        ],
        compiler_params=pltpu.CompilerParams(vmem_limit_bytes=VMEM_LIMIT),
        cost_estimate=pl.CostEstimate(
            flops=2 * rows * width * width * 3, bytes_accessed=20000000, transcendentals=0
        ),
        name="unproject",
    )(dq, dkv, got, w, spots, freqs, tok, gain, d_resid)


def on_device(
    count, tokens, positions, key_mask, norm1_gain, norm1_bias, qkv_weight, qv_bias, out_weight,
    out_bias, norm2_gain, norm2_bias, gate_up_weight, gate_up_bias, inner_gain, inner_bias,
    down_weight, down_bias, cotangent,
):
    b, x, c, y = (lax.axis_index(a) for a in FAR)
    image = 2 * x + y
    local, images, width = tokens.shape
    shard = qkv_weight.shape[0]
    half = qkv_weight.shape[2]
    part = gate_up_weight.shape[2]
    hidden = gate_up_bias.shape[1]
    wide = -(-part // 128) * 128
    more = wide - part
    rows = 4 * PAD

    shards = [
        qkv_weight.astype(low).reshape(shard, 3 * half),
        out_weight.astype(low).T,
        jnp.pad(gate_up_weight.astype(low), ((0, 0), (0, 0), (0, more))).reshape(shard, 2 * wide),
        jnp.pad(down_weight.astype(low).T, ((0, 0), (0, more))),
    ]
    chunks = jnp.pad(jnp.swapaxes(tokens, 0, 1), ((0, 0), (0, PAD - local), (0, 0)))
    cot = jnp.transpose(cotangent.reshape(2, local, images, width), (2, 0, 1, 3))
    cot = jnp.pad(cot, ((0, 0), (0, 0), (0, PAD - local), (0, 0)))
    spots = jnp.transpose(positions.reshape(2, 2, local, images), (3, 1, 2, 0)).astype(low)
    spots = jnp.pad(spots, ((0, 0), (0, 0), (0, PAD - local), (0, 0)))
    pick = (jnp.arange(128) // 32) % 2
    spots = jnp.where(pick == 0, spots[..., 0:1], spots[..., 1:2])
    *full, tok, spot, cot_in = gather_all(count, shards, chunks, spots, cot)
    w_qkv, w_out, w_gu, w_down = (f.reshape(2, width, f.shape[-1]) for f in full)
    one = lambda a: lax.dynamic_slice_in_dim(a, image, 1, 0)
    tok = lax.dynamic_update_slice_in_dim(tok, one(chunks), image, 0).reshape(rows, width)
    spot = lax.dynamic_update_slice_in_dim(spot, one(spots), x, 0).reshape(rows, 128)
    grad = lax.dynamic_update_slice_in_dim(cot_in, one(cot), x, 0).reshape(rows, width)

    live = lax.dynamic_index_in_dim(key_mask, image, 1, keepdims=False)
    live = jnp.pad(live.reshape(2, 2, 2, local), ((0, 0), (0, 0), (0, 0), (0, PAD - local)))
    live = jnp.stack(
        [lax.dynamic_index_in_dim(live, n, 1, keepdims=False).reshape(rows) for n in (c, 1 - c)]
    )
    bias = jnp.where(live > 0, 0.0, masked_score).astype(f32).reshape(1, 2 * rows)

    freqs = (10000.0 ** (-jnp.arange(16).astype(f32) / 16))[jnp.arange(128) % 16].reshape(1, 128)
    row = lambda a: a.reshape(1, -1)
    qkv_bias = jnp.stack([qv_bias[0], jnp.zeros_like(qv_bias[0]), qv_bias[1]])[:, None]
    qkv, h1 = project(tok, row(norm1_gain), row(norm1_bias), w_qkv, qkv_bias, spot, freqs)
    swap = ((0, 1), (1, 0))
    far = lax.ppermute(qkv[1:], "core", swap)
    attended, lse = attend(qkv, far, bias)

    split = lambda a: jnp.pad(a.reshape(a.shape[:-1] + (2, part)), ((0, 0),) * a.ndim + ((0, more),))
    gu_bias = jnp.swapaxes(split(gate_up_bias), 0, 1).reshape(2, 2 * wide)
    in_gain, in_bias = split(inner_gain), split(inner_bias)
    attn = sum(mm(attended[:, n * half : (n + 1) * half], w_out[n], NT) for n in range(2))
    resid = tok.astype(f32) + attn + out_bias
    normed2, inverse2 = normalise(resid, width)
    h2 = (normed2 * norm2_gain + norm2_bias).astype(low)
    gate_up = [mm(h2, w_gu[n], NN) + gu_bias[n] for n in range(2)]
    gate, up = [g[:, :wide] for g in gate_up], [g[:, wide:] for g in gate_up]
    sigma = [jax.nn.sigmoid(g) for g in gate]
    act = [gate[n] * sigma[n] * up[n] for n in range(2)]
    centre = sum(jnp.sum(a, axis=-1, keepdims=True) for a in act) / hidden
    real = (jnp.arange(wide) < part)[None]
    shifted = [jnp.where(real, a - centre, 0.0) for a in act]
    spread = sum(jnp.sum(jnp.square(s), axis=-1, keepdims=True) for s in shifted) / hidden
    inverse3 = lax.rsqrt(spread + epsilon)
    normed3 = [s * inverse3 for s in shifted]
    inner = [(normed3[n] * in_gain[n] + in_bias[n]).astype(low) for n in range(2)]
    ffn = sum(mm(inner[n], w_down[n], NT) for n in range(2))
    mixed = (resid + ffn + down_bias).astype(low)

    d_down_bias = jnp.sum(grad.astype(f32), axis=0)
    d_inner = [mm(grad, w_down[n], NN) for n in range(2)]
    d_in_gain = jnp.stack([jnp.sum(d_inner[n] * normed3[n], axis=0) for n in range(2)])
    d_in_bias = jnp.stack([jnp.sum(d, axis=0) for d in d_inner])
    scaled = [d_inner[n] * in_gain[n] for n in range(2)]
    mean = sum(jnp.sum(s, axis=-1, keepdims=True) for s in scaled) / hidden
    cross = sum(jnp.sum(scaled[n] * normed3[n], axis=-1, keepdims=True) for n in range(2)) / hidden
    d_gu = []
    for n in range(2):
        d_act = inverse3 * (scaled[n] - mean - normed3[n] * cross)
        d_gate = d_act * up[n] * sigma[n] * (1.0 + gate[n] * (1.0 - sigma[n]))
        d_gu.append(jnp.concatenate([d_gate, d_act * gate[n] * sigma[n]], axis=1).astype(low))
    d_gu_bias = jnp.stack([jnp.sum(d.astype(f32), axis=0) for d in d_gu])
    d_h2 = sum(mm(d_gu[n], w_gu[n], NT) for n in range(2))
    d_gain2, d_bias2 = jnp.sum(d_h2 * normed2, axis=0), jnp.sum(d_h2, axis=0)
    scaled2 = d_h2 * norm2_gain
    mean2 = jnp.mean(scaled2, axis=-1, keepdims=True)
    cross2 = jnp.mean(scaled2 * normed2, axis=-1, keepdims=True)
    d_resid = grad.astype(f32) + inverse2 * (scaled2 - mean2 - normed2 * cross2)
    g_attn = d_resid.astype(low)
    d_out_bias = jnp.sum(g_attn.astype(f32), axis=0)
    d_attended = jnp.concatenate([mm(g_attn, w_out[n], NN).astype(low) for n in range(2)], axis=1)

    spread_out = lambda a, b: jnp.stack([mm(a, b[n], TN).astype(low) for n in range(2)]).reshape(
        2, count, 2, 2, shard, -1
    )
    p_down = spread_out(grad, inner)
    p_gu = spread_out(h2, d_gu)
    p_out = spread_out(g_attn, [attended[:, n * half : (n + 1) * half] for n in range(2)])

    dq, dkv, dfar = unattend(qkv, far, bias, lse, d_attended)
    got = lax.ppermute(dfar, "core", swap)
    d_proj, d_tok, sums1, col = unproject(
        dq, dkv, got, w_qkv, spot, freqs, tok, row(norm1_gain), d_resid
    )
    flat = [jnp.concatenate([d_proj[t, :, n * half : (n + 1) * half] for t in range(3)], axis=1) for n in range(2)]
    p_qkv = spread_out(h1, flat)
    r_down, r_gu, r_out, r_qkv = scatter_all(count, [p_down, p_gu, p_out, p_qkv], 1)

    merge = lambda a: a[..., :part].reshape(a.shape[:-2] + (hidden,))
    d_gu_bias = merge(jnp.swapaxes(d_gu_bias.reshape(2, 2, wide), 0, 1))
    vectors = [
        sums1[0], sums1[1], jnp.stack([col[0, 0], col[2, 0]]), d_out_bias, d_gain2, d_bias2,
        d_gu_bias, merge(d_in_gain), merge(d_in_bias), d_down_bias,
    ]
    flat = jnp.concatenate([v.reshape(-1) for v in vectors])
    size = flat.shape[0]
    lines = -(-size // 2048) * 16
    summed = sum_all(count, jnp.pad(flat, (0, lines * 128 - size)).reshape(lines, 128), 2)
    summed = summed.reshape(-1)
    pieces, at = [], 0
    for v in vectors:
        pieces.append(summed[at : at + v.size].reshape(v.shape))
        at += v.size

    def home(values):
        parts = values.reshape(4, PAD, width)
        out = jnp.zeros((images, local, width), low)
        for ox, oy in ((0, 0), (1, 0), (0, 1), (1, 1)):
            there = 2 * (1 - x if ox else x) + (1 - y if oy else y)
            piece = lax.dynamic_slice_in_dim(parts, there, 1, 0)[:, :local]
            if ox and oy:
                piece = lax.ppermute(piece, ("x", "tensor"), ((0, 3), (3, 0), (1, 2), (2, 1)))
            elif ox:
                piece = lax.ppermute(piece, "x", swap)
            elif oy:
                piece = lax.ppermute(piece, "tensor", swap)
            out = lax.dynamic_update_slice_in_dim(out, piece, there, 0)
        return jnp.swapaxes(out, 0, 1)

    return (
        home(mixed), home(d_tok), pieces[0], pieces[1], r_qkv.reshape(shard, 3, half), pieces[2],
        r_out.T, pieces[3], pieces[4], pieces[5], r_gu.reshape(shard, 2, wide)[:, :, :part],
        pieces[6], pieces[7], pieces[8], r_down[:, :part].T, pieces[9],
    )


def solution(mesh):
    count, ctx, tensor = (mesh.shape[a] for a in ("batch", "ctx", "tensor"))
    fine = jax.sharding.Mesh(mesh.devices.reshape(count, ctx // 2, 2, tensor), FAR)
    ctx, wide = ("x", "core"), ("batch", "x", "core")
    return jax.shard_map(
        functools.partial(on_device, count),
        mesh=fine,
        in_specs=(
            P(("x", "core", "tensor"), "batch", None), P(None, ctx, "batch"), P(None, "batch"),
            P(), P(), P(wide, None, "tensor"), P(), P("tensor", wide), P(), P(), P(),
            P(wide, None, "tensor"), P(), P(), P(), P("tensor", wide), P(), P(ctx, "batch", None),
        ),
        out_specs=(
            P(("x", "core", "tensor"), "batch", None), P(("x", "core", "tensor"), "batch", None),
            P(), P(), P(wide, None, "tensor"), P(), P("tensor", wide), P(), P(), P(),
            P(wide, None, "tensor"), P(), P(), P(), P("tensor", wide), P(),
        ),
        check_vma=False,
    )
```

```python
import functools

import jax
import jax.numpy as jnp
from jax import lax
from jax.experimental import pallas as pl
from jax.experimental.pallas import tpu as pltpu

from jax.sharding import PartitionSpec as P
MESH = pl.DeviceIdType.MESH
FAR = ("batch", "x", "core", "tensor")


def place(b, x, c, y):
    return {"batch": b, "x": x, "core": c, "tensor": y}


def ring_offsets(count):
    order = [0]
    for step in range(1, count // 2 + 1):
        for off in (step, count - step):
            if off not in order:
                order.append(off)
    return order


def greet(count, corner=False):
    b, x, c, y = (lax.axis_index(a) for a in FAR)
    barrier = pltpu.get_barrier_semaphore()
    for off in range(1, count):
        pl.semaphore_signal(
            barrier, inc=1, device_id=place(lax.rem(b + off, count), x, c, y), device_id_type=MESH
        )
    near = [place(b, 1 - x, c, y), place(b, x, c, 1 - y), place(b, x, 1 - c, y)]
    if corner:
        near.append(place(b, 1 - x, c, 1 - y))
    for there in near:
        pl.semaphore_signal(barrier, inc=1, device_id=there, device_id_type=MESH)
    pl.semaphore_wait(barrier, count - 1 + len(near))


def gather_kernel(count, groups, *refs):
    own = refs[:groups]
    moved = refs[groups : groups + 3]
    full = refs[groups + 3 : 2 * groups + 3]
    landed = refs[2 * groups + 3 : 2 * groups + 6]
    zs, zr, xs, xr, ys, yr, xds, yds, dr, cs, cr, ls, ts, tr = refs[2 * groups + 6 :]
    b, x, c, y = (lax.axis_index(a) for a in FAR)
    xn, yn, cn = place(b, 1 - x, c, y), place(b, x, c, 1 - y), place(b, x, 1 - c, y)
    offsets = ring_offsets(count)
    tokens, spots, cot = moved
    greet(count, corner=True)

    def send(src, dst, s, r, there):
        pltpu.make_async_remote_copy(
            src_ref=src, dst_ref=dst, send_sem=s, recv_sem=r, device_id=there, device_id_type=MESH
        ).start()

    def arrived(dst, sem):
        pltpu.make_async_copy(dst, dst, sem).wait()

    mine = 2 * x + y
    for n, (ox, oy) in enumerate(((1, 0), (0, 1), (1, 1))):
        px = 1 - x if ox else x
        py = 1 - y if oy else y
        send(
            tokens.at[2 * px + py], landed[0].at[mine], ts.at[n], tr.at[n], place(b, px, c, py)
        )
    far = 2 * (1 - x) + y
    send(spots.at[far], landed[1].at[x], ts.at[3], tr.at[3], xn)

    def block(g, yy, item, xx, cc):
        bb = lax.rem(b + offsets[item], count)
        return full[g].at[yy, bb, xx, cc]

    def shard(g, item):
        return own[g] if item == 0 else block(g, y, item, x, c)

    items = [(g, j) for g in range(groups) for j in range(count)]
    for g in range(groups):
        home = full[g].at[y, b, x, c]
        for j in range(1, count):
            there = place(lax.rem(b + count - offsets[j], count), x, c, y)
            send(own[g], home, zs.at[g], zr.at[g, j], there)
        if g == 0:
            send(cot.at[far], landed[2].at[x], ts.at[4], tr.at[4], xn)

    def stage_column(g, j):
        if j > 0:
            arrived(block(g, y, j, x, c), zr.at[g, j])
        src, dst = shard(g, j), block(g, y, j, x, c)
        send(src, dst, xs.at[g], xr.at[g, j], xn)
        send(src, dst, ys.at[g], yr.at[g, j], yn)
        send(src, dst, cs.at[g], cr.at[g], cn)

    def stage_plane(g, j):
        from_x, from_y = block(g, y, j, 1 - x, c), block(g, 1 - y, j, x, c)
        arrived(from_x, xr.at[g, j])
        if j % 2 == 0:
            send(from_x, from_x, yds.at[g], dr.at[g, j], yn)
        send(from_x, from_x, cs.at[g], cr.at[g], cn)
        arrived(from_y, yr.at[g, j])
        if j % 2 == 1:
            send(from_y, from_y, xds.at[g], dr.at[g, j], xn)
        send(from_y, from_y, cs.at[g], cr.at[g], cn)

    def stage_corner(g, j):
        corner = block(g, 1 - y, j, 1 - x, c)
        arrived(corner, dr.at[g, j])
        send(corner, corner, cs.at[g], cr.at[g], cn)

    homes = []
    for g in range(groups):
        copy = pltpu.make_async_copy(own[g], full[g].at[y, b, x, c], ls.at[g])
        copy.start()
        homes.append(copy)
    for t in range(len(items) + 2):
        if t < len(items):
            stage_column(*items[t])
        if 1 <= t <= len(items):
            stage_plane(*items[t - 1])
        if t >= 2:
            stage_corner(*items[t - 2])
    for copy in homes:
        copy.wait()
    for n, (ox, oy) in enumerate(((1, 0), (0, 1), (1, 1))):
        px = 1 - x if ox else x
        py = 1 - y if oy else y
        arrived(landed[0].at[2 * px + py], tr.at[n])
        arrived(tokens.at[0], ts.at[n])
    arrived(landed[1].at[1 - x], tr.at[3])
    arrived(spots.at[0], ts.at[3])
    arrived(landed[2].at[1 - x], tr.at[4])
    arrived(cot.at[0], ts.at[4])
    for g in range(groups):
        arrived(full[g].at[:, :, :, 1 - c], cr.at[g])
        arrived(full[g].at[:, :, :, 0], cs.at[g])
        arrived(full[g].at[0, : count - 1, 0, 0], zs.at[g])
        arrived(full[g].at[0, :, 0, 0], xs.at[g])
        arrived(full[g].at[0, :, 0, 0], ys.at[g])
        arrived(full[g].at[0, : count // 2, 0, 0], xds.at[g])
        arrived(full[g].at[0, : (count + 1) // 2, 0, 0], yds.at[g])


def gather_all(count, shards, tokens, spots, cot):
    groups = len(shards)
    any_spec = pl.BlockSpec(memory_space=pl.ANY)
    dma = pltpu.SemaphoreType.DMA
    outs = [jax.ShapeDtypeStruct((2, count, 2, 2) + s.shape, s.dtype) for s in shards]
    outs += [
        jax.ShapeDtypeStruct(tokens.shape, tokens.dtype),
        jax.ShapeDtypeStruct((2,) + spots.shape[1:], spots.dtype),
        jax.ShapeDtypeStruct((2,) + cot.shape[1:], cot.dtype),
    ]
    return pl.pallas_call(
        functools.partial(gather_kernel, count, groups),
        out_shape=outs,
        in_specs=[any_spec] * (groups + 3),
        out_specs=[any_spec] * len(outs),
        scratch_shapes=[
            dma((groups,)), dma((groups, count)), dma((groups,)), dma((groups, count)),
            dma((groups,)), dma((groups, count)), dma((groups,)), dma((groups,)),
            dma((groups, count)), dma((groups,)), dma((groups,)), dma((groups,)),
            dma((5,)), dma((5,)),
        ],
        compiler_params=pltpu.CompilerParams(collective_id=0, has_side_effects=True),
        name="gather_all",
    )(*shards, tokens, spots, cot)
def scatter_kernel(count, groups, moves, *refs):
    parts = refs[:groups]
    leaving = refs[groups : groups + moves]
    outs = refs[groups + moves : 2 * groups + moves]
    landed = refs[2 * groups + moves : 2 * groups + 2 * moves]
    at = 2 * groups + 2 * moves
    held, peer, from_x, from_y, from_d, from_z = (
        refs[at + k * groups : at + (k + 1) * groups] for k in range(6)
    )
    ls, cs, cr, xs, xr, ys, yr, xds, yds, dr, zs, zr, ts, tr, tl = refs[at + 6 * groups :]
    b, x, c, y = (lax.axis_index(a) for a in FAR)
    xn, yn, cn = place(b, 1 - x, c, y), place(b, x, c, 1 - y), place(b, x, 1 - c, y)
    offsets = ring_offsets(count)
    order = list(range(1, count)) + [0]
    rows = held[0].shape[3]
    chunk = min(rows, 16)
    image = 2 * x + y
    corners = ((1, 0), (0, 1), (1, 1))
    greet(count, corner=moves > 0)

    def send(src, dst, s, r, there):
        pltpu.make_async_remote_copy(
            src_ref=src, dst_ref=dst, send_sem=s, recv_sem=r, device_id=there, device_id_type=MESH
        ).start()

    def arrived(dst, sem):
        pltpu.make_async_copy(dst, dst, sem).wait()

    def add_to(target, *others):
        def body(i, carry):
            at_rows = pl.ds(pl.multiple_of(i * chunk, chunk), chunk)
            total = target[at_rows].astype(jnp.float32)
            for other in others:
                total = total + other[at_rows].astype(jnp.float32)
            target[at_rows] = total.astype(target.dtype)
            return carry

        lax.fori_loop(0, rows // chunk, body, 0)

    def where_to(j):
        return lax.rem(b + offsets[j], count)

    items = [(g, j) for g in range(groups) for j in order]
    for g, j in items:
        bb = where_to(j)
        send(parts[g].at[:, bb, :, 1 - c], peer[g].at[:, bb], cs.at[g], cr.at[g, j], cn)
        pltpu.make_async_copy(parts[g].at[:, bb, :, c], held[g].at[:, bb], ls.at[g, j]).start()

    for m in range(moves):
        pltpu.make_async_copy(leaving[m].at[image], landed[m].at[image], tl.at[m]).start()
        for n, (ox, oy) in enumerate(corners):
            px, py = (1 - x if ox else x), (1 - y if oy else y)
            send(
                leaving[m].at[2 * px + py], landed[m].at[image], ts.at[m, n], tr.at[m, n],
                place(b, px, c, py),
            )

    def merge_core(g, j):
        bb = where_to(j)
        arrived(held[g].at[:, bb], ls.at[g, j])
        arrived(peer[g].at[:, bb], cr.at[g, j])
        for yy, xx in ((1 - y, 1 - x), (y, 1 - x), (1 - y, x), (y, x)):
            add_to(held[g].at[yy, bb, xx], peer[g].at[yy, bb, xx])

    def send_corner(g, j):
        src = held[g].at[1 - y, where_to(j), 1 - x]
        if j % 2 == 0:
            send(src, from_d[g].at[j], xds.at[g], dr.at[g, j], xn)
        else:
            send(src, from_d[g].at[j], yds.at[g], dr.at[g, j], yn)

    def merge_corner(g, j):
        bb = where_to(j)
        arrived(from_d[g].at[j], dr.at[g, j])
        if j % 2 == 0:
            add_to(held[g].at[1 - y, bb, x], from_d[g].at[j])
        else:
            add_to(held[g].at[y, bb, 1 - x], from_d[g].at[j])

    def send_plane(g, j):
        bb = where_to(j)
        send(held[g].at[y, bb, 1 - x], from_x[g].at[j], xs.at[g], xr.at[g, j], xn)
        send(held[g].at[1 - y, bb, x], from_y[g].at[j], ys.at[g], yr.at[g, j], yn)

    def merge_plane(g, j):
        arrived(from_x[g].at[j], xr.at[g, j])
        arrived(from_y[g].at[j], yr.at[g, j])
        add_to(held[g].at[y, where_to(j), x], from_x[g].at[j], from_y[g].at[j])

    def send_column(g, j):
        if j > 0:
            bb = where_to(j)
            send(
                held[g].at[y, bb, x], from_z[g].at[j], zs.at[g], zr.at[g, j], place(bb, x, c, y)
            )

    total = len(items)
    for t in range(total + 2):
        now = items[t] if t < total else None
        one = items[t - 1] if 1 <= t <= total else None
        two = items[t - 2] if 2 <= t else None
        if two:
            merge_plane(*two)
        if one:
            merge_corner(*one)
        if now:
            merge_core(*now)
            send_corner(*now)
        if one:
            send_plane(*one)
        if two:
            send_column(*two)
    for g in range(groups):
        for j in range(1, count):
            arrived(from_z[g].at[j], zr.at[g, j])

        def body(i, carry, g=g):
            at_rows = pl.ds(pl.multiple_of(i * chunk, chunk), chunk)
            result = held[g][y, b, x, at_rows].astype(jnp.float32)
            for j in range(1, count):
                result = result + from_z[g][j, at_rows].astype(jnp.float32)
            outs[g][at_rows] = result
            return carry

        lax.fori_loop(0, rows // chunk, body, 0)
        arrived(peer[g], cs.at[g])
        arrived(from_x[g], xs.at[g])
        arrived(from_y[g], ys.at[g])
        arrived(from_d[g].at[: (count + 1) // 2], xds.at[g])
        arrived(from_d[g].at[: count // 2], yds.at[g])
        arrived(from_z[g].at[1:], zs.at[g])
    for m in range(moves):
        pltpu.make_async_copy(leaving[m].at[image], landed[m].at[image], tl.at[m]).wait()
        for n, (ox, oy) in enumerate(corners):
            px, py = (1 - x if ox else x), (1 - y if oy else y)
            arrived(landed[m].at[2 * px + py], tr.at[m, n])
            arrived(leaving[m].at[0], ts.at[m, n])


def scatter_all(count, parts, leaving, number):
    groups, moves = len(parts), len(leaving)
    dma = pltpu.SemaphoreType.DMA
    shapes = [p.shape[4:] for p in parts]
    low = jnp.bfloat16
    scratch = [pltpu.VMEM((2, count, 2) + s, low) for s in shapes] * 2
    scratch += [pltpu.VMEM((count,) + s, low) for s in shapes] * 4
    many, one = dma((groups, count)), dma((groups,))
    scratch += [many, one, many, one, many, one, many, one, one, many, one, many]
    scratch += [dma((max(moves, 1), 3)), dma((max(moves, 1), 3)), dma((max(moves, 1),))]
    return pl.pallas_call(
        functools.partial(scatter_kernel, count, groups, moves),
        out_shape=[jax.ShapeDtypeStruct(s, jnp.float32) for s in shapes]
        + [jax.ShapeDtypeStruct(a.shape, a.dtype) for a in leaving],
        in_specs=[pl.BlockSpec(memory_space=pl.ANY)] * (groups + moves),
        out_specs=[pl.BlockSpec(memory_space=pltpu.VMEM)] * groups
        + [pl.BlockSpec(memory_space=pl.ANY)] * moves,
        scratch_shapes=scratch,
        compiler_params=pltpu.CompilerParams(
            collective_id=number, has_side_effects=True, vmem_limit_bytes=64000000
        ),
        name="scatter_all",
    )(*parts, *leaving)


def sum_kernel(count, v_ref, o_ref, got, lane, plane, slots, ss, rs, zs, zr):
    b, x, c, y = (lax.axis_index(a) for a in FAR)
    xn, yn, cn = place(b, 1 - x, c, y), place(b, x, c, 1 - y), place(b, x, 1 - c, y)
    half = v_ref.shape[0] // 2
    mine = pl.ds(pl.multiple_of(c * half, 8), half)
    theirs = pl.ds(pl.multiple_of((1 - c) * half, 8), half)
    greet(count)

    def swap(src, dst, n, there):
        copy = pltpu.make_async_remote_copy(
            src_ref=src, dst_ref=dst, send_sem=ss.at[n], recv_sem=rs.at[n], device_id=there,
            device_id_type=MESH,
        )
        copy.start()
        copy.wait()

    swap(v_ref.at[theirs], got.at[0], 0, cn)
    lane[...] = v_ref[mine] + got[0]
    swap(lane, got.at[1], 1, xn)
    plane[...] = lane[...] + got[1]
    swap(plane, got.at[2], 2, yn)
    slots[b] = plane[...] + got[2]
    for off in range(1, count):
        pltpu.make_async_remote_copy(
            src_ref=slots.at[b], dst_ref=slots.at[b], send_sem=zs, recv_sem=zr.at[off],
            device_id=place(lax.rem(b + off, count), x, c, y), device_id_type=MESH,
        ).start()
    for off in range(1, count):
        there = slots.at[lax.rem(b + count - off, count)]
        pltpu.make_async_copy(there, there, zr.at[off]).wait()
    total = slots[0]
    for n in range(1, count):
        total = total + slots[n]
    o_ref[mine] = total
    swap(o_ref.at[mine], o_ref.at[mine], 3, cn)
    rest = slots.at[: count - 1]
    pltpu.make_async_copy(rest, rest, zs).wait()


def sum_all(count, vector, number):
    rows = vector.shape[0]
    half = (rows // 2, 128)
    dma = pltpu.SemaphoreType.DMA
    vm = pltpu.VMEM
    return pl.pallas_call(
        functools.partial(sum_kernel, count),
        out_shape=jax.ShapeDtypeStruct(vector.shape, jnp.float32),
        in_specs=[pl.BlockSpec(memory_space=pltpu.VMEM)],
        out_specs=pl.BlockSpec(memory_space=pltpu.VMEM),
        scratch_shapes=[
            vm((3,) + half, jnp.float32), vm(half, jnp.float32), vm(half, jnp.float32),
            vm((count,) + half, jnp.float32), dma((4,)), dma((4,)), dma(()), dma((count,)),
        ],
        compiler_params=pltpu.CompilerParams(collective_id=number, has_side_effects=True),
        name="sum_all",
    )(vector)

PAD = 136
WIDTH_TILE = 128
HEAD_DIM = 64
epsilon = 1e-06
masked_score = -1e30
f32, low = jnp.float32, jnp.bfloat16
VMEM_LIMIT = 60000000


def mm(a, b, dims):
    return lax.dot_general(a, b, (dims, ((), ())), preferred_element_type=f32)


NN = ((1,), (0,))
NT = ((1,), (1,))
TN = ((0,), (0,))


def normalise(values, width):
    centre = jnp.sum(values, axis=-1, keepdims=True) / width
    shifted = values - centre
    spread = jnp.sum(jnp.square(shifted), axis=-1, keepdims=True) / width
    inverse = lax.rsqrt(spread + epsilon)
    return shifted * inverse, inverse


def turn(values, cosine, sine):
    lane = lax.broadcasted_iota(jnp.int32, values.shape, 1)
    other = jnp.where((lane // 16) % 2 == 0, pltpu.roll(values, 112, 1), pltpu.roll(values, 16, 1))
    return values * cosine + other * sine


def tables(spots, freqs):
    angles = spots.astype(f32) * freqs
    lane = lax.broadcasted_iota(jnp.int32, angles.shape, 1)
    sine = jnp.sin(angles)
    return jnp.cos(angles), jnp.where((lane // 16) % 2 == 0, -sine, sine)


def project_kernel(tok, gain, shift, w, bias, spots, freqs, out, h_out, hid, cos, sin):
    y, t = pl.program_id(0), pl.program_id(1)

    @pl.when((y == 0) & (t == 0))
    def _():
        normed, _ = normalise(tok[...].astype(f32), tok.shape[1])
        hid[...] = (normed * gain[...] + shift[...]).astype(low)
        h_out[...] = hid[...]
        cosine, sine = tables(spots[...], freqs[...])
        cos[...] = cosine
        sin[...] = sine

    acc = mm(hid[...], w[0], NN) + bias[0]

    @pl.when(t < 2)
    def _():
        for n in range(acc.shape[1] // 128):
            part = acc[:, n * 128 : (n + 1) * 128]
            out[0, :, n * 128 : (n + 1) * 128] = turn(part, cos[...], sin[...]).astype(low)

    @pl.when(t == 2)
    def _():
        out[0] = acc.astype(low)


def project(tok, gain, shift, w, bias, spots, freqs):
    rows, width = tok.shape
    half = w.shape[2] // 3
    whole = lambda *s: pl.BlockSpec(s, lambda y, t: (0,) * len(s))
    return pl.pallas_call(
        project_kernel,
        grid=(2, 3),
        out_shape=(
            jax.ShapeDtypeStruct((3, rows, width), low),
            jax.ShapeDtypeStruct((rows, width), low),
        ),
        in_specs=[
            whole(rows, width), whole(1, width), whole(1, width),
            pl.BlockSpec((1, width, half), lambda y, t: (y, 0, t)),
            pl.BlockSpec((1, 1, half), lambda y, t: (t, 0, y)),
            whole(rows, 128), whole(1, 128),
        ],
        out_specs=(
            pl.BlockSpec((1, rows, half), lambda y, t: (t, 0, y)), whole(rows, width),
        ),
        scratch_shapes=[
            pltpu.VMEM((rows, width), low), pltpu.VMEM((rows, 128), f32),
            pltpu.VMEM((rows, 128), f32),
        ],
        compiler_params=pltpu.CompilerParams(vmem_limit_bytes=VMEM_LIMIT),
        cost_estimate=pl.CostEstimate(
            flops=2 * rows * width * width * 3, bytes_accessed=14000000, transcendentals=0
        ),
        name="project",
    )(tok, gain, shift, w, bias, spots, freqs)


def head_lanes(rows):
    return lax.broadcasted_iota(jnp.int32, (rows, 128), 1) // HEAD_DIM


def attend_kernel(q, k, v, kp, vp, bias, out, lse, keys, vals, *, chunk):
    pair = pl.program_id(0)
    rows = q.shape[1]
    keys[:rows], keys[rows:] = k[0], kp[0]
    vals[:rows], vals[rows:] = v[0], vp[0]
    lanes = head_lanes(chunk)
    spot = lax.broadcasted_iota(jnp.int32, (chunk, 128), 1)
    for n in range(rows // chunk):
        here = slice(n * chunk, (n + 1) * chunk)
        query = q[0, here] * low(HEAD_DIM**-0.5)
        result = None
        kept = lse[here]
        for h in range(2):
            mine = jnp.where(lanes == h, query, low(0))
            scores = mm(mine, keys[...], NT) + bias[...]
            top = jnp.max(scores, axis=-1, keepdims=True)
            weight = jnp.exp(scores - top)
            total = jnp.sum(weight, axis=-1, keepdims=True)
            probs = (weight * (1.0 / total)).astype(low)
            got = mm(probs, vals[...], NN)
            result = got if h == 0 else jnp.where(lanes == 0, result, got)
            kept = jnp.where(spot == 2 * pair + h, top + jnp.log(total), kept)
        lse[here] = kept
        out[here] = result.astype(low)


def attend(qkv, far, bias):
    _, rows, width = qkv.shape
    keys = 2 * rows
    at = lambda t: pl.BlockSpec((1, rows, 128), lambda g: (t, 0, g))
    return pl.pallas_call(
        functools.partial(attend_kernel, chunk=rows // 2),
        grid=(width // 128,),
        out_shape=(
            jax.ShapeDtypeStruct((rows, width), low), jax.ShapeDtypeStruct((rows, 128), f32),
        ),
        in_specs=[at(0), at(1), at(2), at(0), at(1), pl.BlockSpec((1, keys), lambda g: (0, 0))],
        out_specs=(
            pl.BlockSpec((rows, 128), lambda g: (0, g)),
            pl.BlockSpec((rows, 128), lambda g: (0, 0)),
        ),
        scratch_shapes=[pltpu.VMEM((keys, 128), low)] * 2,
        compiler_params=pltpu.CompilerParams(vmem_limit_bytes=VMEM_LIMIT),
        cost_estimate=pl.CostEstimate(
            flops=16 * rows * keys * width, bytes_accessed=10000000, transcendentals=0
        ),
        name="attend",
    )(qkv, qkv, qkv, far, far, bias)


def unattend_kernel(q, k, v, kp, vp, bias, lse, grad, dq, dkv, dfar, keys, vals, dk, dv, *, chunk):
    pair = pl.program_id(0)
    rows = q.shape[1]
    keys[:rows], keys[rows:] = k[0], kp[0]
    vals[:rows], vals[rows:] = v[0], vp[0]
    lanes = head_lanes(chunk)
    spot = lax.broadcasted_iota(jnp.int32, (chunk, 128), 1)
    for n in range(rows // chunk):
        here = slice(n * chunk, (n + 1) * chunk)
        query = q[0, here] * low(HEAD_DIM**-0.5)
        out_grad = grad[here]
        result = None
        for h in range(2):
            mine = jnp.where(lanes == h, query, low(0))
            mine_grad = jnp.where(lanes == h, out_grad, low(0))
            shift = jnp.sum(jnp.where(spot == 2 * pair + h, lse[here], 0.0), axis=-1, keepdims=True)
            probs = jnp.exp(mm(mine, keys[...], NT) + bias[...] - shift)
            d_probs = mm(mine_grad, vals[...], NT)
            both = probs * d_probs
            inner = jnp.sum(both, axis=-1, keepdims=True)
            d_scores = (both - probs * inner).astype(low)
            got = mm(d_scores, keys[...], NN)
            result = got if h == 0 else jnp.where(lanes == 0, result, got)
            key_part = mm(d_scores, mine, TN)
            value_part = mm(probs.astype(low), mine_grad, TN)
            if n == 0 and h == 0:
                dk[...], dv[...] = key_part, value_part
            else:
                dk[...] += key_part
                dv[...] += value_part
        dq[here] = result * HEAD_DIM**-0.5
    dkv[0], dkv[1] = dk[:rows], dv[:rows]
    dfar[0], dfar[1] = dk[rows:].astype(low), dv[rows:].astype(low)


def unattend(qkv, far, bias, lse, grad):
    _, rows, width = qkv.shape
    keys = 2 * rows
    at = lambda t: pl.BlockSpec((1, rows, 128), lambda g: (t, 0, g))
    both = pl.BlockSpec((2, rows, 128), lambda g: (0, 0, g))
    column = pl.BlockSpec((rows, 128), lambda g: (0, g))
    return pl.pallas_call(
        functools.partial(unattend_kernel, chunk=rows // 2),
        grid=(width // 128,),
        out_shape=(
            jax.ShapeDtypeStruct((rows, width), f32),
            jax.ShapeDtypeStruct((2, rows, width), f32),
            jax.ShapeDtypeStruct((2, rows, width), low),
        ),
        in_specs=[
            at(0), at(1), at(2), at(0), at(1), pl.BlockSpec((1, keys), lambda g: (0, 0)),
            pl.BlockSpec((rows, 128), lambda g: (0, 0)), column,
        ],
        out_specs=(column, both, both),
        scratch_shapes=[pltpu.VMEM((keys, 128), low)] * 2 + [pltpu.VMEM((keys, 128), f32)] * 2,
        compiler_params=pltpu.CompilerParams(vmem_limit_bytes=VMEM_LIMIT),
        cost_estimate=pl.CostEstimate(
            flops=40 * rows * keys * width, bytes_accessed=20000000, transcendentals=0
        ),
        name="unattend",
    )(qkv, qkv, qkv, far, far, bias, lse, grad)


def unproject_kernel(
    dq, dkv, got, w, spots, freqs, tok, gain, d_resid, d_proj, d_tok, sums, col, acc, cos, sin
):
    y, t = pl.program_id(0), pl.program_id(1)
    first = (y == 0) & (t == 0)

    @pl.when(first)
    def _():
        cosine, sine = tables(spots[...], freqs[...])
        cos[...] = cosine
        sin[...] = -sine

    def put(value):
        rounded = value.astype(low)
        d_proj[0] = rounded
        return rounded

    def turned(value):
        parts = [
            turn(value[:, n * 128 : (n + 1) * 128], cos[...], sin[...])
            for n in range(value.shape[1] // 128)
        ]
        return jnp.concatenate(parts, axis=1)

    @pl.when(t == 0)
    def _():
        put(turned(dq[...]))

    @pl.when(t == 1)
    def _():
        put(turned(dkv[0] + got[0].astype(f32)))

    @pl.when(t == 2)
    def _():
        put(dkv[0] + got[0].astype(f32))

    rounded = d_proj[0]
    col[0] = jnp.sum(rounded.astype(f32), axis=0, keepdims=True)
    part = mm(rounded, w[0], NT)

    @pl.when(first)
    def _():
        acc[...] = part

    @pl.when(jnp.logical_not(first))
    def _():
        acc[...] += part

    @pl.when((y == 1) & (t == 2))
    def _():
        width = tok.shape[1]
        normed, inverse = normalise(tok[...].astype(f32), width)
        up = acc[...]
        sums[0:1] = jnp.sum(up * normed, axis=0, keepdims=True)
        sums[1:2] = jnp.sum(up, axis=0, keepdims=True)
        scaled = up * gain[...]
        mean = jnp.sum(scaled, axis=-1, keepdims=True) / width
        cross = jnp.sum(scaled * normed, axis=-1, keepdims=True) / width
        d_tok[...] = (d_resid[...] + inverse * (scaled - mean - normed * cross)).astype(low)


def unproject(dq, dkv, got, w, spots, freqs, tok, gain, d_resid):
    rows, width = tok.shape
    half = w.shape[2] // 3
    whole = lambda *s: pl.BlockSpec(s, lambda y, t: (0,) * len(s))
    pick = lambda y, t: (jnp.maximum(t - 1, 0), 0, y)
    return pl.pallas_call(
        unproject_kernel,
        grid=(2, 3),
        out_shape=(
            jax.ShapeDtypeStruct((3, rows, width), low),
            jax.ShapeDtypeStruct((rows, width), low),
            jax.ShapeDtypeStruct((2, width), f32),
            jax.ShapeDtypeStruct((3, 1, width), f32),
        ),
        in_specs=[
            pl.BlockSpec((rows, half), lambda y, t: (0, y)),
            pl.BlockSpec((1, rows, half), pick), pl.BlockSpec((1, rows, half), pick),
            pl.BlockSpec((1, width, half), lambda y, t: (y, 0, t)),
            whole(rows, 128), whole(1, 128), whole(rows, width), whole(1, width),
            whole(rows, width),
        ],
        out_specs=(
            pl.BlockSpec((1, rows, half), lambda y, t: (t, 0, y)), whole(rows, width),
            whole(2, width), pl.BlockSpec((1, 1, half), lambda y, t: (t, 0, y)),
        ),
        scratch_shapes=[
            pltpu.VMEM((rows, width), f32), pltpu.VMEM((rows, 128), f32),
            pltpu.VMEM((rows, 128), f32),
        ],
        compiler_params=pltpu.CompilerParams(vmem_limit_bytes=VMEM_LIMIT),
        cost_estimate=pl.CostEstimate(
            flops=2 * rows * width * width * 3, bytes_accessed=20000000, transcendentals=0
        ),
        name="unproject",
    )(dq, dkv, got, w, spots, freqs, tok, gain, d_resid)


SLAB = 16


def in_slabs(rows, body):
    def step(i, carry):
        body(pl.ds(pl.multiple_of(i * SLAB, SLAB), SLAB))
        return carry

    lax.fori_loop(0, rows // SLAB, step, 0)


def fold(values):
    return values[:8] + values[8:]


def across(values):
    return jnp.sum(values, axis=-1, keepdims=True)


def down_rows(acc):
    return jnp.sum(acc, axis=0, keepdims=True)


def ffn_kernel(
    hidden, part, att, tok, grad, w_out, w_gu, w_down, gu_bias, in_gain, in_bias, gain2, shift2,
    b_out, b_down, mixed, inner, d_gu, h2, d_resid, g_attn, d_att, wide_sums, thin_sums,
    resid, gate, up, act, acc, d_in, stats, wide_acc, thin_acc,
):
    step = pl.program_id(0)
    rows, width = tok.shape
    wide = in_gain.shape[2]
    half = w_out.shape[2]
    edge = lax.broadcasted_iota(jnp.int32, (SLAB, wide), 1) < part

    def at(n):
        return pl.when(step == n)

    @at(0)
    def _():
        acc[...] = mm(att[:, :half], w_out[0], NT)
        wide_acc[...] = jnp.zeros_like(wide_acc)
        thin_acc[...] = jnp.zeros_like(thin_acc)

    @at(1)
    def _():
        acc[...] += mm(att[:, half:], w_out[0], NT)

        def body(s):
            value = tok[s].astype(f32) + acc[s] + b_out[...]
            resid[s] = value
            normed, _ = normalise(value, width)
            h2[s] = (normed * gain2[...] + shift2[...]).astype(low)

        in_slabs(rows, body)

    for n in range(2):

        @at(2 + 2 * n)
        def _(n=n):
            gate[n] = mm(h2[...], w_gu[0], NN) + gu_bias[0]

        @at(3 + 2 * n)
        def _(n=n):
            up[n] = mm(h2[...], w_gu[0], NN) + gu_bias[0]

            def body(s):
                value = gate[n, s]
                out = value * jax.nn.sigmoid(value) * up[n, s]
                act[n, s] = out
                total = across(out)
                stats[0, s] = total if n == 0 else stats[0, s] + total

            in_slabs(rows, body)

    @at(6)
    def _():
        def body(s):
            centre = stats[0, s] / hidden
            total = 0.0
            moved = []
            for n in range(2):
                shifted = jnp.where(edge, act[n, s] - centre, 0.0)
                moved.append(shifted)
                total = total + across(jnp.square(shifted))
            inverse = lax.rsqrt(total / hidden + epsilon)
            stats[1, s] = inverse
            for n in range(2):
                normed = moved[n] * inverse
                act[n, s] = normed
                inner[n, s] = (normed * in_gain[n] + in_bias[n]).astype(low)

        in_slabs(rows, body)

    for n in range(2):

        @at(6 + n)
        def _(n=n):
            out = mm(inner[n], w_down[0], NT)
            if n == 0:
                acc[...] = out
            else:
                acc[...] += out
            d_in[n] = mm(grad[...], w_down[0], NN)

    @at(7)
    def _():
        def first(s):
            mixed[s] = (resid[s] + acc[s] + b_down[...]).astype(low)
            thin_acc[0] += fold(grad[s].astype(f32))

        in_slabs(rows, first)

        def second(s):
            mean, cross = 0.0, 0.0
            kept = []
            for n in range(2):
                value, normed = d_in[n, s], act[n, s]
                wide_acc[n, 0] += fold(value * normed)
                wide_acc[n, 1] += fold(value)
                scaled = value * in_gain[n]
                mean = mean + across(scaled)
                cross = cross + across(scaled * normed)
            mean, cross = mean / hidden, cross / hidden
            for n in range(2):
                normed, value, other = act[n, s], gate[n, s], up[n, s]
                d_act = stats[1, s] * (d_in[n, s] * in_gain[n] - mean - normed * cross)
                sigma = jax.nn.sigmoid(value)
                d_gate = (d_act * other * sigma * (1.0 + value * (1.0 - sigma))).astype(low)
                d_up = (d_act * value * sigma).astype(low)
                wide_acc[n, 2] += fold(d_gate.astype(f32))
                wide_acc[n, 3] += fold(d_up.astype(f32))
                d_gu[n, s, :wide] = d_gate
                d_gu[n, s, wide:] = d_up

        in_slabs(rows, second)
        for n in range(2):
            for k in range(4):
                wide_sums[n, k : k + 1] = down_rows(wide_acc[n, k])

    for n in range(4):

        @at(8 + n)
        def _(n=n):
            out = mm(d_gu[n // 2, :, (n % 2) * wide : (n % 2 + 1) * wide], w_gu[0], NT)
            if n == 0:
                acc[...] = out
            else:
                acc[...] += out

    @at(11)
    def _():
        def body(s):
            value = acc[s]
            normed, inverse = normalise(resid[s], width)
            thin_acc[1] += fold(value * normed)
            thin_acc[2] += fold(value)
            scaled = value * gain2[...]
            mean, cross = across(scaled) / width, across(scaled * normed) / width
            out = grad[s].astype(f32) + inverse * (scaled - mean - normed * cross)
            d_resid[s] = out
            rounded = out.astype(low)
            g_attn[s] = rounded
            thin_acc[3] += fold(rounded.astype(f32))

        in_slabs(rows, body)
        for k in range(4):
            thin_sums[k : k + 1] = down_rows(thin_acc[k])

    for n in range(2):

        @at(12 + n)
        def _(n=n):
            d_att[:, n * half : (n + 1) * half] = mm(g_attn[...], w_out[0], NN).astype(low)


def ffn(hidden, part, att, tok, grad, w_out, w_gu, w_down, gu_bias, in_gain, in_bias, gain2, shift2, b_out, b_down):
    rows, width = tok.shape
    half, wide = w_out.shape[2], w_down.shape[2]
    whole = lambda *s: pl.BlockSpec(s, lambda i: (0,) * len(s))
    out_at = lambda i: (jnp.where(i < 1, 0, jnp.where(i < 12, 1, jnp.where(i < 13, 0, 1))), 0, 0)

    def gu_at(i):
        n = jnp.where(i < 8, jnp.clip(i - 2, 0, 3), jnp.clip(i - 8, 0, 3))
        return n // 2, n % 2

    sds = jax.ShapeDtypeStruct
    shapes = [
        sds((rows, width), low), sds((2, rows, wide), low), sds((2, rows, 2 * wide), low),
        sds((rows, width), low), sds((rows, width), f32), sds((rows, width), low),
        sds((rows, width), low), sds((2, 4, wide), f32), sds((4, width), f32),
    ]
    return pl.pallas_call(
        functools.partial(ffn_kernel, hidden, part),
        grid=(14,),
        out_shape=shapes,
        in_specs=[
            whole(rows, width), whole(rows, width), whole(rows, width),
            pl.BlockSpec((1, width, half), out_at),
            pl.BlockSpec((1, width, wide), lambda i: (gu_at(i)[0], 0, gu_at(i)[1])),
            pl.BlockSpec((1, width, wide), lambda i: (jnp.where(i < 7, 0, 1), 0, 0)),
            pl.BlockSpec((1, 1, wide), lambda i: (gu_at(i)[0], 0, gu_at(i)[1])),
            whole(2, 1, wide), whole(2, 1, wide), whole(1, width), whole(1, width),
            whole(1, width), whole(1, width),
        ],
        out_specs=[pl.BlockSpec(s.shape, lambda i, k=len(s.shape): (0,) * k, pipeline_mode=pl.Buffered(1)) for s in shapes],
        scratch_shapes=[
            pltpu.VMEM((rows, width), f32), pltpu.VMEM((2, rows, wide), f32),
            pltpu.VMEM((2, rows, wide), f32), pltpu.VMEM((2, rows, wide), f32),
            pltpu.VMEM((rows, width), f32), pltpu.VMEM((2, rows, wide), f32),
            pltpu.VMEM((2, rows, 1), f32), pltpu.VMEM((2, 4, 8, wide), f32),
            pltpu.VMEM((4, 8, width), f32),
        ],
        compiler_params=pltpu.CompilerParams(vmem_limit_bytes=66000000),
        cost_estimate=pl.CostEstimate(flops=20000000000, bytes_accessed=50000000, transcendentals=0),
        name="ffn",
    )(att, tok, grad, w_out, w_gu, w_down, gu_bias, in_gain, in_bias, gain2, shift2, b_out, b_down)


def outer_kernel(left, right, out, flipped):
    @pl.when((pl.program_id(0) == 0) & (pl.program_id(1) == 0))
    def _():
        flipped[...] = left[...].T

    out[0] = mm(flipped[...], right[...] if len(right.shape) == 2 else right[0], NN).astype(low)


def outer(left, right, block, right_spec, total):
    rows, width = left.shape
    return pl.pallas_call(
        outer_kernel,
        grid=(2, total // block),
        out_shape=jax.ShapeDtypeStruct((2, width, total), low),
        in_specs=[pl.BlockSpec((rows, width), lambda y, n: (0, 0)), right_spec],
        out_specs=pl.BlockSpec((1, width, block), lambda y, n: (y, 0, n)),
        scratch_shapes=[pltpu.VMEM((width, rows), low)],
        compiler_params=pltpu.CompilerParams(vmem_limit_bytes=VMEM_LIMIT),
        cost_estimate=pl.CostEstimate(
            flops=4 * rows * width * total, bytes_accessed=4 * width * total, transcendentals=0
        ),
        name="outer",
    )(left, right)


def on_device(
    count, tokens, positions, key_mask, norm1_gain, norm1_bias, qkv_weight, qv_bias, out_weight,
    out_bias, norm2_gain, norm2_bias, gate_up_weight, gate_up_bias, inner_gain, inner_bias,
    down_weight, down_bias, cotangent,
):
    b, x, c, y = (lax.axis_index(a) for a in FAR)
    image = 2 * x + y
    local, images, width = tokens.shape
    shard = qkv_weight.shape[0]
    half = qkv_weight.shape[2]
    part = gate_up_weight.shape[2]
    hidden = gate_up_bias.shape[1]
    wide = -(-part // 128) * 128
    more = wide - part
    rows = 4 * PAD

    shards = [
        qkv_weight.astype(low).reshape(shard, 3 * half),
        out_weight.astype(low).T,
        jnp.pad(gate_up_weight.astype(low), ((0, 0), (0, 0), (0, more))).reshape(shard, 2 * wide),
        jnp.pad(down_weight.astype(low).T, ((0, 0), (0, more))),
    ]
    chunks = jnp.pad(jnp.swapaxes(tokens, 0, 1), ((0, 0), (0, PAD - local), (0, 0)))
    cot = jnp.transpose(cotangent.reshape(2, local, images, width), (2, 0, 1, 3))
    cot = jnp.pad(cot, ((0, 0), (0, 0), (0, PAD - local), (0, 0)))
    spots = jnp.transpose(positions.reshape(2, 2, local, images), (3, 1, 2, 0)).astype(low)
    spots = jnp.pad(spots, ((0, 0), (0, 0), (0, PAD - local), (0, 0)))
    pick = (jnp.arange(128) // 32) % 2
    spots = jnp.where(pick == 0, spots[..., 0:1], spots[..., 1:2])
    *full, tok, spot, cot_in = gather_all(count, shards, chunks, spots, cot)
    w_qkv, w_out, w_gu, w_down = (f.reshape(2, width, f.shape[-1]) for f in full)
    one = lambda a: lax.dynamic_slice_in_dim(a, image, 1, 0)
    tok = lax.dynamic_update_slice_in_dim(tok, one(chunks), image, 0).reshape(rows, width)
    spot = lax.dynamic_update_slice_in_dim(spot, one(spots), x, 0).reshape(rows, 128)
    grad = lax.dynamic_update_slice_in_dim(cot_in, one(cot), x, 0).reshape(rows, width)

    live = lax.dynamic_index_in_dim(key_mask, image, 1, keepdims=False)
    live = jnp.pad(live.reshape(2, 2, 2, local), ((0, 0), (0, 0), (0, 0), (0, PAD - local)))
    live = jnp.stack(
        [lax.dynamic_index_in_dim(live, n, 1, keepdims=False).reshape(rows) for n in (c, 1 - c)]
    )
    bias = jnp.where(live > 0, 0.0, masked_score).astype(f32).reshape(1, 2 * rows)

    freqs = jnp.tile(10000.0 ** (-jnp.arange(16).astype(f32) / 16), 8).reshape(1, 128)
    row = lambda a: a.reshape(1, -1)
    qkv_bias = jnp.stack([qv_bias[0], jnp.zeros_like(qv_bias[0]), qv_bias[1]])[:, None]
    qkv, h1 = project(tok, row(norm1_gain), row(norm1_bias), w_qkv, qkv_bias, spot, freqs)
    swap = ((0, 1), (1, 0))
    far = lax.ppermute(qkv[1:], "core", swap)
    attended, lse = attend(qkv, far, bias)

    split = lambda a: jnp.pad(a.reshape(a.shape[:-1] + (2, part)), ((0, 0),) * a.ndim + ((0, more),))
    gu_bias = jnp.swapaxes(split(gate_up_bias), 0, 1).reshape(2, 1, 2 * wide)
    mixed, inner, d_gu, h2, d_resid, g_attn, d_attended, wide_sums, thin_sums = ffn(
        hidden, part, attended, tok, grad, w_out, w_gu, w_down, gu_bias,
        split(inner_gain)[:, None], split(inner_bias)[:, None], row(norm2_gain), row(norm2_bias),
        row(out_bias), row(down_bias),
    )
    by_owner = lambda a: a.reshape(2, count, 2, 2, shard, a.shape[-1])
    per_half = lambda n: pl.BlockSpec((1, rows, n), lambda y, k: (y, 0, k))
    p_down = by_owner(outer(grad, inner, wide, per_half(wide), wide))
    p_gu = by_owner(outer(h2, d_gu, wide, per_half(wide), 2 * wide))
    flat_half = pl.BlockSpec((rows, half), lambda y, k: (0, y))
    p_out = by_owner(outer(g_attn, attended, half, flat_half, half))

    dq, dkv, dfar = unattend(qkv, far, bias, lse, d_attended)
    got = lax.ppermute(dfar, "core", swap)
    d_proj, d_tok, sums1, col = unproject(
        dq, dkv, got, w_qkv, spot, freqs, tok, row(norm1_gain), d_resid
    )
    per_part = pl.BlockSpec((1, rows, half), lambda y, k: (k, 0, y))
    p_qkv = by_owner(outer(h1, d_proj, half, per_part, 3 * half))
    r_down, r_gu, r_out, r_qkv, mixed_home, d_tok_home = scatter_all(
        count, [p_down, p_gu, p_out, p_qkv], [mixed.reshape(4, PAD, width), d_tok.reshape(4, PAD, width)], 1
    )

    merge = lambda a: a[..., :part].reshape(a.shape[:-2] + (hidden,))
    d_gu_bias = merge(jnp.swapaxes(wide_sums[:, 2:], 0, 1))
    d_in_gain, d_in_bias = wide_sums[:, 0], wide_sums[:, 1]
    d_down_bias, d_gain2, d_bias2, d_out_bias = (thin_sums[n] for n in range(4))
    vectors = [
        sums1[0], sums1[1], jnp.stack([col[0, 0], col[2, 0]]), d_out_bias, d_gain2, d_bias2,
        d_gu_bias, merge(d_in_gain), merge(d_in_bias), d_down_bias,
    ]
    flat = jnp.concatenate([v.reshape(-1) for v in vectors])
    size = flat.shape[0]
    lines = -(-size // 2048) * 16
    summed = sum_all(count, jnp.pad(flat, (0, lines * 128 - size)).reshape(lines, 128), 2)
    summed = summed.reshape(-1)
    pieces, at = [], 0
    for v in vectors:
        pieces.append(summed[at : at + v.size].reshape(v.shape))
        at += v.size

    home = lambda landed: jnp.swapaxes(landed[:, :local], 0, 1)

    return (
        home(mixed_home), home(d_tok_home), pieces[0], pieces[1], r_qkv.reshape(shard, 3, half), pieces[2],
        r_out.T, pieces[3], pieces[4], pieces[5], r_gu.reshape(shard, 2, wide)[:, :, :part],
        pieces[6], pieces[7], pieces[8], r_down[:, :part].T, pieces[9],
    )


def solution(mesh):
    count, ctx, tensor = (mesh.shape[a] for a in ("batch", "ctx", "tensor"))
    fine = jax.sharding.Mesh(mesh.devices.reshape(count, ctx // 2, 2, tensor), FAR)
    ctx, wide = ("x", "core"), ("batch", "x", "core")
    return jax.shard_map(
        functools.partial(on_device, count),
        mesh=fine,
        in_specs=(
            P(("x", "core", "tensor"), "batch", None), P(None, ctx, "batch"), P(None, "batch"),
            P(), P(), P(wide, None, "tensor"), P(), P("tensor", wide), P(), P(), P(),
            P(wide, None, "tensor"), P(), P(), P(), P("tensor", wide), P(), P(ctx, "batch", None),
        ),
        out_specs=(
            P(("x", "core", "tensor"), "batch", None), P(("x", "core", "tensor"), "batch", None),
            P(), P(), P(wide, None, "tensor"), P(), P("tensor", wide), P(), P(), P(),
            P(wide, None, "tensor"), P(), P(), P(), P("tensor", wide), P(),
        ),
        check_vma=False,
    )
```

```python
import functools

import jax
import jax.numpy as jnp
from jax import lax
from jax.experimental import pallas as pl
from jax.experimental.pallas import tpu as pltpu

from jax.sharding import PartitionSpec as P
MESH = pl.DeviceIdType.MESH
FAR = ("batch", "x", "core", "tensor")


def place(b, x, c, y):
    return {"batch": b, "x": x, "core": c, "tensor": y}


def ring_offsets(count):
    order = [0]
    for step in range(1, count // 2 + 1):
        for off in (step, count - step):
            if off not in order:
                order.append(off)
    return order


def greet(count, corner=False):
    b, x, c, y = (lax.axis_index(a) for a in FAR)
    barrier = pltpu.get_barrier_semaphore()
    for off in range(1, count):
        pl.semaphore_signal(
            barrier, inc=1, device_id=place(lax.rem(b + off, count), x, c, y), device_id_type=MESH
        )
    near = [place(b, 1 - x, c, y), place(b, x, c, 1 - y), place(b, x, 1 - c, y)]
    if corner:
        near.append(place(b, 1 - x, c, 1 - y))
    for there in near:
        pl.semaphore_signal(barrier, inc=1, device_id=there, device_id_type=MESH)
    pl.semaphore_wait(barrier, count - 1 + len(near))


def push(src, dst, s, r, there):
    pltpu.make_async_remote_copy(
        src_ref=src, dst_ref=dst, send_sem=s, recv_sem=r, device_id=there, device_id_type=MESH
    ).start()


def arrived(dst, sem):
    pltpu.make_async_copy(dst, dst, sem).wait()


def gather_sems(count, groups):
    dma = pltpu.SemaphoreType.DMA
    many, one = dma((groups, count)), dma((groups,))
    return [one, many, one, many, one, many, one, one, many, one, one, one]


def gather_job(count, own, full, sems):
    groups = len(own)
    zs, zr, xs, xr, ys, yr, xds, yds, dr, cs, cr, ls = sems
    b, x, c, y = (lax.axis_index(a) for a in FAR)
    xn, yn, cn = place(b, 1 - x, c, y), place(b, x, c, 1 - y), place(b, x, 1 - c, y)
    offsets = ring_offsets(count)

    def block(g, yy, item, xx, cc):
        return full[g].at[yy, lax.rem(b + offsets[item], count), xx, cc]

    def begin():
        for g in range(groups):
            for j in range(1, count):
                there = place(lax.rem(b + count - offsets[j], count), x, c, y)
                push(own[g], full[g].at[y, b, x, c], zs.at[g], zr.at[g, j], there)
            pltpu.make_async_copy(own[g], full[g].at[y, b, x, c], ls.at[g]).start()

    def column(g, j):
        dst = block(g, y, j, x, c)
        if j > 0:
            arrived(dst, zr.at[g, j])
        src = own[g] if j == 0 else dst
        push(src, dst, xs.at[g], xr.at[g, j], xn)
        push(src, dst, ys.at[g], yr.at[g, j], yn)
        push(src, dst, cs.at[g], cr.at[g], cn)

    def plane(g, j):
        from_x, from_y = block(g, y, j, 1 - x, c), block(g, 1 - y, j, x, c)
        arrived(from_x, xr.at[g, j])
        if j % 2 == 0:
            push(from_x, from_x, yds.at[g], dr.at[g, j], yn)
        push(from_x, from_x, cs.at[g], cr.at[g], cn)
        arrived(from_y, yr.at[g, j])
        if j % 2 == 1:
            push(from_y, from_y, xds.at[g], dr.at[g, j], xn)
        push(from_y, from_y, cs.at[g], cr.at[g], cn)

    def corner(g, j):
        there = block(g, 1 - y, j, 1 - x, c)
        arrived(there, dr.at[g, j])
        push(there, there, cs.at[g], cr.at[g], cn)

    items = [(g, j) for g in range(groups) for j in range(count)]

    def stage(t):
        if t < len(items):
            column(*items[t])
        if 1 <= t <= len(items):
            plane(*items[t - 1])
        if t >= 2:
            corner(*items[t - 2])

    def end():
        for g in range(groups):
            pltpu.make_async_copy(own[g], full[g].at[y, b, x, c], ls.at[g]).wait()
            arrived(full[g].at[:, :, :, 1 - c], cr.at[g])
            arrived(full[g].at[:, :, :, 0], cs.at[g])
            arrived(full[g].at[0, : count - 1, 0, 0], zs.at[g])
            arrived(full[g].at[0, :, 0, 0], xs.at[g])
            arrived(full[g].at[0, :, 0, 0], ys.at[g])
            arrived(full[g].at[0, : count // 2, 0, 0], xds.at[g])
            arrived(full[g].at[0, : (count + 1) // 2, 0, 0], yds.at[g])

    return begin, [functools.partial(stage, t) for t in range(len(items) + 2)], end


def full_shapes(count, shards):
    return [jax.ShapeDtypeStruct((2, count, 2, 2) + s.shape, s.dtype) for s in shards]


def gather_kernel(count, groups, *refs):
    own = refs[:groups]
    tokens, spots, cot = refs[groups : groups + 3]
    full = refs[groups + 3 : 2 * groups + 3]
    landed = refs[2 * groups + 3 : 2 * groups + 6]
    *sems, ts, tr, tl = refs[2 * groups + 6 :]
    b, x, c, y = (lax.axis_index(a) for a in FAR)
    begin, steps, end = gather_job(count, own, full, sems)
    image = 2 * x + y
    far = 2 * (1 - x) + y
    corners = ((1, 0), (0, 1), (1, 1))
    greet(count, corner=True)
    for n, (ox, oy) in enumerate(corners):
        px, py = (1 - x if ox else x), (1 - y if oy else y)
        push(
            tokens.at[2 * px + py], landed[0].at[image], ts.at[n], tr.at[n], place(b, px, c, py)
        )
    begin()
    xn = place(b, 1 - x, c, y)
    push(spots.at[far], landed[1].at[x], ts.at[3], tr.at[3], xn)
    for step in steps:
        step()
    push(cot.at[far], landed[2].at[x], ts.at[4], tr.at[4], xn)
    homes = [
        pltpu.make_async_copy(tokens.at[image], landed[0].at[image], tl.at[0]),
        pltpu.make_async_copy(spots.at[image], landed[1].at[x], tl.at[1]),
        pltpu.make_async_copy(cot.at[image], landed[2].at[x], tl.at[2]),
    ]
    for copy in homes:
        copy.start()
    end()
    for n, (ox, oy) in enumerate(corners):
        px, py = (1 - x if ox else x), (1 - y if oy else y)
        arrived(landed[0].at[2 * px + py], tr.at[n])
        arrived(tokens.at[0], ts.at[n])
    arrived(landed[1].at[1 - x], tr.at[3])
    arrived(spots.at[0], ts.at[3])
    arrived(landed[2].at[1 - x], tr.at[4])
    arrived(cot.at[0], ts.at[4])
    for copy in homes:
        copy.wait()


def gather_first(count, shards, tokens, spots, cot):
    groups = len(shards)
    any_spec = pl.BlockSpec(memory_space=pl.ANY)
    dma = pltpu.SemaphoreType.DMA
    outs = full_shapes(count, shards) + [
        jax.ShapeDtypeStruct(tokens.shape, tokens.dtype),
        jax.ShapeDtypeStruct((2,) + spots.shape[1:], spots.dtype),
        jax.ShapeDtypeStruct((2,) + cot.shape[1:], cot.dtype),
    ]
    return pl.pallas_call(
        functools.partial(gather_kernel, count, groups),
        out_shape=outs,
        in_specs=[any_spec] * (groups + 3),
        out_specs=[any_spec] * len(outs),
        scratch_shapes=gather_sems(count, groups) + [dma((5,)), dma((5,)), dma((3,))],
        compiler_params=pltpu.CompilerParams(collective_id=0, has_side_effects=True),
        name="gather_first",
    )(*shards, tokens, spots, cot)


def scatter_kernel(count, groups, moves, *refs):
    parts = refs[:groups]
    leaving = refs[groups : groups + moves]
    outs = refs[groups + moves : 2 * groups + moves]
    landed = refs[2 * groups + moves : 2 * groups + 2 * moves]
    at = 2 * groups + 2 * moves
    held, peer, from_x, from_y, from_d, from_z = (
        refs[at + k * groups : at + (k + 1) * groups] for k in range(6)
    )
    ls, cs, cr, xs, xr, ys, yr, xds, yds, dr, zs, zr, ts, tr, tl = refs[at + 6 * groups :]
    b, x, c, y = (lax.axis_index(a) for a in FAR)
    xn, yn, cn = place(b, 1 - x, c, y), place(b, x, c, 1 - y), place(b, x, 1 - c, y)
    offsets = ring_offsets(count)
    order = list(range(1, count)) + [0]
    rows = held[0].shape[3]
    chunk = min(rows, 16)
    image = 2 * x + y
    corners = ((1, 0), (0, 1), (1, 1))
    greet(count, corner=moves > 0)

    def add_to(target, *others):
        def body(i, carry):
            at_rows = pl.ds(pl.multiple_of(i * chunk, chunk), chunk)
            total = target[at_rows].astype(jnp.float32)
            for other in others:
                total = total + other[at_rows].astype(jnp.float32)
            target[at_rows] = total.astype(target.dtype)
            return carry

        lax.fori_loop(0, rows // chunk, body, 0)

    def where_to(j):
        return lax.rem(b + offsets[j], count)

    items = [(g, j) for g in range(groups) for j in order]
    for g, j in items:
        bb = where_to(j)
        push(parts[g].at[:, bb, :, 1 - c], peer[g].at[:, bb], cs.at[g], cr.at[g, j], cn)
        pltpu.make_async_copy(parts[g].at[:, bb, :, c], held[g].at[:, bb], ls.at[g, j]).start()

    for m in range(moves):
        pltpu.make_async_copy(leaving[m].at[image], landed[m].at[image], tl.at[m]).start()
        for n, (ox, oy) in enumerate(corners):
            px, py = (1 - x if ox else x), (1 - y if oy else y)
            push(
                leaving[m].at[2 * px + py], landed[m].at[image], ts.at[m, n], tr.at[m, n],
                place(b, px, c, py),
            )

    def merge_core(g, j):
        bb = where_to(j)
        arrived(held[g].at[:, bb], ls.at[g, j])
        arrived(peer[g].at[:, bb], cr.at[g, j])
        for yy, xx in ((1 - y, 1 - x), (y, 1 - x), (1 - y, x), (y, x)):
            add_to(held[g].at[yy, bb, xx], peer[g].at[yy, bb, xx])

    def send_corner(g, j):
        src = held[g].at[1 - y, where_to(j), 1 - x]
        if j % 2 == 0:
            push(src, from_d[g].at[j], xds.at[g], dr.at[g, j], xn)
        else:
            push(src, from_d[g].at[j], yds.at[g], dr.at[g, j], yn)

    def merge_corner(g, j):
        bb = where_to(j)
        arrived(from_d[g].at[j], dr.at[g, j])
        if j % 2 == 0:
            add_to(held[g].at[1 - y, bb, x], from_d[g].at[j])
        else:
            add_to(held[g].at[y, bb, 1 - x], from_d[g].at[j])

    def send_plane(g, j):
        bb = where_to(j)
        push(held[g].at[y, bb, 1 - x], from_x[g].at[j], xs.at[g], xr.at[g, j], xn)
        push(held[g].at[1 - y, bb, x], from_y[g].at[j], ys.at[g], yr.at[g, j], yn)

    def merge_plane(g, j):
        arrived(from_x[g].at[j], xr.at[g, j])
        arrived(from_y[g].at[j], yr.at[g, j])
        add_to(held[g].at[y, where_to(j), x], from_x[g].at[j], from_y[g].at[j])

    def send_column(g, j):
        if j > 0:
            bb = where_to(j)
            push(
                held[g].at[y, bb, x], from_z[g].at[j], zs.at[g], zr.at[g, j], place(bb, x, c, y)
            )

    total = len(items)
    for t in range(total + 2):
        now = items[t] if t < total else None
        one = items[t - 1] if 1 <= t <= total else None
        two = items[t - 2] if 2 <= t else None
        if two:
            merge_plane(*two)
        if one:
            merge_corner(*one)
        if now:
            merge_core(*now)
            send_corner(*now)
        if one:
            send_plane(*one)
        if two:
            send_column(*two)
    for g in range(groups):
        for j in range(1, count):
            arrived(from_z[g].at[j], zr.at[g, j])

        def body(i, carry, g=g):
            at_rows = pl.ds(pl.multiple_of(i * chunk, chunk), chunk)
            result = held[g][y, b, x, at_rows].astype(jnp.float32)
            for j in range(1, count):
                result = result + from_z[g][j, at_rows].astype(jnp.float32)
            outs[g][at_rows] = result
            return carry

        lax.fori_loop(0, rows // chunk, body, 0)
        arrived(peer[g], cs.at[g])
        arrived(from_x[g], xs.at[g])
        arrived(from_y[g], ys.at[g])
        arrived(from_d[g].at[: (count + 1) // 2], xds.at[g])
        arrived(from_d[g].at[: count // 2], yds.at[g])
        arrived(from_z[g].at[1:], zs.at[g])
    for m in range(moves):
        pltpu.make_async_copy(leaving[m].at[image], landed[m].at[image], tl.at[m]).wait()
        for n, (ox, oy) in enumerate(corners):
            px, py = (1 - x if ox else x), (1 - y if oy else y)
            arrived(landed[m].at[2 * px + py], tr.at[m, n])
            arrived(leaving[m].at[0], ts.at[m, n])


def scatter_all(count, parts, leaving, number):
    groups, moves = len(parts), len(leaving)
    dma = pltpu.SemaphoreType.DMA
    shapes = [p.shape[4:] for p in parts]
    low = jnp.bfloat16
    scratch = [pltpu.VMEM((2, count, 2) + s, low) for s in shapes] * 2
    scratch += [pltpu.VMEM((count,) + s, low) for s in shapes] * 4
    many, one = dma((groups, count)), dma((groups,))
    scratch += [many, one, many, one, many, one, many, one, one, many, one, many]
    scratch += [dma((max(moves, 1), 3)), dma((max(moves, 1), 3)), dma((max(moves, 1),))]
    return pl.pallas_call(
        functools.partial(scatter_kernel, count, groups, moves),
        out_shape=[jax.ShapeDtypeStruct(s, jnp.float32) for s in shapes]
        + [jax.ShapeDtypeStruct(a.shape, a.dtype) for a in leaving],
        in_specs=[pl.BlockSpec(memory_space=pl.ANY)] * (groups + moves),
        out_specs=[pl.BlockSpec(memory_space=pltpu.VMEM)] * groups
        + [pl.BlockSpec(memory_space=pl.ANY)] * moves,
        scratch_shapes=scratch,
        compiler_params=pltpu.CompilerParams(
            collective_id=number, has_side_effects=True, vmem_limit_bytes=64000000
        ),
        name="scatter_all",
    )(*parts, *leaving)


def sum_kernel(count, v_ref, o_ref, got, lane, plane, slots, ss, rs, zs, zr):
    b, x, c, y = (lax.axis_index(a) for a in FAR)
    xn, yn, cn = place(b, 1 - x, c, y), place(b, x, c, 1 - y), place(b, x, 1 - c, y)
    half = v_ref.shape[0] // 2
    mine = pl.ds(pl.multiple_of(c * half, 8), half)
    theirs = pl.ds(pl.multiple_of((1 - c) * half, 8), half)
    greet(count)

    def swap(src, dst, n, there):
        copy = pltpu.make_async_remote_copy(
            src_ref=src, dst_ref=dst, send_sem=ss.at[n], recv_sem=rs.at[n], device_id=there,
            device_id_type=MESH,
        )
        copy.start()
        copy.wait()

    swap(v_ref.at[theirs], got.at[0], 0, cn)
    lane[...] = v_ref[mine] + got[0]
    swap(lane, got.at[1], 1, xn)
    plane[...] = lane[...] + got[1]
    swap(plane, got.at[2], 2, yn)
    slots[b] = plane[...] + got[2]
    for off in range(1, count):
        pltpu.make_async_remote_copy(
            src_ref=slots.at[b], dst_ref=slots.at[b], send_sem=zs, recv_sem=zr.at[off],
            device_id=place(lax.rem(b + off, count), x, c, y), device_id_type=MESH,
        ).start()
    for off in range(1, count):
        there = slots.at[lax.rem(b + count - off, count)]
        pltpu.make_async_copy(there, there, zr.at[off]).wait()
    total = slots[0]
    for n in range(1, count):
        total = total + slots[n]
    o_ref[mine] = total
    swap(o_ref.at[mine], o_ref.at[mine], 3, cn)
    rest = slots.at[: count - 1]
    pltpu.make_async_copy(rest, rest, zs).wait()


def sum_all(count, vector, number):
    rows = vector.shape[0]
    half = (rows // 2, 128)
    dma = pltpu.SemaphoreType.DMA
    vm = pltpu.VMEM
    return pl.pallas_call(
        functools.partial(sum_kernel, count),
        out_shape=jax.ShapeDtypeStruct(vector.shape, jnp.float32),
        in_specs=[pl.BlockSpec(memory_space=pltpu.VMEM)],
        out_specs=pl.BlockSpec(memory_space=pltpu.VMEM),
        scratch_shapes=[
            vm((3,) + half, jnp.float32), vm(half, jnp.float32), vm(half, jnp.float32),
            vm((count,) + half, jnp.float32), dma((4,)), dma((4,)), dma(()), dma((count,)),
        ],
        compiler_params=pltpu.CompilerParams(collective_id=number, has_side_effects=True),
        name="sum_all",
    )(vector)

PAD = 136
WIDTH_TILE = 128
HEAD_DIM = 64
epsilon = 1e-06
masked_score = -1e30
f32, low = jnp.float32, jnp.bfloat16
VMEM_LIMIT = 60000000


def mm(a, b, dims):
    return lax.dot_general(a, b, (dims, ((), ())), preferred_element_type=f32)


NN = ((1,), (0,))
NT = ((1,), (1,))
TN = ((0,), (0,))


def normalise(values, width):
    centre = jnp.sum(values, axis=-1, keepdims=True) / width
    shifted = values - centre
    spread = jnp.sum(jnp.square(shifted), axis=-1, keepdims=True) / width
    inverse = lax.rsqrt(spread + epsilon)
    return shifted * inverse, inverse


def turn(values, cosine, sine):
    lane = lax.broadcasted_iota(jnp.int32, values.shape, 1)
    other = jnp.where((lane // 16) % 2 == 0, pltpu.roll(values, 112, 1), pltpu.roll(values, 16, 1))
    return values * cosine + other * sine


def tables(spots, freqs):
    angles = spots.astype(f32) * freqs
    lane = lax.broadcasted_iota(jnp.int32, angles.shape, 1)
    sine = jnp.sin(angles)
    return jnp.cos(angles), jnp.where((lane // 16) % 2 == 0, -sine, sine)


def head_lanes(rows):
    return lax.broadcasted_iota(jnp.int32, (rows, 128), 1) // HEAD_DIM


def forward_kernel(count, groups, pairs, *refs):
    tok, gain, shift, w, w_bias, spots, freqs, mask = refs[:8]
    own = refs[8 : 8 + groups]
    out, h1, att, lse, far_out = refs[8 + groups : 13 + groups]
    full = refs[13 + groups : 13 + 2 * groups]
    hid, cos, sin, kept, far, keys, vals, ks, kr, fs = refs[13 + 2 * groups : 23 + 2 * groups]
    begin, steps, end = gather_job(count, own, full, refs[23 + 2 * groups :])
    step = pl.program_id(0)
    rows = tok.shape[0]
    half = w.shape[2]
    b, x, c, y = (lax.axis_index(a) for a in FAR)
    cn = place(b, x, 1 - c, y)
    total = 6 + pairs

    def kv(n):
        t, side = n % 2, n // 2
        return t, slice(side * half, (side + 1) * half)

    @pl.when(step == 0)
    def _():
        greet(count)
        begin()
        normed, _ = normalise(tok[...].astype(f32), tok.shape[1])
        hid[...] = (normed * gain[...] + shift[...]).astype(low)
        h1[...] = hid[...]
        lse[...] = jnp.zeros_like(lse)
        cosine, sine = tables(spots[...], freqs[...])
        cos[...] = cosine
        sin[...] = sine

    for s in range(total):
        todo = steps[s * len(steps) // total : (s + 1) * len(steps) // total]
        done = s - 1
        sent = 2 * (done // 3) + done % 3 - 1 if 0 <= done < 6 and done % 3 > 0 else None

        @pl.when(step == s)
        def _(s=s, todo=todo, sent=sent):
            if sent is not None:
                t, lanes = kv(sent)
                push(kept.at[1 + t, :, lanes], far.at[t, :, lanes], ks.at[sent], kr.at[sent], cn)
            for one in todo:
                one()
            if s in (6, 6 + pairs // 2):
                for n in range(2) if s == 6 else range(2, 4):
                    t, lanes = kv(n)
                    arrived(far.at[t, :, lanes], kr.at[n])
            if s == total - 1:
                pltpu.make_async_copy(far, far_out, fs).start()

    for n in range(6):

        @pl.when(step == n)
        def _(n=n):
            t, lanes = n % 3, slice((n // 3) * half, (n // 3 + 1) * half)
            acc = mm(hid[...], w[0], NN) + w_bias[0]
            if t < 2:
                parts = [
                    turn(acc[:, k : k + 128], cos[...], sin[...]).astype(low)
                    for k in range(0, half, 128)
                ]
                result = jnp.concatenate(parts, axis=1)
            else:
                result = acc.astype(low)
            out[0] = result
            kept[t, :, lanes] = result

    @pl.when(step >= 6)
    def _():
        pair = step - 6
        mine_lanes = pl.ds(pl.multiple_of(pair * 128, 128), 128)
        keys[:rows], keys[rows:] = kept[1, :, mine_lanes], far[0, :, mine_lanes]
        vals[:rows], vals[rows:] = kept[2, :, mine_lanes], far[1, :, mine_lanes]
        chunk = rows // 2
        lanes = head_lanes(chunk)
        spot = lax.broadcasted_iota(jnp.int32, (chunk, 128), 1)
        for n in range(rows // chunk):
            here = slice(n * chunk, (n + 1) * chunk)
            query = kept[0, here, mine_lanes] * low(HEAD_DIM**-0.5)
            result = None
            marks = lse[here]
            for h in range(2):
                mine = jnp.where(lanes == h, query, low(0))
                scores = mm(mine, keys[...], NT) + mask[...]
                top = jnp.max(scores, axis=-1, keepdims=True)
                weight = jnp.exp(scores - top)
                sums = jnp.sum(weight, axis=-1, keepdims=True)
                probs = (weight * (1.0 / sums)).astype(low)
                got = mm(probs, vals[...], NN)
                result = got if h == 0 else jnp.where(lanes == 0, result, got)
                marks = jnp.where(spot == 2 * pair + h, top + jnp.log(sums), marks)
            lse[here] = marks
            att[here] = result.astype(low)

    @pl.when(step == total - 1)
    def _():
        end()
        for n in range(4):
            t, lanes = kv(n)
            arrived(kept.at[1 + t, :, lanes], ks.at[n])
        pltpu.make_async_copy(far, far_out, fs).wait()


def forward(count, tok, gain, shift, w, bias, spots, freqs, mask, shards):
    rows, width = tok.shape
    half = w.shape[2] // 3
    groups, pairs = len(shards), width // 128
    whole = lambda *s: pl.BlockSpec(s, lambda i: (0,) * len(s))
    at = lambda i: jnp.minimum(i, 5)
    any_spec = pl.BlockSpec(memory_space=pl.ANY)
    sds, vm, dma = jax.ShapeDtypeStruct, pltpu.VMEM, pltpu.SemaphoreType.DMA
    return pl.pallas_call(
        functools.partial(forward_kernel, count, groups, pairs),
        grid=(6 + pairs,),
        out_shape=[
            sds((3, rows, width), low), sds((rows, width), low), sds((rows, width), low),
            sds((rows, 128), f32), sds((2, rows, width), low),
        ]
        + full_shapes(count, shards),
        in_specs=[
            whole(rows, width), whole(1, width), whole(1, width),
            pl.BlockSpec((1, width, half), lambda i: (at(i) // 3, 0, at(i) % 3)),
            pl.BlockSpec((1, 1, half), lambda i: (at(i) % 3, 0, at(i) // 3)),
            whole(rows, 128), whole(1, 128), whole(1, 2 * rows),
        ]
        + [any_spec] * groups,
        out_specs=[
            pl.BlockSpec((1, rows, half), lambda i: (at(i) % 3, 0, at(i) // 3)),
            whole(rows, width),
            pl.BlockSpec((rows, 128), lambda i: (0, jnp.maximum(i - 6, 0))),
            whole(rows, 128), any_spec,
        ]
        + [any_spec] * groups,
        scratch_shapes=[
            vm((rows, width), low), vm((rows, 128), f32), vm((rows, 128), f32),
            vm((3, rows, width), low), vm((2, rows, width), low), vm((2 * rows, 128), low),
            vm((2 * rows, 128), low), dma((4,)), dma((4,)), dma(()),
        ]
        + gather_sems(count, groups),
        compiler_params=pltpu.CompilerParams(
            vmem_limit_bytes=VMEM_LIMIT, collective_id=3, has_side_effects=True
        ),
        name="forward",
    )(tok, gain, shift, w, bias, spots, freqs, mask, *shards)


def unattend_kernel(q, k, v, kp, vp, bias, lse, grad, dq, dkv, dfar, keys, vals, dk, dv, *, chunk):
    pair = pl.program_id(0)
    rows = q.shape[1]
    keys[:rows], keys[rows:] = k[0], kp[0]
    vals[:rows], vals[rows:] = v[0], vp[0]
    lanes = head_lanes(chunk)
    spot = lax.broadcasted_iota(jnp.int32, (chunk, 128), 1)
    for n in range(rows // chunk):
        here = slice(n * chunk, (n + 1) * chunk)
        query = q[0, here] * low(HEAD_DIM**-0.5)
        out_grad = grad[here]
        result = None
        for h in range(2):
            mine = jnp.where(lanes == h, query, low(0))
            mine_grad = jnp.where(lanes == h, out_grad, low(0))
            shift = jnp.sum(jnp.where(spot == 2 * pair + h, lse[here], 0.0), axis=-1, keepdims=True)
            probs = jnp.exp(mm(mine, keys[...], NT) + bias[...] - shift)
            d_probs = mm(mine_grad, vals[...], NT)
            both = probs * d_probs
            inner = jnp.sum(both, axis=-1, keepdims=True)
            d_scores = (both - probs * inner).astype(low)
            got = mm(d_scores, keys[...], NN)
            result = got if h == 0 else jnp.where(lanes == 0, result, got)
            key_part = mm(d_scores, mine, TN)
            value_part = mm(probs.astype(low), mine_grad, TN)
            if n == 0 and h == 0:
                dk[...], dv[...] = key_part, value_part
            else:
                dk[...] += key_part
                dv[...] += value_part
        dq[here] = result * HEAD_DIM**-0.5
    dkv[0], dkv[1] = dk[:rows], dv[:rows]
    dfar[0], dfar[1] = dk[rows:].astype(low), dv[rows:].astype(low)


def unattend(qkv, far, bias, lse, grad):
    _, rows, width = qkv.shape
    keys = 2 * rows
    at = lambda t: pl.BlockSpec((1, rows, 128), lambda g: (t, 0, g))
    both = pl.BlockSpec((2, rows, 128), lambda g: (0, 0, g))
    column = pl.BlockSpec((rows, 128), lambda g: (0, g))
    return pl.pallas_call(
        functools.partial(unattend_kernel, chunk=rows // 2),
        grid=(width // 128,),
        out_shape=(
            jax.ShapeDtypeStruct((rows, width), f32),
            jax.ShapeDtypeStruct((2, rows, width), f32),
            jax.ShapeDtypeStruct((2, rows, width), low),
        ),
        in_specs=[
            at(0), at(1), at(2), at(0), at(1), pl.BlockSpec((1, keys), lambda g: (0, 0)),
            pl.BlockSpec((rows, 128), lambda g: (0, 0)), column,
        ],
        out_specs=(column, both, both),
        scratch_shapes=[pltpu.VMEM((keys, 128), low)] * 2 + [pltpu.VMEM((keys, 128), f32)] * 2,
        compiler_params=pltpu.CompilerParams(vmem_limit_bytes=VMEM_LIMIT),
        cost_estimate=pl.CostEstimate(
            flops=40 * rows * keys * width, bytes_accessed=20000000, transcendentals=0
        ),
        name="unattend",
    )(qkv, qkv, qkv, far, far, bias, lse, grad)


def unproject_kernel(
    dq, dkv, got, w, spots, freqs, tok, gain, d_resid, d_proj, d_tok, sums, col, acc, cos, sin
):
    y, t = pl.program_id(0), pl.program_id(1)
    first = (y == 0) & (t == 0)

    @pl.when(first)
    def _():
        cosine, sine = tables(spots[...], freqs[...])
        cos[...] = cosine
        sin[...] = -sine

    def put(value):
        rounded = value.astype(low)
        d_proj[0] = rounded
        return rounded

    def turned(value):
        parts = [
            turn(value[:, n * 128 : (n + 1) * 128], cos[...], sin[...])
            for n in range(value.shape[1] // 128)
        ]
        return jnp.concatenate(parts, axis=1)

    @pl.when(t == 0)
    def _():
        put(turned(dq[...]))

    @pl.when(t == 1)
    def _():
        put(turned(dkv[0] + got[0].astype(f32)))

    @pl.when(t == 2)
    def _():
        put(dkv[0] + got[0].astype(f32))

    rounded = d_proj[0]
    col[0] = jnp.sum(rounded.astype(f32), axis=0, keepdims=True)
    part = mm(rounded, w[0], NT)

    @pl.when(first)
    def _():
        acc[...] = part

    @pl.when(jnp.logical_not(first))
    def _():
        acc[...] += part

    @pl.when((y == 1) & (t == 2))
    def _():
        width = tok.shape[1]
        normed, inverse = normalise(tok[...].astype(f32), width)
        up = acc[...]
        sums[0:1] = jnp.sum(up * normed, axis=0, keepdims=True)
        sums[1:2] = jnp.sum(up, axis=0, keepdims=True)
        scaled = up * gain[...]
        mean = jnp.sum(scaled, axis=-1, keepdims=True) / width
        cross = jnp.sum(scaled * normed, axis=-1, keepdims=True) / width
        d_tok[...] = (d_resid[...] + inverse * (scaled - mean - normed * cross)).astype(low)


def unproject(dq, dkv, got, w, spots, freqs, tok, gain, d_resid):
    rows, width = tok.shape
    half = w.shape[2] // 3
    whole = lambda *s: pl.BlockSpec(s, lambda y, t: (0,) * len(s))
    pick = lambda y, t: (jnp.maximum(t - 1, 0), 0, y)
    return pl.pallas_call(
        unproject_kernel,
        grid=(2, 3),
        out_shape=(
            jax.ShapeDtypeStruct((3, rows, width), low),
            jax.ShapeDtypeStruct((rows, width), low),
            jax.ShapeDtypeStruct((2, width), f32),
            jax.ShapeDtypeStruct((3, 1, width), f32),
        ),
        in_specs=[
            pl.BlockSpec((rows, half), lambda y, t: (0, y)),
            pl.BlockSpec((1, rows, half), pick), pl.BlockSpec((1, rows, half), pick),
            pl.BlockSpec((1, width, half), lambda y, t: (y, 0, t)),
            whole(rows, 128), whole(1, 128), whole(rows, width), whole(1, width),
            whole(rows, width),
        ],
        out_specs=(
            pl.BlockSpec((1, rows, half), lambda y, t: (t, 0, y)), whole(rows, width),
            whole(2, width), pl.BlockSpec((1, 1, half), lambda y, t: (t, 0, y)),
        ),
        scratch_shapes=[
            pltpu.VMEM((rows, width), f32), pltpu.VMEM((rows, 128), f32),
            pltpu.VMEM((rows, 128), f32),
        ],
        compiler_params=pltpu.CompilerParams(vmem_limit_bytes=VMEM_LIMIT),
        cost_estimate=pl.CostEstimate(
            flops=2 * rows * width * width * 3, bytes_accessed=20000000, transcendentals=0
        ),
        name="unproject",
    )(dq, dkv, got, w, spots, freqs, tok, gain, d_resid)


SLAB = 16


def in_slabs(rows, body):
    def step(i, carry):
        body(pl.ds(pl.multiple_of(i * SLAB, SLAB), SLAB))
        return carry

    lax.fori_loop(0, rows // SLAB, step, 0)


def fold(values):
    return values[:8] + values[8:]


def across(values):
    return jnp.sum(values, axis=-1, keepdims=True)


def down_rows(acc):
    return jnp.sum(acc, axis=0, keepdims=True)


def ffn_kernel(
    hidden, part, att, tok, grad, w_out, w_gu, w_down, gu_bias, in_gain, in_bias, gain2, shift2,
    b_out, b_down, mixed, inner, d_gu, h2, d_resid, g_attn, d_att, wide_sums, thin_sums,
    resid, gate, up, act, acc, d_in, stats, wide_acc, thin_acc,
):
    step = pl.program_id(0)
    rows, width = tok.shape
    wide = in_gain.shape[2]
    half = w_out.shape[2]
    edge = lax.broadcasted_iota(jnp.int32, (SLAB, wide), 1) < part

    def at(n):
        return pl.when(step == n)

    @at(0)
    def _():
        acc[...] = mm(att[:, :half], w_out[0], NT)
        wide_acc[...] = jnp.zeros_like(wide_acc)
        thin_acc[...] = jnp.zeros_like(thin_acc)

    @at(1)
    def _():
        acc[...] += mm(att[:, half:], w_out[0], NT)

        def body(s):
            value = tok[s].astype(f32) + acc[s] + b_out[...]
            resid[s] = value
            normed, _ = normalise(value, width)
            h2[s] = (normed * gain2[...] + shift2[...]).astype(low)

        in_slabs(rows, body)

    for n in range(2):

        @at(2 + 2 * n)
        def _(n=n):
            gate[n] = mm(h2[...], w_gu[0], NN) + gu_bias[0]

        @at(3 + 2 * n)
        def _(n=n):
            up[n] = mm(h2[...], w_gu[0], NN) + gu_bias[0]

            def body(s):
                value = gate[n, s]
                out = value * jax.nn.sigmoid(value) * up[n, s]
                act[n, s] = out
                total = across(out)
                stats[0, s] = total if n == 0 else stats[0, s] + total

            in_slabs(rows, body)

    @at(6)
    def _():
        def body(s):
            centre = stats[0, s] / hidden
            total = 0.0
            moved = []
            for n in range(2):
                shifted = jnp.where(edge, act[n, s] - centre, 0.0)
                moved.append(shifted)
                total = total + across(jnp.square(shifted))
            inverse = lax.rsqrt(total / hidden + epsilon)
            stats[1, s] = inverse
            for n in range(2):
                normed = moved[n] * inverse
                act[n, s] = normed
                inner[n, s] = (normed * in_gain[n] + in_bias[n]).astype(low)

        in_slabs(rows, body)

    for n in range(2):

        @at(6 + n)
        def _(n=n):
            out = mm(inner[n], w_down[0], NT)
            if n == 0:
                acc[...] = out
            else:
                acc[...] += out
            d_in[n] = mm(grad[...], w_down[0], NN)

    @at(7)
    def _():
        def first(s):
            mixed[s] = (resid[s] + acc[s] + b_down[...]).astype(low)
            thin_acc[0] += fold(grad[s].astype(f32))

        in_slabs(rows, first)

        def second(s):
            mean, cross = 0.0, 0.0
            kept = []
            for n in range(2):
                value, normed = d_in[n, s], act[n, s]
                wide_acc[n, 0] += fold(value * normed)
                wide_acc[n, 1] += fold(value)
                scaled = value * in_gain[n]
                mean = mean + across(scaled)
                cross = cross + across(scaled * normed)
            mean, cross = mean / hidden, cross / hidden
            for n in range(2):
                normed, value, other = act[n, s], gate[n, s], up[n, s]
                d_act = stats[1, s] * (d_in[n, s] * in_gain[n] - mean - normed * cross)
                sigma = jax.nn.sigmoid(value)
                d_gate = (d_act * other * sigma * (1.0 + value * (1.0 - sigma))).astype(low)
                d_up = (d_act * value * sigma).astype(low)
                wide_acc[n, 2] += fold(d_gate.astype(f32))
                wide_acc[n, 3] += fold(d_up.astype(f32))
                d_gu[n, s, :wide] = d_gate
                d_gu[n, s, wide:] = d_up

        in_slabs(rows, second)
        for n in range(2):
            for k in range(4):
                wide_sums[n, k : k + 1] = down_rows(wide_acc[n, k])

    for n in range(4):

        @at(8 + n)
        def _(n=n):
            out = mm(d_gu[n // 2, :, (n % 2) * wide : (n % 2 + 1) * wide], w_gu[0], NT)
            if n == 0:
                acc[...] = out
            else:
                acc[...] += out

    @at(11)
    def _():
        def body(s):
            value = acc[s]
            normed, inverse = normalise(resid[s], width)
            thin_acc[1] += fold(value * normed)
            thin_acc[2] += fold(value)
            scaled = value * gain2[...]
            mean, cross = across(scaled) / width, across(scaled * normed) / width
            out = grad[s].astype(f32) + inverse * (scaled - mean - normed * cross)
            d_resid[s] = out
            rounded = out.astype(low)
            g_attn[s] = rounded
            thin_acc[3] += fold(rounded.astype(f32))

        in_slabs(rows, body)
        for k in range(4):
            thin_sums[k : k + 1] = down_rows(thin_acc[k])

    for n in range(2):

        @at(12 + n)
        def _(n=n):
            d_att[:, n * half : (n + 1) * half] = mm(g_attn[...], w_out[0], NN).astype(low)


def ffn(hidden, part, att, tok, grad, w_out, w_gu, w_down, gu_bias, in_gain, in_bias, gain2, shift2, b_out, b_down):
    rows, width = tok.shape
    half, wide = w_out.shape[2], w_down.shape[2]
    whole = lambda *s: pl.BlockSpec(s, lambda i: (0,) * len(s))
    out_at = lambda i: (jnp.where(i < 1, 0, jnp.where(i < 12, 1, jnp.where(i < 13, 0, 1))), 0, 0)

    def gu_at(i):
        n = jnp.where(i < 8, jnp.clip(i - 2, 0, 3), jnp.clip(i - 8, 0, 3))
        return n // 2, n % 2

    sds = jax.ShapeDtypeStruct
    shapes = [
        sds((rows, width), low), sds((2, rows, wide), low), sds((2, rows, 2 * wide), low),
        sds((rows, width), low), sds((rows, width), f32), sds((rows, width), low),
        sds((rows, width), low), sds((2, 4, wide), f32), sds((4, width), f32),
    ]
    return pl.pallas_call(
        functools.partial(ffn_kernel, hidden, part),
        grid=(14,),
        out_shape=shapes,
        in_specs=[
            whole(rows, width), whole(rows, width), whole(rows, width),
            pl.BlockSpec((1, width, half), out_at),
            pl.BlockSpec((1, width, wide), lambda i: (gu_at(i)[0], 0, gu_at(i)[1])),
            pl.BlockSpec((1, width, wide), lambda i: (jnp.where(i < 7, 0, 1), 0, 0)),
            pl.BlockSpec((1, 1, wide), lambda i: (gu_at(i)[0], 0, gu_at(i)[1])),
            whole(2, 1, wide), whole(2, 1, wide), whole(1, width), whole(1, width),
            whole(1, width), whole(1, width),
        ],
        out_specs=[pl.BlockSpec(s.shape, lambda i, k=len(s.shape): (0,) * k, pipeline_mode=pl.Buffered(1)) for s in shapes],
        scratch_shapes=[
            pltpu.VMEM((rows, width), f32), pltpu.VMEM((2, rows, wide), f32),
            pltpu.VMEM((2, rows, wide), f32), pltpu.VMEM((2, rows, wide), f32),
            pltpu.VMEM((rows, width), f32), pltpu.VMEM((2, rows, wide), f32),
            pltpu.VMEM((2, rows, 1), f32), pltpu.VMEM((2, 4, 8, wide), f32),
            pltpu.VMEM((4, 8, width), f32),
        ],
        compiler_params=pltpu.CompilerParams(vmem_limit_bytes=66000000),
        cost_estimate=pl.CostEstimate(flops=20000000000, bytes_accessed=50000000, transcendentals=0),
        name="ffn",
    )(att, tok, grad, w_out, w_gu, w_down, gu_bias, in_gain, in_bias, gain2, shift2, b_out, b_down)


def outer_kernel(left, right, out, flipped):
    @pl.when((pl.program_id(0) == 0) & (pl.program_id(1) == 0))
    def _():
        flipped[...] = left[...].T

    out[0] = mm(flipped[...], right[...] if len(right.shape) == 2 else right[0], NN).astype(low)


def outer(left, right, block, right_spec, total):
    rows, width = left.shape
    return pl.pallas_call(
        outer_kernel,
        grid=(2, total // block),
        out_shape=jax.ShapeDtypeStruct((2, width, total), low),
        in_specs=[pl.BlockSpec((rows, width), lambda y, n: (0, 0)), right_spec],
        out_specs=pl.BlockSpec((1, width, block), lambda y, n: (y, 0, n)),
        scratch_shapes=[pltpu.VMEM((width, rows), low)],
        compiler_params=pltpu.CompilerParams(vmem_limit_bytes=VMEM_LIMIT),
        cost_estimate=pl.CostEstimate(
            flops=4 * rows * width * total, bytes_accessed=4 * width * total, transcendentals=0
        ),
        name="outer",
    )(left, right)


def on_device(
    count, tokens, positions, key_mask, norm1_gain, norm1_bias, qkv_weight, qv_bias, out_weight,
    out_bias, norm2_gain, norm2_bias, gate_up_weight, gate_up_bias, inner_gain, inner_bias,
    down_weight, down_bias, cotangent,
):
    b, x, c, y = (lax.axis_index(a) for a in FAR)
    image = 2 * x + y
    local, images, width = tokens.shape
    shard = qkv_weight.shape[0]
    half = qkv_weight.shape[2]
    part = gate_up_weight.shape[2]
    hidden = gate_up_bias.shape[1]
    wide = -(-part // 128) * 128
    more = wide - part
    rows = 4 * PAD

    shards = [
        qkv_weight.astype(low).reshape(shard, 3 * half),
        out_weight.astype(low).T,
        jnp.pad(gate_up_weight.astype(low), ((0, 0), (0, 0), (0, more))).reshape(shard, 2 * wide),
        jnp.pad(down_weight.astype(low).T, ((0, 0), (0, more))),
    ]
    chunks = jnp.pad(jnp.swapaxes(tokens, 0, 1), ((0, 0), (0, PAD - local), (0, 0)))
    cot = jnp.transpose(cotangent.reshape(2, local, images, width), (2, 0, 1, 3))
    cot = jnp.pad(cot, ((0, 0), (0, 0), (0, PAD - local), (0, 0)))
    spots = jnp.transpose(positions.reshape(2, 2, local, images), (3, 1, 2, 0)).astype(low)
    spots = jnp.pad(spots, ((0, 0), (0, 0), (0, PAD - local), (0, 0)))
    pick = (jnp.arange(128) // 32) % 2
    spots = jnp.where(pick == 0, spots[..., 0:1], spots[..., 1:2])
    join = lambda f: f.reshape(2, width, f.shape[-1])
    w_qkv, tok, spot, grad = gather_first(count, shards[:1], chunks, spots, cot)
    w_qkv = join(w_qkv)
    tok, spot, grad = tok.reshape(rows, width), spot.reshape(rows, 128), grad.reshape(rows, width)

    live = lax.dynamic_index_in_dim(key_mask, image, 1, keepdims=False)
    live = jnp.pad(live.reshape(2, 2, 2, local), ((0, 0), (0, 0), (0, 0), (0, PAD - local)))
    live = jnp.stack(
        [lax.dynamic_index_in_dim(live, n, 1, keepdims=False).reshape(rows) for n in (c, 1 - c)]
    )
    bias = jnp.where(live > 0, 0.0, masked_score).astype(f32).reshape(1, 2 * rows)

    freqs = jnp.tile(10000.0 ** (-jnp.arange(16).astype(f32) / 16), 8).reshape(1, 128)
    row = lambda a: a.reshape(1, -1)
    qkv_bias = jnp.stack([qv_bias[0], jnp.zeros_like(qv_bias[0]), qv_bias[1]])[:, None]
    swap = ((0, 1), (1, 0))
    qkv, h1, attended, lse, far, *full = forward(
        count, tok, row(norm1_gain), row(norm1_bias), w_qkv, qkv_bias, spot, freqs, bias, shards[1:]
    )
    w_out, w_gu, w_down = (join(f) for f in full)

    split = lambda a: jnp.pad(a.reshape(a.shape[:-1] + (2, part)), ((0, 0),) * a.ndim + ((0, more),))
    gu_bias = jnp.swapaxes(split(gate_up_bias), 0, 1).reshape(2, 1, 2 * wide)
    mixed, inner, d_gu, h2, d_resid, g_attn, d_attended, wide_sums, thin_sums = ffn(
        hidden, part, attended, tok, grad, w_out, w_gu, w_down, gu_bias,
        split(inner_gain)[:, None], split(inner_bias)[:, None], row(norm2_gain), row(norm2_bias),
        row(out_bias), row(down_bias),
    )
    by_owner = lambda a: a.reshape(2, count, 2, 2, shard, a.shape[-1])
    per_half = lambda n: pl.BlockSpec((1, rows, n), lambda y, k: (y, 0, k))
    p_down = by_owner(outer(grad, inner, wide, per_half(wide), wide))
    p_gu = by_owner(outer(h2, d_gu, wide, per_half(wide), 2 * wide))
    flat_half = pl.BlockSpec((rows, half), lambda y, k: (0, y))
    p_out = by_owner(outer(g_attn, attended, half, flat_half, half))

    dq, dkv, dfar = unattend(qkv, far, bias, lse, d_attended)
    got = lax.ppermute(dfar, "core", swap)
    d_proj, d_tok, sums1, col = unproject(
        dq, dkv, got, w_qkv, spot, freqs, tok, row(norm1_gain), d_resid
    )
    per_part = pl.BlockSpec((1, rows, half), lambda y, k: (k, 0, y))
    p_qkv = by_owner(outer(h1, d_proj, half, per_part, 3 * half))
    r_down, r_gu, r_out, r_qkv, mixed_home, d_tok_home = scatter_all(
        count, [p_down, p_gu, p_out, p_qkv], [mixed.reshape(4, PAD, width), d_tok.reshape(4, PAD, width)], 1
    )

    merge = lambda a: a[..., :part].reshape(a.shape[:-2] + (hidden,))
    d_gu_bias = merge(jnp.swapaxes(wide_sums[:, 2:], 0, 1))
    d_in_gain, d_in_bias = wide_sums[:, 0], wide_sums[:, 1]
    d_down_bias, d_gain2, d_bias2, d_out_bias = (thin_sums[n] for n in range(4))
    vectors = [
        sums1[0], sums1[1], jnp.stack([col[0, 0], col[2, 0]]), d_out_bias, d_gain2, d_bias2,
        d_gu_bias, merge(d_in_gain), merge(d_in_bias), d_down_bias,
    ]
    flat = jnp.concatenate([v.reshape(-1) for v in vectors])
    size = flat.shape[0]
    lines = -(-size // 2048) * 16
    summed = sum_all(count, jnp.pad(flat, (0, lines * 128 - size)).reshape(lines, 128), 2)
    summed = summed.reshape(-1)
    pieces, at = [], 0
    for v in vectors:
        pieces.append(summed[at : at + v.size].reshape(v.shape))
        at += v.size

    home = lambda landed: jnp.swapaxes(landed[:, :local], 0, 1)

    return (
        home(mixed_home), home(d_tok_home), pieces[0], pieces[1], r_qkv.reshape(shard, 3, half), pieces[2],
        r_out.T, pieces[3], pieces[4], pieces[5], r_gu.reshape(shard, 2, wide)[:, :, :part],
        pieces[6], pieces[7], pieces[8], r_down[:, :part].T, pieces[9],
    )


def solution(mesh):
    count, ctx, tensor = (mesh.shape[a] for a in ("batch", "ctx", "tensor"))
    fine = jax.sharding.Mesh(mesh.devices.reshape(count, ctx // 2, 2, tensor), FAR)
    ctx, wide = ("x", "core"), ("batch", "x", "core")
    return jax.shard_map(
        functools.partial(on_device, count),
        mesh=fine,
        in_specs=(
            P(("x", "core", "tensor"), "batch", None), P(None, ctx, "batch"), P(None, "batch"),
            P(), P(), P(wide, None, "tensor"), P(), P("tensor", wide), P(), P(), P(),
            P(wide, None, "tensor"), P(), P(), P(), P("tensor", wide), P(), P(ctx, "batch", None),
        ),
        out_specs=(
            P(("x", "core", "tensor"), "batch", None), P(("x", "core", "tensor"), "batch", None),
            P(), P(), P(wide, None, "tensor"), P(), P("tensor", wide), P(), P(), P(),
            P(wide, None, "tensor"), P(), P(), P(), P("tensor", wide), P(),
        ),
        check_vma=False,
    )
```

```python
import functools

import jax
import jax.numpy as jnp
from jax import lax
from jax.experimental import pallas as pl
from jax.experimental.pallas import tpu as pltpu

from jax.sharding import PartitionSpec as P
MESH = pl.DeviceIdType.MESH
FAR = ("batch", "x", "core", "tensor")


def place(b, x, c, y):
    return {"batch": b, "x": x, "core": c, "tensor": y}


def ring_offsets(count):
    order = [0]
    for step in range(1, count // 2 + 1):
        for off in (step, count - step):
            if off not in order:
                order.append(off)
    return order


def greet(count, corner=False):
    b, x, c, y = (lax.axis_index(a) for a in FAR)
    barrier = pltpu.get_barrier_semaphore()
    for off in range(1, count):
        pl.semaphore_signal(
            barrier, inc=1, device_id=place(lax.rem(b + off, count), x, c, y), device_id_type=MESH
        )
    near = [place(b, 1 - x, c, y), place(b, x, c, 1 - y), place(b, x, 1 - c, y)]
    if corner:
        near.append(place(b, 1 - x, c, 1 - y))
    for there in near:
        pl.semaphore_signal(barrier, inc=1, device_id=there, device_id_type=MESH)
    pl.semaphore_wait(barrier, count - 1 + len(near))


def push(src, dst, s, r, there):
    pltpu.make_async_remote_copy(
        src_ref=src, dst_ref=dst, send_sem=s, recv_sem=r, device_id=there, device_id_type=MESH
    ).start()


def arrived(dst, sem):
    pltpu.make_async_copy(dst, dst, sem).wait()


def gather_sems(count, groups):
    dma = pltpu.SemaphoreType.DMA
    many, one = dma((groups, count)), dma((groups,))
    return [one, many, one, many, one, many, one, one, many, one, one, one]


def gather_job(count, own, full, sems):
    groups = len(own)
    zs, zr, xs, xr, ys, yr, xds, yds, dr, cs, cr, ls = sems
    b, x, c, y = (lax.axis_index(a) for a in FAR)
    xn, yn, cn = place(b, 1 - x, c, y), place(b, x, c, 1 - y), place(b, x, 1 - c, y)
    offsets = ring_offsets(count)

    def block(g, yy, item, xx, cc):
        return full[g].at[yy, lax.rem(b + offsets[item], count), xx, cc]

    def begin():
        for g in range(groups):
            for j in range(1, count):
                there = place(lax.rem(b + count - offsets[j], count), x, c, y)
                push(own[g], full[g].at[y, b, x, c], zs.at[g], zr.at[g, j], there)
            pltpu.make_async_copy(own[g], full[g].at[y, b, x, c], ls.at[g]).start()

    def column(g, j):
        dst = block(g, y, j, x, c)
        if j > 0:
            arrived(dst, zr.at[g, j])
        src = own[g] if j == 0 else dst
        push(src, dst, xs.at[g], xr.at[g, j], xn)
        push(src, dst, ys.at[g], yr.at[g, j], yn)
        push(src, dst, cs.at[g], cr.at[g], cn)

    def plane(g, j):
        from_x, from_y = block(g, y, j, 1 - x, c), block(g, 1 - y, j, x, c)
        arrived(from_x, xr.at[g, j])
        if j % 2 == 0:
            push(from_x, from_x, yds.at[g], dr.at[g, j], yn)
        push(from_x, from_x, cs.at[g], cr.at[g], cn)
        arrived(from_y, yr.at[g, j])
        if j % 2 == 1:
            push(from_y, from_y, xds.at[g], dr.at[g, j], xn)
        push(from_y, from_y, cs.at[g], cr.at[g], cn)

    def corner(g, j):
        there = block(g, 1 - y, j, 1 - x, c)
        arrived(there, dr.at[g, j])
        push(there, there, cs.at[g], cr.at[g], cn)

    items = [(g, j) for g in range(groups) for j in range(count)]

    def stage(t):
        if t < len(items):
            column(*items[t])
        if 1 <= t <= len(items):
            plane(*items[t - 1])
        if t >= 2:
            corner(*items[t - 2])

    def end():
        for g in range(groups):
            pltpu.make_async_copy(own[g], full[g].at[y, b, x, c], ls.at[g]).wait()
            arrived(full[g].at[:, :, :, 1 - c], cr.at[g])
            arrived(full[g].at[:, :, :, 0], cs.at[g])
            arrived(full[g].at[0, : count - 1, 0, 0], zs.at[g])
            arrived(full[g].at[0, :, 0, 0], xs.at[g])
            arrived(full[g].at[0, :, 0, 0], ys.at[g])
            arrived(full[g].at[0, : count // 2, 0, 0], xds.at[g])
            arrived(full[g].at[0, : (count + 1) // 2, 0, 0], yds.at[g])

    return begin, [functools.partial(stage, t) for t in range(len(items) + 2)], end


def full_shapes(count, shards):
    return [jax.ShapeDtypeStruct((2, count, 2, 2) + s.shape, s.dtype) for s in shards]


def gather_kernel(count, groups, *refs):
    own = refs[:groups]
    tokens, spots, cot = refs[groups : groups + 3]
    full = refs[groups + 3 : 2 * groups + 3]
    landed = refs[2 * groups + 3 : 2 * groups + 6]
    *sems, ts, tr, tl = refs[2 * groups + 6 :]
    b, x, c, y = (lax.axis_index(a) for a in FAR)
    begin, steps, end = gather_job(count, own, full, sems)
    image = 2 * x + y
    far = 2 * (1 - x) + y
    corners = ((1, 0), (0, 1), (1, 1))
    greet(count, corner=True)
    for n, (ox, oy) in enumerate(corners):
        px, py = (1 - x if ox else x), (1 - y if oy else y)
        push(
            tokens.at[2 * px + py], landed[0].at[image], ts.at[n], tr.at[n], place(b, px, c, py)
        )
    begin()
    xn = place(b, 1 - x, c, y)
    push(spots.at[far], landed[1].at[x], ts.at[3], tr.at[3], xn)
    for step in steps:
        step()
    push(cot.at[far], landed[2].at[x], ts.at[4], tr.at[4], xn)
    homes = [
        pltpu.make_async_copy(tokens.at[image], landed[0].at[image], tl.at[0]),
        pltpu.make_async_copy(spots.at[image], landed[1].at[x], tl.at[1]),
        pltpu.make_async_copy(cot.at[image], landed[2].at[x], tl.at[2]),
    ]
    for copy in homes:
        copy.start()
    end()
    for n, (ox, oy) in enumerate(corners):
        px, py = (1 - x if ox else x), (1 - y if oy else y)
        arrived(landed[0].at[2 * px + py], tr.at[n])
        arrived(tokens.at[0], ts.at[n])
    arrived(landed[1].at[1 - x], tr.at[3])
    arrived(spots.at[0], ts.at[3])
    arrived(landed[2].at[1 - x], tr.at[4])
    arrived(cot.at[0], ts.at[4])
    for copy in homes:
        copy.wait()


def gather_first(count, shards, tokens, spots, cot):
    groups = len(shards)
    any_spec = pl.BlockSpec(memory_space=pl.ANY)
    dma = pltpu.SemaphoreType.DMA
    outs = full_shapes(count, shards) + [
        jax.ShapeDtypeStruct(tokens.shape, tokens.dtype),
        jax.ShapeDtypeStruct((2,) + spots.shape[1:], spots.dtype),
        jax.ShapeDtypeStruct((2,) + cot.shape[1:], cot.dtype),
    ]
    return pl.pallas_call(
        functools.partial(gather_kernel, count, groups),
        out_shape=outs,
        in_specs=[any_spec] * (groups + 3),
        out_specs=[any_spec] * len(outs),
        scratch_shapes=gather_sems(count, groups) + [dma((5,)), dma((5,)), dma((3,))],
        compiler_params=pltpu.CompilerParams(collective_id=0, has_side_effects=True),
        name="gather_first",
    )(*shards, tokens, spots, cot)


def scatter_scratch(count, shapes):
    groups = len(shapes)
    dma = pltpu.SemaphoreType.DMA
    scratch = [pltpu.VMEM((2, count, 2) + s, jnp.bfloat16) for s in shapes] * 2
    scratch += [pltpu.VMEM((count,) + s, jnp.bfloat16) for s in shapes] * 4
    many, one = dma((groups, count)), dma((groups,))
    return scratch + [many, one, many, one, many, one, many, one, one, many, one, many]


def scatter_job(count, parts, outs, scratch):
    groups = len(parts)
    held, peer, from_x, from_y, from_d, from_z = (
        scratch[k * groups : (k + 1) * groups] for k in range(6)
    )
    ls, cs, cr, xs, xr, ys, yr, xds, yds, dr, zs, zr = scratch[6 * groups :]
    b, x, c, y = (lax.axis_index(a) for a in FAR)
    xn, yn, cn = place(b, 1 - x, c, y), place(b, x, c, 1 - y), place(b, x, 1 - c, y)
    offsets = ring_offsets(count)
    order = list(range(1, count)) + [0]
    rows = held[0].shape[3]
    chunk = min(rows, 16)

    def add_to(target, *others):
        def body(i, carry):
            at_rows = pl.ds(pl.multiple_of(i * chunk, chunk), chunk)
            total = target[at_rows].astype(jnp.float32)
            for other in others:
                total = total + other[at_rows].astype(jnp.float32)
            target[at_rows] = total.astype(target.dtype)
            return carry

        lax.fori_loop(0, rows // chunk, body, 0)

    def where_to(j):
        return lax.rem(b + offsets[j], count)

    items = [(g, j) for g in range(groups) for j in order]

    def begin():
        for g, j in items:
            bb = where_to(j)
            push(parts[g].at[:, bb, :, 1 - c], peer[g].at[:, bb], cs.at[g], cr.at[g, j], cn)
            pltpu.make_async_copy(
                parts[g].at[:, bb, :, c], held[g].at[:, bb], ls.at[g, j]
            ).start()

    def merge_core(g, j):
        bb = where_to(j)
        arrived(held[g].at[:, bb], ls.at[g, j])
        arrived(peer[g].at[:, bb], cr.at[g, j])
        for yy, xx in ((1 - y, 1 - x), (y, 1 - x), (1 - y, x), (y, x)):
            add_to(held[g].at[yy, bb, xx], peer[g].at[yy, bb, xx])

    def send_corner(g, j):
        src = held[g].at[1 - y, where_to(j), 1 - x]
        if j % 2 == 0:
            push(src, from_d[g].at[j], xds.at[g], dr.at[g, j], xn)
        else:
            push(src, from_d[g].at[j], yds.at[g], dr.at[g, j], yn)

    def merge_corner(g, j):
        bb = where_to(j)
        arrived(from_d[g].at[j], dr.at[g, j])
        if j % 2 == 0:
            add_to(held[g].at[1 - y, bb, x], from_d[g].at[j])
        else:
            add_to(held[g].at[y, bb, 1 - x], from_d[g].at[j])

    def send_plane(g, j):
        bb = where_to(j)
        push(held[g].at[y, bb, 1 - x], from_x[g].at[j], xs.at[g], xr.at[g, j], xn)
        push(held[g].at[1 - y, bb, x], from_y[g].at[j], ys.at[g], yr.at[g, j], yn)

    def merge_plane(g, j):
        arrived(from_x[g].at[j], xr.at[g, j])
        arrived(from_y[g].at[j], yr.at[g, j])
        add_to(held[g].at[y, where_to(j), x], from_x[g].at[j], from_y[g].at[j])

    def send_column(g, j):
        if j > 0:
            bb = where_to(j)
            push(
                held[g].at[y, bb, x], from_z[g].at[j], zs.at[g], zr.at[g, j], place(bb, x, c, y)
            )

    total = len(items)

    def stage(t):
        now = items[t] if t < total else None
        one = items[t - 1] if 1 <= t <= total else None
        two = items[t - 2] if 2 <= t else None
        if two:
            merge_plane(*two)
        if one:
            merge_corner(*one)
        if now:
            merge_core(*now)
            send_corner(*now)
        if one:
            send_plane(*one)
        if two:
            send_column(*two)

    def end():
        for g in range(groups):
            for j in range(1, count):
                arrived(from_z[g].at[j], zr.at[g, j])

            def body(i, carry, g=g):
                at_rows = pl.ds(pl.multiple_of(i * chunk, chunk), chunk)
                result = held[g][y, b, x, at_rows].astype(jnp.float32)
                for j in range(1, count):
                    result = result + from_z[g][j, at_rows].astype(jnp.float32)
                outs[g][at_rows] = result
                return carry

            lax.fori_loop(0, rows // chunk, body, 0)
            arrived(peer[g], cs.at[g])
            arrived(from_x[g], xs.at[g])
            arrived(from_y[g], ys.at[g])
            arrived(from_d[g].at[: (count + 1) // 2], xds.at[g])
            arrived(from_d[g].at[: count // 2], yds.at[g])
            arrived(from_z[g].at[1:], zs.at[g])

    return begin, [functools.partial(stage, t) for t in range(total + 2)], end


CORNERS = ((1, 0), (0, 1), (1, 1))


def deliver_job(leaving, landed, ts, tr, tl):
    b, x, c, y = (lax.axis_index(a) for a in FAR)
    image = 2 * x + y

    def begin():
        pltpu.make_async_copy(leaving.at[image], landed.at[image], tl).start()
        for n, (ox, oy) in enumerate(CORNERS):
            px, py = (1 - x if ox else x), (1 - y if oy else y)
            there = place(b, px, c, py)
            push(leaving.at[2 * px + py], landed.at[image], ts.at[n], tr.at[n], there)

    def end():
        pltpu.make_async_copy(leaving.at[image], landed.at[image], tl).wait()
        for n, (ox, oy) in enumerate(CORNERS):
            px, py = (1 - x if ox else x), (1 - y if oy else y)
            arrived(landed.at[2 * px + py], tr.at[n])
            arrived(leaving.at[0], ts.at[n])

    return begin, end


def deliver_sems():
    dma = pltpu.SemaphoreType.DMA
    return [dma((3,)), dma((3,)), dma(())]


def share(todo, step, total):
    return todo[step * len(todo) // total : (step + 1) * len(todo) // total]


def sum_scratch(count, rows):
    half = (rows // 2, 128)
    dma, vm = pltpu.SemaphoreType.DMA, pltpu.VMEM
    return [
        vm((3,) + half, jnp.float32), vm(half, jnp.float32), vm(half, jnp.float32),
        vm((count,) + half, jnp.float32), dma((4,)), dma((4,)), dma(()), dma((count,)),
    ]


def sum_job(count, v_ref, o_ref, scratch):
    got, lane, plane, slots, ss, rs, zs, zr = scratch
    b, x, c, y = (lax.axis_index(a) for a in FAR)
    xn, yn, cn = place(b, 1 - x, c, y), place(b, x, c, 1 - y), place(b, x, 1 - c, y)
    half = v_ref.shape[0] // 2
    mine = pl.ds(pl.multiple_of(c * half, 8), half)
    theirs = pl.ds(pl.multiple_of((1 - c) * half, 8), half)

    def swap(src, dst, n, there):
        return pltpu.make_async_remote_copy(
            src_ref=src, dst_ref=dst, send_sem=ss.at[n], recv_sem=rs.at[n], device_id=there,
            device_id_type=MESH,
        )

    swaps = (
        lambda: swap(v_ref.at[theirs], got.at[0], 0, cn),
        lambda: swap(lane, got.at[1], 1, xn),
        lambda: swap(plane, got.at[2], 2, yn),
        lambda: swap(o_ref.at[mine], o_ref.at[mine], 3, cn),
    )

    def one():
        swaps[0]().start()

    def two():
        swaps[0]().wait()
        lane[...] = v_ref[mine] + got[0]
        swaps[1]().start()

    def three():
        swaps[1]().wait()
        plane[...] = lane[...] + got[1]
        swaps[2]().start()

    def four():
        swaps[2]().wait()
        slots[b] = plane[...] + got[2]
        for off in range(1, count):
            pltpu.make_async_remote_copy(
                src_ref=slots.at[b], dst_ref=slots.at[b], send_sem=zs, recv_sem=zr.at[off],
                device_id=place(lax.rem(b + off, count), x, c, y), device_id_type=MESH,
            ).start()

    def five():
        for off in range(1, count):
            there = slots.at[lax.rem(b + count - off, count)]
            pltpu.make_async_copy(there, there, zr.at[off]).wait()
        total = slots[0]
        for n in range(1, count):
            total = total + slots[n]
        o_ref[mine] = total
        swaps[3]().start()

    def six():
        swaps[3]().wait()
        rest = slots.at[: count - 1]
        pltpu.make_async_copy(rest, rest, zs).wait()

    return [one, two, three, four, five, six]


def last_kernel(count, p_qkv, vector, r_qkv, summed, *scratch):
    sums = sum_scratch(count, vector.shape[0])
    parts = [p_qkv.at[n] for n in range(3)]
    outs = [r_qkv.at[n] for n in range(3)]
    begin, steps, end = scatter_job(count, parts, outs, scratch[: -len(sums)])
    adds = sum_job(count, vector, summed, scratch[-len(sums) :])
    greet(count)
    begin()
    for n, step in enumerate(steps):
        step()
        for add in share(adds, n, len(steps)):
            add()
    end()


def last(count, p_qkv, vector, number):
    shapes = [p_qkv.shape[5:]] * 3
    vmem = pl.BlockSpec(memory_space=pltpu.VMEM)
    return pl.pallas_call(
        functools.partial(last_kernel, count),
        out_shape=[
            jax.ShapeDtypeStruct((3,) + shapes[0], jnp.float32),
            jax.ShapeDtypeStruct(vector.shape, jnp.float32),
        ],
        in_specs=[pl.BlockSpec(memory_space=pl.ANY), vmem],
        out_specs=[vmem, vmem],
        scratch_shapes=scatter_scratch(count, shapes) + sum_scratch(count, vector.shape[0]),
        compiler_params=pltpu.CompilerParams(
            collective_id=number, has_side_effects=True, vmem_limit_bytes=VMEM_LIMIT
        ),
        name="last",
    )(p_qkv, vector)


PAD = 136
WIDTH_TILE = 128
HEAD_DIM = 64
epsilon = 1e-06
masked_score = -1e30
f32, low = jnp.float32, jnp.bfloat16
VMEM_LIMIT = 60000000


def mm(a, b, dims):
    return lax.dot_general(a, b, (dims, ((), ())), preferred_element_type=f32)


NN = ((1,), (0,))
NT = ((1,), (1,))
TN = ((0,), (0,))


def normalise(values, width):
    centre = jnp.sum(values, axis=-1, keepdims=True) / width
    shifted = values - centre
    spread = jnp.sum(jnp.square(shifted), axis=-1, keepdims=True) / width
    inverse = lax.rsqrt(spread + epsilon)
    return shifted * inverse, inverse


def turn(values, cosine, sine):
    lane = lax.broadcasted_iota(jnp.int32, values.shape, 1)
    other = jnp.where((lane // 16) % 2 == 0, pltpu.roll(values, 112, 1), pltpu.roll(values, 16, 1))
    return values * cosine + other * sine


def tables(spots, freqs):
    angles = spots.astype(f32) * freqs
    lane = lax.broadcasted_iota(jnp.int32, angles.shape, 1)
    sine = jnp.sin(angles)
    return jnp.cos(angles), jnp.where((lane // 16) % 2 == 0, -sine, sine)


def head_lanes(rows):
    return lax.broadcasted_iota(jnp.int32, (rows, 128), 1) // HEAD_DIM


def forward_kernel(count, groups, pairs, *refs):
    tok, gain, shift, w, w_bias, spots, freqs, mask = refs[:8]
    own = refs[8 : 8 + groups]
    out, h1, att, lse, far_out = refs[8 + groups : 13 + groups]
    full = refs[13 + groups : 13 + 2 * groups]
    hid, cos, sin, kept, far, keys, vals, ks, kr, fs = refs[13 + 2 * groups : 23 + 2 * groups]
    begin, steps, end = gather_job(count, own, full, refs[23 + 2 * groups :])
    step = pl.program_id(0)
    rows = tok.shape[0]
    half = w.shape[2]
    b, x, c, y = (lax.axis_index(a) for a in FAR)
    cn = place(b, x, 1 - c, y)
    total = 6 + pairs

    def kv(n):
        t, side = n % 2, n // 2
        return t, slice(side * half, (side + 1) * half)

    @pl.when(step == 0)
    def _():
        greet(count)
        begin()
        normed, _ = normalise(tok[...].astype(f32), tok.shape[1])
        hid[...] = (normed * gain[...] + shift[...]).astype(low)
        h1[...] = hid[...]
        lse[...] = jnp.zeros_like(lse)
        cosine, sine = tables(spots[...], freqs[...])
        cos[...] = cosine
        sin[...] = sine

    for s in range(total):
        todo = steps[s * len(steps) // total : (s + 1) * len(steps) // total]
        done = s - 1
        sent = 2 * (done // 3) + done % 3 - 1 if 0 <= done < 6 and done % 3 > 0 else None

        @pl.when(step == s)
        def _(s=s, todo=todo, sent=sent):
            if sent is not None:
                t, lanes = kv(sent)
                push(kept.at[1 + t, :, lanes], far.at[t, :, lanes], ks.at[sent], kr.at[sent], cn)
            for one in todo:
                one()
            if s in (6, 6 + pairs // 2):
                for n in range(2) if s == 6 else range(2, 4):
                    t, lanes = kv(n)
                    arrived(far.at[t, :, lanes], kr.at[n])
            if s == total - 1:
                pltpu.make_async_copy(far, far_out, fs).start()

    for n in range(6):

        @pl.when(step == n)
        def _(n=n):
            t, lanes = n % 3, slice((n // 3) * half, (n // 3 + 1) * half)
            acc = mm(hid[...], w[0], NN) + w_bias[0]
            if t < 2:
                parts = [
                    turn(acc[:, k : k + 128], cos[...], sin[...]).astype(low)
                    for k in range(0, half, 128)
                ]
                result = jnp.concatenate(parts, axis=1)
            else:
                result = acc.astype(low)
            out[0] = result
            kept[t, :, lanes] = result

    @pl.when(step >= 6)
    def _():
        pair = step - 6
        mine_lanes = pl.ds(pl.multiple_of(pair * 128, 128), 128)
        keys[:rows], keys[rows:] = kept[1, :, mine_lanes], far[0, :, mine_lanes]
        vals[:rows], vals[rows:] = kept[2, :, mine_lanes], far[1, :, mine_lanes]
        chunk = rows // 2
        lanes = head_lanes(chunk)
        spot = lax.broadcasted_iota(jnp.int32, (chunk, 128), 1)
        for n in range(rows // chunk):
            here = slice(n * chunk, (n + 1) * chunk)
            query = kept[0, here, mine_lanes] * low(HEAD_DIM**-0.5)
            result = None
            marks = lse[here]
            for h in range(2):
                mine = jnp.where(lanes == h, query, low(0))
                scores = mm(mine, keys[...], NT) + mask[...]
                top = jnp.max(scores, axis=-1, keepdims=True)
                weight = jnp.exp(scores - top)
                sums = jnp.sum(weight, axis=-1, keepdims=True)
                probs = (weight * (1.0 / sums)).astype(low)
                got = mm(probs, vals[...], NN)
                result = got if h == 0 else jnp.where(lanes == 0, result, got)
                marks = jnp.where(spot == 2 * pair + h, top + jnp.log(sums), marks)
            lse[here] = marks
            att[here] = result.astype(low)

    @pl.when(step == total - 1)
    def _():
        end()
        for n in range(4):
            t, lanes = kv(n)
            arrived(kept.at[1 + t, :, lanes], ks.at[n])
        pltpu.make_async_copy(far, far_out, fs).wait()


def forward(count, tok, gain, shift, w, bias, spots, freqs, mask, shards):
    rows, width = tok.shape
    half = w.shape[2] // 3
    groups, pairs = len(shards), width // 128
    whole = lambda *s: pl.BlockSpec(s, lambda i: (0,) * len(s))
    at = lambda i: jnp.minimum(i, 5)
    any_spec = pl.BlockSpec(memory_space=pl.ANY)
    sds, vm, dma = jax.ShapeDtypeStruct, pltpu.VMEM, pltpu.SemaphoreType.DMA
    return pl.pallas_call(
        functools.partial(forward_kernel, count, groups, pairs),
        grid=(6 + pairs,),
        out_shape=[
            sds((3, rows, width), low), sds((rows, width), low), sds((rows, width), low),
            sds((rows, 128), f32), sds((2, rows, width), low),
        ]
        + full_shapes(count, shards),
        in_specs=[
            whole(rows, width), whole(1, width), whole(1, width),
            pl.BlockSpec((1, width, half), lambda i: (at(i) // 3, 0, at(i) % 3)),
            pl.BlockSpec((1, 1, half), lambda i: (at(i) % 3, 0, at(i) // 3)),
            whole(rows, 128), whole(1, 128), whole(1, 2 * rows),
        ]
        + [any_spec] * groups,
        out_specs=[
            pl.BlockSpec((1, rows, half), lambda i: (at(i) % 3, 0, at(i) // 3)),
            whole(rows, width),
            pl.BlockSpec((rows, 128), lambda i: (0, jnp.maximum(i - 6, 0))),
            whole(rows, 128), any_spec,
        ]
        + [any_spec] * groups,
        scratch_shapes=[
            vm((rows, width), low), vm((rows, 128), f32), vm((rows, 128), f32),
            vm((3, rows, width), low), vm((2, rows, width), low), vm((2 * rows, 128), low),
            vm((2 * rows, 128), low), dma((4,)), dma((4,)), dma(()),
        ]
        + gather_sems(count, groups),
        compiler_params=pltpu.CompilerParams(
            vmem_limit_bytes=VMEM_LIMIT, collective_id=3, has_side_effects=True
        ),
        name="forward",
    )(tok, gain, shift, w, bias, spots, freqs, mask, *shards)


def unattend_kernel(count, groups, pairs, *refs):
    q, k, v, kp, vp, mask, lse, grad = refs[:8]
    parts, mixed = refs[8 : 8 + groups], refs[8 + groups]
    dq, dkv, dfar = refs[9 + groups : 12 + groups]
    outs, home = refs[12 + groups : 12 + 2 * groups], refs[12 + 2 * groups]
    keys, vals, dk, dv, ts, tr, tl = refs[13 + 2 * groups : 20 + 2 * groups]
    begin, steps, end = scatter_job(count, parts, outs, refs[20 + 2 * groups :])
    deliver, delivered = deliver_job(mixed, home, ts, tr, tl)
    pair = pl.program_id(0)
    rows = q.shape[1]
    chunk = rows // 2

    for n in range(pairs):

        @pl.when(pair == n)
        def _(n=n):
            if n == 0:
                greet(count, corner=True)
                begin()
                deliver()
            for one in share(steps, n, pairs):
                one()

    keys[:rows], keys[rows:] = k[0], kp[0]
    vals[:rows], vals[rows:] = v[0], vp[0]
    lanes = head_lanes(chunk)
    spot = lax.broadcasted_iota(jnp.int32, (chunk, 128), 1)
    for n in range(rows // chunk):
        here = slice(n * chunk, (n + 1) * chunk)
        query = q[0, here] * low(HEAD_DIM**-0.5)
        out_grad = grad[here]
        result = None
        for h in range(2):
            mine = jnp.where(lanes == h, query, low(0))
            mine_grad = jnp.where(lanes == h, out_grad, low(0))
            shift = jnp.sum(jnp.where(spot == 2 * pair + h, lse[here], 0.0), axis=-1, keepdims=True)
            probs = jnp.exp(mm(mine, keys[...], NT) + mask[...] - shift)
            d_probs = mm(mine_grad, vals[...], NT)
            both = probs * d_probs
            inner = jnp.sum(both, axis=-1, keepdims=True)
            d_scores = (both - probs * inner).astype(low)
            got = mm(d_scores, keys[...], NN)
            result = got if h == 0 else jnp.where(lanes == 0, result, got)
            key_part = mm(d_scores, mine, TN)
            value_part = mm(probs.astype(low), mine_grad, TN)
            if n == 0 and h == 0:
                dk[...], dv[...] = key_part, value_part
            else:
                dk[...] += key_part
                dv[...] += value_part
        dq[here] = result * HEAD_DIM**-0.5
    dkv[0], dkv[1] = dk[:rows], dv[:rows]
    dfar[0], dfar[1] = dk[rows:].astype(low), dv[rows:].astype(low)

    @pl.when(pair == pairs - 1)
    def _():
        end()
        delivered()


def unattend(count, qkv, far, mask, lse, grad, parts, mixed):
    _, rows, width = qkv.shape
    keys, groups, pairs = 2 * rows, len(parts), width // 128
    shapes = [p.shape[4:] for p in parts]
    any_spec = pl.BlockSpec(memory_space=pl.ANY)
    at = lambda t: pl.BlockSpec((1, rows, 128), lambda g: (t, 0, g))
    both = pl.BlockSpec((2, rows, 128), lambda g: (0, 0, g))
    column = pl.BlockSpec((rows, 128), lambda g: (0, g))
    whole = lambda *s: pl.BlockSpec(s, lambda g: (0,) * len(s))
    sds, vm = jax.ShapeDtypeStruct, pltpu.VMEM
    return pl.pallas_call(
        functools.partial(unattend_kernel, count, groups, pairs),
        grid=(pairs,),
        out_shape=[
            sds((rows, width), f32), sds((2, rows, width), f32), sds((2, rows, width), low),
        ]
        + [sds(s, f32) for s in shapes]
        + [sds(mixed.shape, low)],
        in_specs=[
            at(0), at(1), at(2), at(0), at(1), whole(1, keys), whole(rows, 128), column,
        ]
        + [any_spec] * (groups + 1),
        out_specs=[column, both, both] + [whole(*s) for s in shapes] + [any_spec],
        scratch_shapes=[vm((keys, 128), low)] * 2
        + [vm((keys, 128), f32)] * 2
        + deliver_sems()
        + scatter_scratch(count, shapes),
        compiler_params=pltpu.CompilerParams(
            vmem_limit_bytes=VMEM_LIMIT, collective_id=4, has_side_effects=True
        ),
        name="unattend",
    )(qkv, qkv, qkv, far, far, mask, lse, grad, *parts, mixed)


def unproject_kernel(count, *refs):
    dq, dkv, got, w, spots, freqs, tok, gain, d_resid, h1, p_gu = refs[:11]
    p_qkv, sums, col, r_gu, home = refs[11:16]
    acc, cos, sin, flipped, leaving, ts, tr, tl = refs[16:24]
    parts, outs = [p_gu.at[0], p_gu.at[1]], [r_gu.at[0], r_gu.at[1]]
    begin, steps, end = scatter_job(count, parts, outs, refs[24:])
    deliver, delivered = deliver_job(leaving, home, ts, tr, tl)
    step = pl.program_id(0)
    t = lax.rem(step, 3)

    @pl.when(step == 0)
    def _():
        greet(count, corner=True)
        begin()
        cosine, sine = tables(spots[...], freqs[...])
        cos[...] = cosine
        sin[...] = -sine
        flipped[...] = h1[...].T

    for n in range(6):

        @pl.when(step == n)
        def _(n=n):
            for one in share(steps, n, 6):
                one()

    def turned(value):
        parts = [
            turn(value[:, n * 128 : (n + 1) * 128], cos[...], sin[...])
            for n in range(value.shape[1] // 128)
        ]
        return jnp.concatenate(parts, axis=1)

    def use(value):
        rounded = value.astype(low)
        col[0] = jnp.sum(rounded.astype(f32), axis=0, keepdims=True)
        p_qkv[0, 0] = mm(flipped[...], rounded, NN).astype(low)
        part = mm(rounded, w[0], NT)

        @pl.when(step == 0)
        def _():
            acc[...] = part

        @pl.when(step > 0)
        def _():
            acc[...] += part

    @pl.when(t == 0)
    def _():
        use(turned(dq[...]))

    @pl.when(t == 1)
    def _():
        use(turned(dkv[0] + got[0].astype(f32)))

    @pl.when(t == 2)
    def _():
        use(dkv[0] + got[0].astype(f32))

    @pl.when(step == 5)
    def _():
        width = tok.shape[1]
        normed, inverse = normalise(tok[...].astype(f32), width)
        up = acc[...]
        sums[0:1] = jnp.sum(up * normed, axis=0, keepdims=True)
        sums[1:2] = jnp.sum(up, axis=0, keepdims=True)
        scaled = up * gain[...]
        mean = jnp.sum(scaled, axis=-1, keepdims=True) / width
        cross = jnp.sum(scaled * normed, axis=-1, keepdims=True) / width
        result = d_resid[...] + inverse * (scaled - mean - normed * cross)
        for n in range(4):
            leaving[n] = result[n * PAD : (n + 1) * PAD].astype(low)
        end()
        deliver()
        delivered()


def unproject(count, dq, dkv, got, w, spots, freqs, tok, gain, d_resid, h1, p_gu):
    rows, width = tok.shape
    half = w.shape[2] // 3
    whole = lambda *s: pl.BlockSpec(s, lambda i: (0,) * len(s))
    once = lambda *s: pl.BlockSpec(s, lambda i: (0,) * len(s), pipeline_mode=pl.Buffered(1))
    pick = lambda i: (jnp.maximum(i % 3 - 1, 0), 0, i // 3)
    any_spec = pl.BlockSpec(memory_space=pl.ANY)
    shape = p_gu.shape[5:]
    sds, vm = jax.ShapeDtypeStruct, pltpu.VMEM
    return pl.pallas_call(
        functools.partial(unproject_kernel, count),
        grid=(6,),
        out_shape=[
            sds((3, 2, width, half), low), sds((2, width), f32), sds((3, 1, width), f32),
            sds((2,) + shape, f32), sds((4, PAD, width), low),
        ],
        in_specs=[
            pl.BlockSpec((rows, half), lambda i: (0, i // 3)),
            pl.BlockSpec((1, rows, half), pick), pl.BlockSpec((1, rows, half), pick),
            pl.BlockSpec((1, width, half), lambda i: (i // 3, 0, i % 3)),
            once(rows, 128), once(1, 128), once(rows, width), once(1, width),
            once(rows, width), once(rows, width), any_spec,
        ],
        out_specs=[
            pl.BlockSpec((1, 1, width, half), lambda i: (i % 3, i // 3, 0, 0)),
            whole(2, width), pl.BlockSpec((1, 1, half), lambda i: (i % 3, 0, i // 3)),
            whole(2, *shape), any_spec,
        ],
        scratch_shapes=[
            vm((rows, width), f32), vm((rows, 128), f32), vm((rows, 128), f32),
            vm((width, rows), low), vm((4, PAD, width), low),
        ]
        + deliver_sems()
        + scatter_scratch(count, [shape, shape]),
        compiler_params=pltpu.CompilerParams(
            vmem_limit_bytes=VMEM_LIMIT, collective_id=5, has_side_effects=True
        ),
        name="unproject",
    )(dq, dkv, got, w, spots, freqs, tok, gain, d_resid, h1, p_gu)


SLAB = 16


def in_slabs(rows, body):
    def step(i, carry):
        body(pl.ds(pl.multiple_of(i * SLAB, SLAB), SLAB))
        return carry

    lax.fori_loop(0, rows // SLAB, step, 0)


def fold(values):
    return values[:8] + values[8:]


def across(values):
    return jnp.sum(values, axis=-1, keepdims=True)


def down_rows(acc):
    return jnp.sum(acc, axis=0, keepdims=True)


def ffn_kernel(
    hidden, part, att, tok, grad, w_out, w_gu, w_down, gu_bias, in_gain, in_bias, gain2, shift2,
    b_out, b_down, mixed, inner, d_gu, h2, d_resid, g_attn, d_att, wide_sums, thin_sums,
    resid, gate, up, act, acc, d_in, stats, wide_acc, thin_acc,
):
    step = pl.program_id(0)
    rows, width = tok.shape
    wide = in_gain.shape[2]
    half = w_out.shape[2]
    edge = lax.broadcasted_iota(jnp.int32, (SLAB, wide), 1) < part

    def at(n):
        return pl.when(step == n)

    @at(0)
    def _():
        acc[...] = mm(att[:, :half], w_out[0], NT)
        wide_acc[...] = jnp.zeros_like(wide_acc)
        thin_acc[...] = jnp.zeros_like(thin_acc)

    @at(1)
    def _():
        acc[...] += mm(att[:, half:], w_out[0], NT)

        def body(s):
            value = tok[s].astype(f32) + acc[s] + b_out[...]
            resid[s] = value
            normed, _ = normalise(value, width)
            h2[s] = (normed * gain2[...] + shift2[...]).astype(low)

        in_slabs(rows, body)

    for n in range(2):

        @at(2 + 2 * n)
        def _(n=n):
            gate[n] = mm(h2[...], w_gu[0], NN) + gu_bias[0]

        @at(3 + 2 * n)
        def _(n=n):
            up[n] = mm(h2[...], w_gu[0], NN) + gu_bias[0]

            def body(s):
                value = gate[n, s]
                out = value * jax.nn.sigmoid(value) * up[n, s]
                act[n, s] = out
                total = across(out)
                stats[0, s] = total if n == 0 else stats[0, s] + total

            in_slabs(rows, body)

    @at(6)
    def _():
        def body(s):
            centre = stats[0, s] / hidden
            total = 0.0
            moved = []
            for n in range(2):
                shifted = jnp.where(edge, act[n, s] - centre, 0.0)
                moved.append(shifted)
                total = total + across(jnp.square(shifted))
            inverse = lax.rsqrt(total / hidden + epsilon)
            stats[1, s] = inverse
            for n in range(2):
                normed = moved[n] * inverse
                act[n, s] = normed
                inner[n, s] = (normed * in_gain[n] + in_bias[n]).astype(low)

        in_slabs(rows, body)

    for n in range(2):

        @at(6 + n)
        def _(n=n):
            out = mm(inner[n], w_down[0], NT)
            if n == 0:
                acc[...] = out
            else:
                acc[...] += out
            d_in[n] = mm(grad[...], w_down[0], NN)

    @at(7)
    def _():
        def first(s):
            mixed[s] = (resid[s] + acc[s] + b_down[...]).astype(low)
            thin_acc[0] += fold(grad[s].astype(f32))

        in_slabs(rows, first)

        def second(s):
            mean, cross = 0.0, 0.0
            kept = []
            for n in range(2):
                value, normed = d_in[n, s], act[n, s]
                wide_acc[n, 0] += fold(value * normed)
                wide_acc[n, 1] += fold(value)
                scaled = value * in_gain[n]
                mean = mean + across(scaled)
                cross = cross + across(scaled * normed)
            mean, cross = mean / hidden, cross / hidden
            for n in range(2):
                normed, value, other = act[n, s], gate[n, s], up[n, s]
                d_act = stats[1, s] * (d_in[n, s] * in_gain[n] - mean - normed * cross)
                sigma = jax.nn.sigmoid(value)
                d_gate = (d_act * other * sigma * (1.0 + value * (1.0 - sigma))).astype(low)
                d_up = (d_act * value * sigma).astype(low)
                wide_acc[n, 2] += fold(d_gate.astype(f32))
                wide_acc[n, 3] += fold(d_up.astype(f32))
                d_gu[n, s, :wide] = d_gate
                d_gu[n, s, wide:] = d_up

        in_slabs(rows, second)
        for n in range(2):
            for k in range(4):
                wide_sums[n, k : k + 1] = down_rows(wide_acc[n, k])

    for n in range(4):

        @at(8 + n)
        def _(n=n):
            out = mm(d_gu[n // 2, :, (n % 2) * wide : (n % 2 + 1) * wide], w_gu[0], NT)
            if n == 0:
                acc[...] = out
            else:
                acc[...] += out

    @at(11)
    def _():
        def body(s):
            value = acc[s]
            normed, inverse = normalise(resid[s], width)
            thin_acc[1] += fold(value * normed)
            thin_acc[2] += fold(value)
            scaled = value * gain2[...]
            mean, cross = across(scaled) / width, across(scaled * normed) / width
            out = grad[s].astype(f32) + inverse * (scaled - mean - normed * cross)
            d_resid[s] = out
            rounded = out.astype(low)
            g_attn[s] = rounded
            thin_acc[3] += fold(rounded.astype(f32))

        in_slabs(rows, body)
        for k in range(4):
            thin_sums[k : k + 1] = down_rows(thin_acc[k])

    for n in range(2):

        @at(12 + n)
        def _(n=n):
            d_att[:, n * half : (n + 1) * half] = mm(g_attn[...], w_out[0], NN).astype(low)


def ffn(hidden, part, att, tok, grad, w_out, w_gu, w_down, gu_bias, in_gain, in_bias, gain2, shift2, b_out, b_down):
    rows, width = tok.shape
    half, wide = w_out.shape[2], w_down.shape[2]
    whole = lambda *s: pl.BlockSpec(s, lambda i: (0,) * len(s))
    out_at = lambda i: (jnp.where(i < 1, 0, jnp.where(i < 12, 1, jnp.where(i < 13, 0, 1))), 0, 0)

    def gu_at(i):
        n = jnp.where(i < 8, jnp.clip(i - 2, 0, 3), jnp.clip(i - 8, 0, 3))
        return n // 2, n % 2

    sds = jax.ShapeDtypeStruct
    shapes = [
        sds((rows, width), low), sds((2, rows, wide), low), sds((2, rows, 2 * wide), low),
        sds((rows, width), low), sds((rows, width), f32), sds((rows, width), low),
        sds((rows, width), low), sds((2, 4, wide), f32), sds((4, width), f32),
    ]
    return pl.pallas_call(
        functools.partial(ffn_kernel, hidden, part),
        grid=(14,),
        out_shape=shapes,
        in_specs=[
            whole(rows, width), whole(rows, width), whole(rows, width),
            pl.BlockSpec((1, width, half), out_at),
            pl.BlockSpec((1, width, wide), lambda i: (gu_at(i)[0], 0, gu_at(i)[1])),
            pl.BlockSpec((1, width, wide), lambda i: (jnp.where(i < 7, 0, 1), 0, 0)),
            pl.BlockSpec((1, 1, wide), lambda i: (gu_at(i)[0], 0, gu_at(i)[1])),
            whole(2, 1, wide), whole(2, 1, wide), whole(1, width), whole(1, width),
            whole(1, width), whole(1, width),
        ],
        out_specs=[pl.BlockSpec(s.shape, lambda i, k=len(s.shape): (0,) * k, pipeline_mode=pl.Buffered(1)) for s in shapes],
        scratch_shapes=[
            pltpu.VMEM((rows, width), f32), pltpu.VMEM((2, rows, wide), f32),
            pltpu.VMEM((2, rows, wide), f32), pltpu.VMEM((2, rows, wide), f32),
            pltpu.VMEM((rows, width), f32), pltpu.VMEM((2, rows, wide), f32),
            pltpu.VMEM((2, rows, 1), f32), pltpu.VMEM((2, 4, 8, wide), f32),
            pltpu.VMEM((4, 8, width), f32),
        ],
        compiler_params=pltpu.CompilerParams(vmem_limit_bytes=66000000),
        cost_estimate=pl.CostEstimate(flops=20000000000, bytes_accessed=50000000, transcendentals=0),
        name="ffn",
    )(att, tok, grad, w_out, w_gu, w_down, gu_bias, in_gain, in_bias, gain2, shift2, b_out, b_down)


def outer_kernel(left, right, out, flipped):
    @pl.when(pl.program_id(0) == 0)
    def _():
        flipped[...] = left[...].T

    right = right[...] if len(right.shape) == 2 else right[0]
    result = mm(flipped[...], right, NN).astype(low)
    if len(out.shape) == 4:
        out[0, 0] = result
    else:
        out[0] = result


def outer(left, right, steps, right_spec, out_spec, out_shape):
    rows, width = left.shape
    return pl.pallas_call(
        outer_kernel,
        grid=(steps,),
        out_shape=jax.ShapeDtypeStruct(out_shape, low),
        in_specs=[pl.BlockSpec((rows, width), lambda i: (0, 0)), right_spec],
        out_specs=out_spec,
        scratch_shapes=[pltpu.VMEM((width, rows), low)],
        compiler_params=pltpu.CompilerParams(vmem_limit_bytes=VMEM_LIMIT),
        name="outer",
    )(left, right)


def on_device(
    count, tokens, positions, key_mask, norm1_gain, norm1_bias, qkv_weight, qv_bias, out_weight,
    out_bias, norm2_gain, norm2_bias, gate_up_weight, gate_up_bias, inner_gain, inner_bias,
    down_weight, down_bias, cotangent,
):
    b, x, c, y = (lax.axis_index(a) for a in FAR)
    image = 2 * x + y
    local, images, width = tokens.shape
    shard = qkv_weight.shape[0]
    half = qkv_weight.shape[2]
    part = gate_up_weight.shape[2]
    hidden = gate_up_bias.shape[1]
    wide = -(-part // 128) * 128
    more = wide - part
    rows = 4 * PAD

    shards = [
        qkv_weight.astype(low).reshape(shard, 3 * half),
        out_weight.astype(low).T,
        jnp.pad(gate_up_weight.astype(low), ((0, 0), (0, 0), (0, more))).reshape(shard, 2 * wide),
        jnp.pad(down_weight.astype(low).T, ((0, 0), (0, more))),
    ]
    chunks = jnp.pad(jnp.swapaxes(tokens, 0, 1), ((0, 0), (0, PAD - local), (0, 0)))
    cot = jnp.transpose(cotangent.reshape(2, local, images, width), (2, 0, 1, 3))
    cot = jnp.pad(cot, ((0, 0), (0, 0), (0, PAD - local), (0, 0)))
    spots = jnp.transpose(positions.reshape(2, 2, local, images), (3, 1, 2, 0)).astype(low)
    spots = jnp.pad(spots, ((0, 0), (0, 0), (0, PAD - local), (0, 0)))
    pick = (jnp.arange(128) // 32) % 2
    spots = jnp.where(pick == 0, spots[..., 0:1], spots[..., 1:2])
    join = lambda f: f.reshape(2, width, f.shape[-1])
    w_qkv, tok, spot, grad = gather_first(count, shards[:1], chunks, spots, cot)
    w_qkv = join(w_qkv)
    tok, spot, grad = tok.reshape(rows, width), spot.reshape(rows, 128), grad.reshape(rows, width)

    live = lax.dynamic_index_in_dim(key_mask, image, 1, keepdims=False)
    live = jnp.pad(live.reshape(2, 2, 2, local), ((0, 0), (0, 0), (0, 0), (0, PAD - local)))
    live = jnp.stack(
        [lax.dynamic_index_in_dim(live, n, 1, keepdims=False).reshape(rows) for n in (c, 1 - c)]
    )
    bias = jnp.where(live > 0, 0.0, masked_score).astype(f32).reshape(1, 2 * rows)

    freqs = jnp.tile(10000.0 ** (-jnp.arange(16).astype(f32) / 16), 8).reshape(1, 128)
    row = lambda a: a.reshape(1, -1)
    qkv_bias = jnp.stack([qv_bias[0], jnp.zeros_like(qv_bias[0]), qv_bias[1]])[:, None]
    swap = ((0, 1), (1, 0))
    qkv, h1, attended, lse, far, *full = forward(
        count, tok, row(norm1_gain), row(norm1_bias), w_qkv, qkv_bias, spot, freqs, bias, shards[1:]
    )
    w_out, w_gu, w_down = (join(f) for f in full)

    split = lambda a: jnp.pad(a.reshape(a.shape[:-1] + (2, part)), ((0, 0),) * a.ndim + ((0, more),))
    gu_bias = jnp.swapaxes(split(gate_up_bias), 0, 1).reshape(2, 1, 2 * wide)
    mixed, inner, d_gu, h2, d_resid, g_attn, d_attended, wide_sums, thin_sums = ffn(
        hidden, part, attended, tok, grad, w_out, w_gu, w_down, gu_bias,
        split(inner_gain)[:, None], split(inner_bias)[:, None], row(norm2_gain), row(norm2_bias),
        row(out_bias), row(down_bias),
    )
    by_owner = lambda a: a.reshape(a.shape[:-2] + (count, 2, 2, shard, a.shape[-1]))
    p_down = by_owner(
        outer(
            grad, inner, 2, pl.BlockSpec((1, rows, wide), lambda i: (i, 0, 0)),
            pl.BlockSpec((1, width, wide), lambda i: (i, 0, 0)), (2, width, wide),
        )
    )
    p_out = by_owner(
        outer(
            g_attn, attended, 2, pl.BlockSpec((rows, half), lambda i: (0, i)),
            pl.BlockSpec((1, width, half), lambda i: (i, 0, 0)), (2, width, half),
        )
    )
    p_gu = by_owner(
        outer(
            h2, d_gu, 4, pl.BlockSpec((1, rows, wide), lambda i: (i % 2, 0, i // 2)),
            pl.BlockSpec((1, 1, width, wide), lambda i: (i // 2, i % 2, 0, 0)),
            (2, 2, width, wide),
        )
    )
    dq, dkv, dfar, r_down, r_out, mixed_home = unattend(
        count, qkv, far, bias, lse, d_attended, [p_down, p_out], mixed.reshape(4, PAD, width)
    )
    got = lax.ppermute(dfar, "core", swap)
    p_qkv, sums1, col, r_gu, d_tok_home = unproject(
        count, dq, dkv, got, w_qkv, spot, freqs, tok, row(norm1_gain), d_resid, h1, p_gu
    )

    merge = lambda a: a[..., :part].reshape(a.shape[:-2] + (hidden,))
    d_gu_bias = merge(jnp.swapaxes(wide_sums[:, 2:], 0, 1))
    d_in_gain, d_in_bias = wide_sums[:, 0], wide_sums[:, 1]
    d_down_bias, d_gain2, d_bias2, d_out_bias = (thin_sums[n] for n in range(4))
    vectors = [
        sums1[0], sums1[1], jnp.stack([col[0, 0], col[2, 0]]), d_out_bias, d_gain2, d_bias2,
        d_gu_bias, merge(d_in_gain), merge(d_in_bias), d_down_bias,
    ]
    flat = jnp.concatenate([v.reshape(-1) for v in vectors])
    size = flat.shape[0]
    lines = -(-size // 2048) * 16
    flat = jnp.pad(flat, (0, lines * 128 - size)).reshape(lines, 128)
    r_qkv, summed = last(count, by_owner(p_qkv), flat, 1)
    summed = summed.reshape(-1)
    pieces, at = [], 0
    for v in vectors:
        pieces.append(summed[at : at + v.size].reshape(v.shape))
        at += v.size

    home = lambda landed: jnp.swapaxes(landed[:, :local], 0, 1)

    return (
        home(mixed_home), home(d_tok_home), pieces[0], pieces[1], jnp.swapaxes(r_qkv, 0, 1), pieces[2],
        r_out.T, pieces[3], pieces[4], pieces[5], jnp.swapaxes(r_gu[:, :, :part], 0, 1),
        pieces[6], pieces[7], pieces[8], r_down[:, :part].T, pieces[9],
    )


def solution(mesh):
    count, ctx, tensor = (mesh.shape[a] for a in ("batch", "ctx", "tensor"))
    fine = jax.sharding.Mesh(mesh.devices.reshape(count, ctx // 2, 2, tensor), FAR)
    ctx, wide = ("x", "core"), ("batch", "x", "core")
    return jax.shard_map(
        functools.partial(on_device, count),
        mesh=fine,
        in_specs=(
            P(("x", "core", "tensor"), "batch", None), P(None, ctx, "batch"), P(None, "batch"),
            P(), P(), P(wide, None, "tensor"), P(), P("tensor", wide), P(), P(), P(),
            P(wide, None, "tensor"), P(), P(), P(), P("tensor", wide), P(), P(ctx, "batch", None),
        ),
        out_specs=(
            P(("x", "core", "tensor"), "batch", None), P(("x", "core", "tensor"), "batch", None),
            P(), P(), P(wide, None, "tensor"), P(), P("tensor", wide), P(), P(), P(),
            P(wide, None, "tensor"), P(), P(), P(), P("tensor", wide), P(),
        ),
        check_vma=False,
    )
```

```python
import functools

import jax
import jax.numpy as jnp
from jax import lax
from jax.experimental import pallas as pl
from jax.experimental.pallas import tpu as pltpu

from jax.sharding import PartitionSpec as P
MESH = pl.DeviceIdType.MESH
FAR = ("batch", "x", "core", "tensor")


def place(b, x, c, y):
    return {"batch": b, "x": x, "core": c, "tensor": y}


def ring_offsets(count):
    order = [0]
    for step in range(1, count // 2 + 1):
        for off in (step, count - step):
            if off not in order:
                order.append(off)
    return order


def greet(count, corner=False):
    b, x, c, y = (lax.axis_index(a) for a in FAR)
    barrier = pltpu.get_barrier_semaphore()
    for off in range(1, count):
        pl.semaphore_signal(
            barrier, inc=1, device_id=place(lax.rem(b + off, count), x, c, y), device_id_type=MESH
        )
    near = [place(b, 1 - x, c, y), place(b, x, c, 1 - y), place(b, x, 1 - c, y)]
    if corner:
        near.append(place(b, 1 - x, c, 1 - y))
    for there in near:
        pl.semaphore_signal(barrier, inc=1, device_id=there, device_id_type=MESH)
    pl.semaphore_wait(barrier, count - 1 + len(near))


def push(src, dst, s, r, there):
    pltpu.make_async_remote_copy(
        src_ref=src, dst_ref=dst, send_sem=s, recv_sem=r, device_id=there, device_id_type=MESH
    ).start()


def arrived(dst, sem):
    pltpu.make_async_copy(dst, dst, sem).wait()


def bounce(src, via, dst, sems):
    inward = pltpu.make_async_copy(src, via, sems.at[0])
    outward = pltpu.make_async_copy(via, dst, sems.at[1])

    def turn_round():
        inward.wait()
        outward.start()

    return inward.start, turn_round, outward.wait


def gather_scratch(count, shapes):
    groups = len(shapes)
    dma = pltpu.SemaphoreType.DMA
    many, one = dma((groups, count)), dma((groups,))
    sems = [one, many, one, many, one, many, one, one, many, one, one, dma((groups, 2))]
    return sems + [pltpu.VMEM(s, jnp.bfloat16) for s in shapes]


def gather_job(count, own, full, sems, by_x=lambda j: j % 2 == 1):
    groups = len(own)
    zs, zr, xs, xr, ys, yr, xds, yds, dr, cs, cr, ls, *vias = sems
    b, x, c, y = (lax.axis_index(a) for a in FAR)
    xn, yn, cn = place(b, 1 - x, c, y), place(b, x, c, 1 - y), place(b, x, 1 - c, y)
    offsets = ring_offsets(count)

    def block(g, yy, item, xx, cc):
        return full[g].at[yy, lax.rem(b + offsets[item], count), xx, cc]

    copies = [
        bounce(own[g], vias[g], full[g].at[y, b, x, c], ls.at[g]) for g in range(groups)
    ]

    def begin():
        for g in range(groups):
            for j in range(1, count):
                there = place(lax.rem(b + count - offsets[j], count), x, c, y)
                push(own[g], full[g].at[y, b, x, c], zs.at[g], zr.at[g, j], there)
            copies[g][0]()

    def column(g, j):
        dst = block(g, y, j, x, c)
        if j > 0:
            arrived(dst, zr.at[g, j])
        src = own[g] if j == 0 else dst
        push(src, dst, xs.at[g], xr.at[g, j], xn)
        push(src, dst, ys.at[g], yr.at[g, j], yn)
        push(src, dst, cs.at[g], cr.at[g], cn)

    def plane(g, j):
        from_x, from_y = block(g, y, j, 1 - x, c), block(g, 1 - y, j, x, c)
        arrived(from_x, xr.at[g, j])
        if not by_x(j):
            push(from_x, from_x, yds.at[g], dr.at[g, j], yn)
        push(from_x, from_x, cs.at[g], cr.at[g], cn)
        arrived(from_y, yr.at[g, j])
        if by_x(j):
            push(from_y, from_y, xds.at[g], dr.at[g, j], xn)
        push(from_y, from_y, cs.at[g], cr.at[g], cn)

    def corner(g, j):
        there = block(g, 1 - y, j, 1 - x, c)
        arrived(there, dr.at[g, j])
        push(there, there, cs.at[g], cr.at[g], cn)

    items = [(g, 0) for g in range(groups)]
    items += [(g, j) for g in range(groups) for j in range(1, count)]
    lag = min(3, max(1, len(items) // 4))

    def stage(t):
        if t < len(items):
            column(*items[t])
        if 0 <= t - lag < len(items):
            plane(*items[t - lag])
        if t - 2 * lag >= 0:
            corner(*items[t - 2 * lag])
        if t == 1:
            for copy in copies:
                copy[1]()

    def end():
        for g in range(groups):
            copies[g][2]()
            arrived(full[g].at[:, :, :, 1 - c], cr.at[g])
            arrived(full[g].at[:, :, :, 0], cs.at[g])
            arrived(full[g].at[0, : count - 1, 0, 0], zs.at[g])
            arrived(full[g].at[0, :, 0, 0], xs.at[g])
            arrived(full[g].at[0, :, 0, 0], ys.at[g])
            xd = sum(1 for j in range(count) if by_x(j))
            if xd:
                arrived(full[g].at[0, :xd, 0, 0], xds.at[g])
            if xd < count:
                arrived(full[g].at[0, : count - xd, 0, 0], yds.at[g])

    return begin, [functools.partial(stage, t) for t in range(len(items) + 2 * lag)], end


def full_shapes(count, shards):
    return [jax.ShapeDtypeStruct((2, count, 2, 2) + s.shape, s.dtype) for s in shards]


def gather_kernel(count, groups, *refs):
    own = [refs[0].at[n] for n in range(groups)]
    tokens, spots = refs[1:3]
    full = [refs[3].at[n] for n in range(groups)]
    landed = refs[4:6]
    *sems, ts, tr, tl, via_t, via_s = refs[6:]
    b, x, c, y = (lax.axis_index(a) for a in FAR)
    begin, steps, end = gather_job(count, own, full, sems)
    image = 2 * x + y
    far = 2 * (1 - x) + y
    corners = ((1, 0), (0, 1), (1, 1))
    greet(count, corner=True)
    for n, (ox, oy) in enumerate(corners):
        px, py = (1 - x if ox else x), (1 - y if oy else y)
        push(
            tokens.at[2 * px + py], landed[0].at[image], ts.at[n], tr.at[n], place(b, px, c, py)
        )
    begin()
    xn = place(b, 1 - x, c, y)
    push(spots.at[far], landed[1].at[x], ts.at[3], tr.at[3], xn)
    homes = [
        bounce(tokens.at[image], via_t, landed[0].at[image], tl.at[0]),
        bounce(spots.at[image], via_s, landed[1].at[x], tl.at[1]),
    ]
    for copy in homes:
        copy[0]()
    for n, step in enumerate(steps):
        step()
        if n == 1:
            for copy in homes:
                copy[1]()
    end()
    for n, (ox, oy) in enumerate(corners):
        px, py = (1 - x if ox else x), (1 - y if oy else y)
        arrived(landed[0].at[2 * px + py], tr.at[n])
        arrived(tokens.at[0], ts.at[n])
    arrived(landed[1].at[1 - x], tr.at[3])
    arrived(spots.at[0], ts.at[3])
    for copy in homes:
        copy[2]()


def gather_first(count, shards, tokens, spots):
    groups = shards.shape[0]
    any_spec = pl.BlockSpec(memory_space=pl.ANY)
    dma = pltpu.SemaphoreType.DMA
    outs = [
        jax.ShapeDtypeStruct((groups, 2, count, 2, 2) + shards.shape[1:], shards.dtype),
        jax.ShapeDtypeStruct(tokens.shape, tokens.dtype),
        jax.ShapeDtypeStruct((2,) + spots.shape[1:], spots.dtype),
    ]
    return pl.pallas_call(
        functools.partial(gather_kernel, count, groups),
        out_shape=outs,
        in_specs=[any_spec] * 3,
        out_specs=[any_spec] * 3,
        scratch_shapes=gather_scratch(count, [shards.shape[1:]] * groups)
        + [dma((4,)), dma((4,)), dma((2, 2))]
        + [pltpu.VMEM(a.shape[1:], a.dtype) for a in (tokens, spots)],
        compiler_params=pltpu.CompilerParams(collective_id=0, has_side_effects=True),
        name="gather_first",
    )(shards, tokens, spots)


def scatter_scratch(count, shapes):
    groups = len(shapes)
    dma = pltpu.SemaphoreType.DMA
    scratch = [pltpu.VMEM((2, count, 2) + s, jnp.bfloat16) for s in shapes] * 2
    scratch += [pltpu.VMEM((count,) + s, jnp.bfloat16) for s in shapes] * 4
    many, one = dma((groups, count)), dma((groups,))
    return scratch + [many, one, many, one, many, one, many, one, one, many, one, many]


def scatter_job(count, parts, outs, scratch):
    groups = len(parts)
    held, peer, from_x, from_y, from_d, from_z = (
        scratch[k * groups : (k + 1) * groups] for k in range(6)
    )
    ls, cs, cr, xs, xr, ys, yr, xds, yds, dr, zs, zr = scratch[6 * groups :]
    b, x, c, y = (lax.axis_index(a) for a in FAR)
    xn, yn, cn = place(b, 1 - x, c, y), place(b, x, c, 1 - y), place(b, x, 1 - c, y)
    offsets = ring_offsets(count)
    order = list(range(1, count)) + [0]
    rows = held[0].shape[3]
    chunk = min(rows, 16)

    def add_to(target, *others):
        def body(i, carry):
            at_rows = pl.ds(pl.multiple_of(i * chunk, chunk), chunk)
            total = target[at_rows].astype(jnp.float32)
            for other in others:
                total = total + other[at_rows].astype(jnp.float32)
            target[at_rows] = total.astype(target.dtype)
            return carry

        lax.fori_loop(0, rows // chunk, body, 0)

    def where_to(j):
        return lax.rem(b + offsets[j], count)

    items = [(g, j) for g in range(groups) for j in order]

    def begin():
        for g, j in items:
            bb = where_to(j)
            push(parts[g].at[:, bb, :, 1 - c], peer[g].at[:, bb], cs.at[g], cr.at[g, j], cn)
            pltpu.make_async_copy(
                parts[g].at[:, bb, :, c], held[g].at[:, bb], ls.at[g, j]
            ).start()

    def merge_core(g, j):
        bb = where_to(j)
        arrived(held[g].at[:, bb], ls.at[g, j])
        arrived(peer[g].at[:, bb], cr.at[g, j])
        for yy, xx in ((1 - y, 1 - x), (y, 1 - x), (1 - y, x), (y, x)):
            add_to(held[g].at[yy, bb, xx], peer[g].at[yy, bb, xx])

    def send_corner(g, j):
        src = held[g].at[1 - y, where_to(j), 1 - x]
        if j % 2 == 0:
            push(src, from_d[g].at[j], xds.at[g], dr.at[g, j], xn)
        else:
            push(src, from_d[g].at[j], yds.at[g], dr.at[g, j], yn)

    def merge_corner(g, j):
        bb = where_to(j)
        arrived(from_d[g].at[j], dr.at[g, j])
        if j % 2 == 0:
            add_to(held[g].at[1 - y, bb, x], from_d[g].at[j])
        else:
            add_to(held[g].at[y, bb, 1 - x], from_d[g].at[j])

    def send_plane(g, j, by_x):
        bb = where_to(j)
        if by_x:
            push(held[g].at[y, bb, 1 - x], from_x[g].at[j], xs.at[g], xr.at[g, j], xn)
        else:
            push(held[g].at[1 - y, bb, x], from_y[g].at[j], ys.at[g], yr.at[g, j], yn)

    def merge_plane(g, j):
        arrived(from_x[g].at[j], xr.at[g, j])
        arrived(from_y[g].at[j], yr.at[g, j])
        add_to(held[g].at[y, where_to(j), x], from_x[g].at[j], from_y[g].at[j])

    def send_column(g, j):
        if j > 0:
            bb = where_to(j)
            push(
                held[g].at[y, bb, x], from_z[g].at[j], zs.at[g], zr.at[g, j], place(bb, x, c, y)
            )

    total = len(items)
    lag = min(3, max(1, total // 4))

    def stage(t):
        now = items[t] if t < total else None
        one = items[t - lag] if 0 <= t - lag < total else None
        two = items[t - 2 * lag] if t - 2 * lag >= 0 else None
        if two:
            merge_plane(*two)
        if one:
            merge_corner(*one)
        if now:
            merge_core(*now)
            send_corner(*now)
            send_plane(*now, now[1] % 2 == 0)
        if one:
            send_plane(*one, one[1] % 2 == 1)
        if two:
            send_column(*two)

    def end():
        for g in range(groups):
            for j in range(1, count):
                arrived(from_z[g].at[j], zr.at[g, j])

            def body(i, carry, g=g):
                at_rows = pl.ds(pl.multiple_of(i * chunk, chunk), chunk)
                result = held[g][y, b, x, at_rows].astype(jnp.float32)
                for j in range(1, count):
                    result = result + from_z[g][j, at_rows].astype(jnp.float32)
                outs[g][at_rows] = result
                return carry

            lax.fori_loop(0, rows // chunk, body, 0)
            arrived(peer[g], cs.at[g])
            arrived(from_x[g], xs.at[g])
            arrived(from_y[g], ys.at[g])
            arrived(from_d[g].at[: (count + 1) // 2], xds.at[g])
            arrived(from_d[g].at[: count // 2], yds.at[g])
            arrived(from_z[g].at[1:], zs.at[g])

    return begin, [functools.partial(stage, t) for t in range(total + 2 * lag)], end


CORNERS = ((1, 0), (0, 1), (1, 1))


def deliver_job(leaving, landed, ts, tr, tl, via):
    b, x, c, y = (lax.axis_index(a) for a in FAR)
    image = 2 * x + y
    copy = bounce(leaving.at[image], via, landed.at[image], tl)

    def begin():
        copy[0]()
        for n, (ox, oy) in enumerate(CORNERS):
            px, py = (1 - x if ox else x), (1 - y if oy else y)
            there = place(b, px, c, py)
            push(leaving.at[2 * px + py], landed.at[image], ts.at[n], tr.at[n], there)

    def end():
        copy[1]()
        copy[2]()
        for n, (ox, oy) in enumerate(CORNERS):
            px, py = (1 - x if ox else x), (1 - y if oy else y)
            arrived(landed.at[2 * px + py], tr.at[n])
            arrived(leaving.at[0], ts.at[n])

    return begin, end


def deliver_scratch(shape):
    dma = pltpu.SemaphoreType.DMA
    return [dma((3,)), dma((3,)), dma((2,)), pltpu.VMEM(shape, jnp.bfloat16)]


def share(todo, step, total):
    return todo[step * len(todo) // total : (step + 1) * len(todo) // total]


def sum_scratch(count, rows):
    half = (rows // 2, 128)
    dma, vm = pltpu.SemaphoreType.DMA, pltpu.VMEM
    return [
        vm((3,) + half, jnp.float32), vm(half, jnp.float32), vm(half, jnp.float32),
        vm((count,) + half, jnp.float32), dma((4,)), dma((4,)), dma(()), dma((count,)),
    ]


def sum_job(count, v_ref, o_ref, scratch):
    got, lane, plane, slots, ss, rs, zs, zr = scratch
    b, x, c, y = (lax.axis_index(a) for a in FAR)
    xn, yn, cn = place(b, 1 - x, c, y), place(b, x, c, 1 - y), place(b, x, 1 - c, y)
    half = v_ref.shape[0] // 2
    mine = pl.ds(pl.multiple_of(c * half, 8), half)
    theirs = pl.ds(pl.multiple_of((1 - c) * half, 8), half)

    def swap(src, dst, n, there):
        return pltpu.make_async_remote_copy(
            src_ref=src, dst_ref=dst, send_sem=ss.at[n], recv_sem=rs.at[n], device_id=there,
            device_id_type=MESH,
        )

    swaps = (
        lambda: swap(v_ref.at[theirs], got.at[0], 0, cn),
        lambda: swap(lane, got.at[1], 1, xn),
        lambda: swap(plane, got.at[2], 2, yn),
        lambda: swap(o_ref.at[mine], o_ref.at[mine], 3, cn),
    )

    def one():
        swaps[0]().start()

    def two():
        swaps[0]().wait()
        lane[...] = v_ref[mine] + got[0]
        swaps[1]().start()

    def three():
        swaps[1]().wait()
        plane[...] = lane[...] + got[1]
        swaps[2]().start()

    def four():
        swaps[2]().wait()
        slots[b] = plane[...] + got[2]
        for off in range(1, count):
            pltpu.make_async_remote_copy(
                src_ref=slots.at[b], dst_ref=slots.at[b], send_sem=zs, recv_sem=zr.at[off],
                device_id=place(lax.rem(b + off, count), x, c, y), device_id_type=MESH,
            ).start()

    def five():
        for off in range(1, count):
            there = slots.at[lax.rem(b + count - off, count)]
            pltpu.make_async_copy(there, there, zr.at[off]).wait()
        total = slots[0]
        for n in range(1, count):
            total = total + slots[n]
        o_ref[mine] = total
        swaps[3]().start()

    def six():
        swaps[3]().wait()
        rest = slots.at[: count - 1]
        pltpu.make_async_copy(rest, rest, zs).wait()

    return [one, two, three, four, five, six]


def last_kernel(count, p_qkv, vector, r_qkv, summed, *scratch):
    sums = sum_scratch(count, vector.shape[0])
    parts = [p_qkv.at[n] for n in range(3)]
    outs = [r_qkv.at[n] for n in range(3)]
    begin, steps, end = scatter_job(count, parts, outs, scratch[: -len(sums)])
    adds = sum_job(count, vector, summed, scratch[-len(sums) :])
    greet(count)
    begin()
    for n, step in enumerate(steps):
        step()
        for add in share(adds, n, len(steps)):
            add()
    end()


def last(count, p_qkv, vector, number):
    shapes = [p_qkv.shape[5:]] * 3
    vmem = pl.BlockSpec(memory_space=pltpu.VMEM)
    return pl.pallas_call(
        functools.partial(last_kernel, count),
        out_shape=[
            jax.ShapeDtypeStruct((3,) + shapes[0], jnp.float32),
            jax.ShapeDtypeStruct(vector.shape, jnp.float32),
        ],
        in_specs=[pl.BlockSpec(memory_space=pl.ANY), vmem],
        out_specs=[vmem, vmem],
        scratch_shapes=scatter_scratch(count, shapes) + sum_scratch(count, vector.shape[0]),
        compiler_params=pltpu.CompilerParams(
            collective_id=number, has_side_effects=True, vmem_limit_bytes=VMEM_LIMIT
        ),
        name="last",
    )(p_qkv, vector)


PAD = 136
WIDTH_TILE = 128
HEAD_DIM = 64
epsilon = 1e-06
masked_score = -1e30
f32, low = jnp.float32, jnp.bfloat16
VMEM_LIMIT = 60000000


def mm(a, b, dims):
    return lax.dot_general(a, b, (dims, ((), ())), preferred_element_type=f32)


NN = ((1,), (0,))
NT = ((1,), (1,))
TN = ((0,), (0,))


def normalise(values, width):
    centre = jnp.sum(values, axis=-1, keepdims=True) / width
    shifted = values - centre
    spread = jnp.sum(jnp.square(shifted), axis=-1, keepdims=True) / width
    inverse = lax.rsqrt(spread + epsilon)
    return shifted * inverse, inverse


def turn(values, cosine, sine):
    lane = lax.broadcasted_iota(jnp.int32, values.shape, 1)
    other = jnp.where((lane // 16) % 2 == 0, pltpu.roll(values, 112, 1), pltpu.roll(values, 16, 1))
    return values * cosine + other * sine


def tables(spots, freqs):
    angles = spots.astype(f32) * freqs
    lane = lax.broadcasted_iota(jnp.int32, angles.shape, 1)
    sine = jnp.sin(angles)
    return jnp.cos(angles), jnp.where((lane // 16) % 2 == 0, -sine, sine)


def head_lanes(rows):
    return lax.broadcasted_iota(jnp.int32, (rows, 128), 1) // HEAD_DIM


def forward_kernel(count, groups, pairs, *refs):
    tok, gain, shift, w, w_bias, spots, freqs, mask = refs[:8]
    own = refs[8 : 8 + groups]
    out, h1, att, lse, far_out = refs[8 + groups : 13 + groups]
    full = refs[13 + groups : 13 + 2 * groups]
    hid, cos, sin, kept, far, keys, vals, ks, kr, fs = refs[13 + 2 * groups : 23 + 2 * groups]
    begin, steps, end = gather_job(count, own, full, refs[23 + 2 * groups :])
    step = pl.program_id(0)
    rows = tok.shape[0]
    half = w.shape[3]
    b, x, c, y = (lax.axis_index(a) for a in FAR)
    cn = place(b, x, 1 - c, y)
    total = 6 + pairs

    def kv(n):
        t, side = n % 2, n // 2
        return t, slice(side * half, (side + 1) * half)

    @pl.when(step == 0)
    def _():
        greet(count)
        begin()
        normed, _ = normalise(tok[...].astype(f32), tok.shape[1])
        hid[...] = (normed * gain[...] + shift[...]).astype(low)
        h1[...] = hid[...]
        lse[...] = jnp.zeros_like(lse)
        cosine, sine = tables(spots[...], freqs[...])
        cos[...] = cosine
        sin[...] = sine

    for s in range(total):
        todo = steps[s * len(steps) // total : (s + 1) * len(steps) // total]
        done = s - 1
        sent = 2 * (done // 3) + done % 3 - 1 if 0 <= done < 6 and done % 3 > 0 else None

        @pl.when(step == s)
        def _(s=s, todo=todo, sent=sent):
            if sent is not None:
                t, lanes = kv(sent)
                push(kept.at[1 + t, :, lanes], far.at[t, :, lanes], ks.at[sent], kr.at[sent], cn)
            for one in todo:
                one()
            if s in (6, 6 + pairs // 2):
                for n in range(2) if s == 6 else range(2, 4):
                    t, lanes = kv(n)
                    arrived(far.at[t, :, lanes], kr.at[n])
            if s == total - 1:
                pltpu.make_async_copy(far, far_out, fs).start()

    for n in range(6):

        @pl.when(step == n)
        def _(n=n):
            t, lanes = n % 3, slice((n // 3) * half, (n // 3 + 1) * half)
            acc = mm(hid[...], w[0, 0], NN) + w_bias[0]
            if t < 2:
                parts = [
                    turn(acc[:, k : k + 128], cos[...], sin[...]).astype(low)
                    for k in range(0, half, 128)
                ]
                result = jnp.concatenate(parts, axis=1)
            else:
                result = acc.astype(low)
            out[0] = result
            kept[t, :, lanes] = result

    @pl.when(step >= 6)
    def _():
        pair = step - 6
        mine_lanes = pl.ds(pl.multiple_of(pair * 128, 128), 128)
        keys[:rows], keys[rows:] = kept[1, :, mine_lanes], far[0, :, mine_lanes]
        vals[:rows], vals[rows:] = kept[2, :, mine_lanes], far[1, :, mine_lanes]
        chunk = rows // 2
        lanes = head_lanes(chunk)
        spot = lax.broadcasted_iota(jnp.int32, (chunk, 128), 1)
        for n in range(rows // chunk):
            here = slice(n * chunk, (n + 1) * chunk)
            query = kept[0, here, mine_lanes] * low(HEAD_DIM**-0.5)
            result = None
            marks = lse[here]
            for h in range(2):
                mine = jnp.where(lanes == h, query, low(0))
                scores = mm(mine, keys[...], NT) + mask[...]
                top = jnp.max(scores, axis=-1, keepdims=True)
                weight = jnp.exp(scores - top)
                sums = jnp.sum(weight, axis=-1, keepdims=True)
                probs = (weight * (1.0 / sums)).astype(low)
                got = mm(probs, vals[...], NN)
                result = got if h == 0 else jnp.where(lanes == 0, result, got)
                marks = jnp.where(spot == 2 * pair + h, top + jnp.log(sums), marks)
            lse[here] = marks
            att[here] = result.astype(low)

    @pl.when(step == total - 1)
    def _():
        end()
        for n in range(4):
            t, lanes = kv(n)
            arrived(kept.at[1 + t, :, lanes], ks.at[n])
        pltpu.make_async_copy(far, far_out, fs).wait()


def forward(count, tok, gain, shift, w, bias, spots, freqs, mask, shards):
    rows, width = tok.shape
    half = w.shape[3]
    groups, pairs = len(shards), width // 128
    whole = lambda *s: pl.BlockSpec(s, lambda i: (0,) * len(s))
    at = lambda i: jnp.minimum(i, 5)
    any_spec = pl.BlockSpec(memory_space=pl.ANY)
    sds, vm, dma = jax.ShapeDtypeStruct, pltpu.VMEM, pltpu.SemaphoreType.DMA
    return pl.pallas_call(
        functools.partial(forward_kernel, count, groups, pairs),
        grid=(6 + pairs,),
        out_shape=[
            sds((3, rows, width), low), sds((rows, width), low), sds((rows, width), low),
            sds((rows, 128), f32), sds((2, rows, width), low),
        ]
        + full_shapes(count, shards),
        in_specs=[
            whole(rows, width), whole(1, width), whole(1, width),
            pl.BlockSpec((1, 1, width, half), lambda i: (at(i) % 3, at(i) // 3, 0, 0)),
            pl.BlockSpec((1, 1, half), lambda i: (at(i) % 3, 0, at(i) // 3)),
            whole(rows, 128), whole(1, 128), whole(1, 2 * rows),
        ]
        + [any_spec] * groups,
        out_specs=[
            pl.BlockSpec((1, rows, half), lambda i: (at(i) % 3, 0, at(i) // 3)),
            whole(rows, width),
            pl.BlockSpec((rows, 128), lambda i: (0, jnp.maximum(i - 6, 0))),
            whole(rows, 128), any_spec,
        ]
        + [any_spec] * groups,
        scratch_shapes=[
            vm((rows, width), low), vm((rows, 128), f32), vm((rows, 128), f32),
            vm((3, rows, width), low), vm((2, rows, width), low), vm((2 * rows, 128), low),
            vm((2 * rows, 128), low), dma((4,)), dma((4,)), dma(()),
        ]
        + gather_scratch(count, [a.shape for a in shards]),
        compiler_params=pltpu.CompilerParams(
            vmem_limit_bytes=VMEM_LIMIT, collective_id=3, has_side_effects=True
        ),
        name="forward",
    )(tok, gain, shift, w, bias, spots, freqs, mask, *shards)


def unattend_kernel(count, groups, pairs, *refs):
    q, k, v, kp, vp, mask, lse, grad = refs[:8]
    parts, mixed = refs[8 : 8 + groups], refs[8 + groups]
    dq, dkv, dfar = refs[9 + groups : 12 + groups]
    outs, home = refs[12 + groups : 12 + 2 * groups], refs[12 + 2 * groups]
    keys, vals, dk, dv, *moving = refs[13 + 2 * groups : 21 + 2 * groups]
    begin, steps, end = scatter_job(count, parts, outs, refs[21 + 2 * groups :])
    deliver, delivered = deliver_job(mixed, home, *moving)
    pair = pl.program_id(0)
    rows = q.shape[1]
    chunk = rows // 2

    for n in range(pairs):

        @pl.when(pair == n)
        def _(n=n):
            if n == 0:
                greet(count, corner=True)
                begin()
                deliver()
            for one in share(steps, n, pairs):
                one()

    keys[:rows], keys[rows:] = k[0], kp[0]
    vals[:rows], vals[rows:] = v[0], vp[0]
    lanes = head_lanes(chunk)
    spot = lax.broadcasted_iota(jnp.int32, (chunk, 128), 1)
    for n in range(rows // chunk):
        here = slice(n * chunk, (n + 1) * chunk)
        query = q[0, here] * low(HEAD_DIM**-0.5)
        out_grad = grad[here]
        result = None
        for h in range(2):
            mine = jnp.where(lanes == h, query, low(0))
            mine_grad = jnp.where(lanes == h, out_grad, low(0))
            shift = jnp.sum(jnp.where(spot == 2 * pair + h, lse[here], 0.0), axis=-1, keepdims=True)
            probs = jnp.exp(mm(mine, keys[...], NT) + mask[...] - shift)
            d_probs = mm(mine_grad, vals[...], NT)
            both = probs * d_probs
            inner = jnp.sum(both, axis=-1, keepdims=True)
            d_scores = (both - probs * inner).astype(low)
            got = mm(d_scores, keys[...], NN)
            result = got if h == 0 else jnp.where(lanes == 0, result, got)
            key_part = mm(d_scores, mine, TN)
            value_part = mm(probs.astype(low), mine_grad, TN)
            if n == 0 and h == 0:
                dk[...], dv[...] = key_part, value_part
            else:
                dk[...] += key_part
                dv[...] += value_part
        dq[here] = result * HEAD_DIM**-0.5
    dkv[0], dkv[1] = dk[:rows], dv[:rows]
    dfar[0], dfar[1] = dk[rows:].astype(low), dv[rows:].astype(low)

    @pl.when(pair == pairs - 1)
    def _():
        end()
        delivered()


def unattend(count, qkv, far, mask, lse, grad, parts, mixed):
    _, rows, width = qkv.shape
    keys, groups, pairs = 2 * rows, len(parts), width // 128
    shapes = [p.shape[4:] for p in parts]
    any_spec = pl.BlockSpec(memory_space=pl.ANY)
    at = lambda t: pl.BlockSpec((1, rows, 128), lambda g: (t, 0, g))
    both = pl.BlockSpec((2, rows, 128), lambda g: (0, 0, g))
    column = pl.BlockSpec((rows, 128), lambda g: (0, g))
    whole = lambda *s: pl.BlockSpec(s, lambda g: (0,) * len(s))
    sds, vm = jax.ShapeDtypeStruct, pltpu.VMEM
    return pl.pallas_call(
        functools.partial(unattend_kernel, count, groups, pairs),
        grid=(pairs,),
        out_shape=[
            sds((rows, width), f32), sds((2, rows, width), f32), sds((2, rows, width), low),
        ]
        + [sds(s, f32) for s in shapes]
        + [sds(mixed.shape, low)],
        in_specs=[
            at(0), at(1), at(2), at(0), at(1), whole(1, keys), whole(rows, 128), column,
        ]
        + [any_spec] * (groups + 1),
        out_specs=[column, both, both] + [whole(*s) for s in shapes] + [any_spec],
        scratch_shapes=[vm((keys, 128), low)] * 2
        + [vm((keys, 128), f32)] * 2
        + deliver_scratch(mixed.shape[1:])
        + scatter_scratch(count, shapes),
        compiler_params=pltpu.CompilerParams(
            vmem_limit_bytes=VMEM_LIMIT, collective_id=4, has_side_effects=True
        ),
        name="unattend",
    )(qkv, qkv, qkv, far, far, mask, lse, grad, *parts, mixed)


def unproject_kernel(count, *refs):
    dq, dkv, got, w, spots, freqs, tok, gain, d_resid, h1, p_gu = refs[:11]
    p_qkv, sums, col, r_gu, home = refs[11:16]
    acc, cos, sin, flipped, leaving, *moving = refs[16:25]
    parts, outs = [p_gu.at[0], p_gu.at[1]], [r_gu.at[0], r_gu.at[1]]
    begin, steps, end = scatter_job(count, parts, outs, refs[25:])
    deliver, delivered = deliver_job(leaving, home, *moving)
    step = pl.program_id(0)
    t = lax.rem(step, 3)

    @pl.when(step == 0)
    def _():
        greet(count, corner=True)
        begin()
        cosine, sine = tables(spots[...], freqs[...])
        cos[...] = cosine
        sin[...] = -sine
        flipped[...] = h1[...].T

    for n in range(6):

        @pl.when(step == n)
        def _(n=n):
            for one in share(steps, n, 6):
                one()

    def turned(value):
        parts = [
            turn(value[:, n * 128 : (n + 1) * 128], cos[...], sin[...])
            for n in range(value.shape[1] // 128)
        ]
        return jnp.concatenate(parts, axis=1)

    def use(value):
        rounded = value.astype(low)
        col[0] = jnp.sum(rounded.astype(f32), axis=0, keepdims=True)
        p_qkv[0, 0] = mm(flipped[...], rounded, NN).astype(low)
        part = mm(rounded, w[0, 0], NT)

        @pl.when(step == 0)
        def _():
            acc[...] = part

        @pl.when(step > 0)
        def _():
            acc[...] += part

    @pl.when(t == 0)
    def _():
        use(turned(dq[...]))

    @pl.when(t == 1)
    def _():
        use(turned(dkv[0] + got[0].astype(f32)))

    @pl.when(t == 2)
    def _():
        use(dkv[0] + got[0].astype(f32))

    @pl.when(step == 5)
    def _():
        width = tok.shape[1]
        normed, inverse = normalise(tok[...].astype(f32), width)
        up = acc[...]
        sums[0:1] = jnp.sum(up * normed, axis=0, keepdims=True)
        sums[1:2] = jnp.sum(up, axis=0, keepdims=True)
        scaled = up * gain[...]
        mean = jnp.sum(scaled, axis=-1, keepdims=True) / width
        cross = jnp.sum(scaled * normed, axis=-1, keepdims=True) / width
        result = d_resid[...] + inverse * (scaled - mean - normed * cross)
        for n in range(4):
            leaving[n] = result[n * PAD : (n + 1) * PAD].astype(low)
        deliver()
        end()
        delivered()


def unproject(count, dq, dkv, got, w, spots, freqs, tok, gain, d_resid, h1, p_gu):
    rows, width = tok.shape
    half = w.shape[3]
    whole = lambda *s: pl.BlockSpec(s, lambda i: (0,) * len(s))
    once = lambda *s: pl.BlockSpec(s, lambda i: (0,) * len(s), pipeline_mode=pl.Buffered(1))
    pick = lambda i: (jnp.maximum(i % 3 - 1, 0), 0, i // 3)
    any_spec = pl.BlockSpec(memory_space=pl.ANY)
    shape = p_gu.shape[5:]
    sds, vm = jax.ShapeDtypeStruct, pltpu.VMEM
    return pl.pallas_call(
        functools.partial(unproject_kernel, count),
        grid=(6,),
        out_shape=[
            sds((3, 2, width, half), low), sds((2, width), f32), sds((3, 1, width), f32),
            sds((2,) + shape, f32), sds((4, PAD, width), low),
        ],
        in_specs=[
            pl.BlockSpec((rows, half), lambda i: (0, i // 3)),
            pl.BlockSpec((1, rows, half), pick), pl.BlockSpec((1, rows, half), pick),
            pl.BlockSpec((1, 1, width, half), lambda i: (i % 3, i // 3, 0, 0)),
            once(rows, 128), once(1, 128), once(rows, width), once(1, width),
            once(rows, width), once(rows, width), any_spec,
        ],
        out_specs=[
            pl.BlockSpec((1, 1, width, half), lambda i: (i % 3, i // 3, 0, 0)),
            whole(2, width), pl.BlockSpec((1, 1, half), lambda i: (i % 3, 0, i // 3)),
            whole(2, *shape), any_spec,
        ],
        scratch_shapes=[
            vm((rows, width), f32), vm((rows, 128), f32), vm((rows, 128), f32),
            vm((width, rows), low), vm((4, PAD, width), low),
        ]
        + deliver_scratch((PAD, width))
        + scatter_scratch(count, [shape, shape]),
        compiler_params=pltpu.CompilerParams(
            vmem_limit_bytes=VMEM_LIMIT, collective_id=5, has_side_effects=True
        ),
        name="unproject",
    )(dq, dkv, got, w, spots, freqs, tok, gain, d_resid, h1, p_gu)


SLAB = 32


def in_slabs(rows, body):
    def step(i, carry):
        body(pl.ds(pl.multiple_of(i * SLAB, SLAB), SLAB))
        return carry

    lax.fori_loop(0, rows // SLAB, step, 0)


def fold(values):
    return values[:8] + values[8:16] + values[16:24] + values[24:]


def across(values):
    return jnp.sum(values, axis=-1, keepdims=True)


def down_rows(acc):
    return jnp.sum(acc, axis=0, keepdims=True)


def ffn_kernel(
    count, hidden, part, att, tok, w_out, w_gu, gu_bias, in_gain, in_bias, gain2, shift2, b_out,
    b_down, cot, own, mixed, inner, d_gu, h2, d_resid, g_attn, d_att, wide_sums, thin_sums, grad_out,
    full, resid, gate, up, act, acc, d_in, stats, wide_acc, thin_acc, grad, w_down, ws, gs, gr, gl,
    *scratch,
):
    step = pl.program_id(0)
    rows, width = tok.shape
    wide = in_gain.shape[2]
    half = w_out.shape[2]
    shard = own.shape[0]
    edge = lax.broadcasted_iota(jnp.int32, (SLAB, wide), 1) < part
    cut = wide // 256 * 128
    sides = (slice(0, cut), slice(cut, wide))
    begin, steps, end = gather_job(
        count, [own.at[:, k] for k in sides], [full.at[:, :, :, :, :, k] for k in sides], scratch,
        lambda j: j % 4 == 3,
    )
    b, x, c, y = (lax.axis_index(a) for a in FAR)
    band = rows // 2
    mine = pl.ds(pl.multiple_of(x * band, 16), band)
    theirs = pl.ds(pl.multiple_of((1 - x) * band, 16), band)
    local = pltpu.make_async_copy(cot.at[2 * x + y], grad.at[mine], gl)

    for n in range(7):

        @pl.when(step == n)
        def _(n=n):
            if n == 0:
                greet(count)
                local.start()
                begin()
            for one in share(steps, n, 6) if n < 6 else ():
                one()
            if n == 3:
                push(cot.at[2 * (1 - x) + y], grad.at[mine], gs, gr, place(b, 1 - x, c, y))
            if n == 6:
                end()
                for side in range(2):
                    for k in range(4 * count):
                        block = full.at[side, k // 4, (k // 2) % 2, k % 2]
                        there = w_down.at[side, k * shard : (k + 1) * shard]
                        pltpu.make_async_copy(block, there, ws.at[side]).start()
                local.wait()
                arrived(grad.at[theirs], gr)
                arrived(cot.at[0], gs)

    def at(n):
        return pl.when(step == n)

    @at(0)
    def _():
        acc[...] = mm(att[:, :half], w_out[0], NT)
        wide_acc[...] = jnp.zeros_like(wide_acc)
        thin_acc[...] = jnp.zeros_like(thin_acc)

    @at(1)
    def _():
        acc[...] += mm(att[:, half:], w_out[0], NT)

        def body(s):
            value = tok[s].astype(f32) + acc[s] + b_out[...]
            resid[s] = value
            normed, _ = normalise(value, width)
            h2[s] = (normed * gain2[...] + shift2[...]).astype(low)

        in_slabs(rows, body)

    for n in range(2):

        @at(2 + 2 * n)
        def _(n=n):
            gate[n] = mm(h2[...], w_gu[0], NN) + gu_bias[0]

        @at(3 + 2 * n)
        def _(n=n):
            up[n] = mm(h2[...], w_gu[0], NN) + gu_bias[0]

            def body(s):
                value = gate[n, s]
                out = value * jax.nn.sigmoid(value) * up[n, s]
                act[n, s] = out
                total = across(out)
                stats[0, s] = total if n == 0 else stats[0, s] + total

            in_slabs(rows, body)

    @at(6)
    def _():
        def body(s):
            centre = stats[0, s] / hidden
            total = 0.0
            moved = []
            for n in range(2):
                shifted = jnp.where(edge, act[n, s] - centre, 0.0)
                moved.append(shifted)
                total = total + across(jnp.square(shifted))
            inverse = lax.rsqrt(total / hidden + epsilon)
            stats[1, s] = inverse
            for n in range(2):
                normed = moved[n] * inverse
                act[n, s] = normed
                inner[n, s] = (normed * in_gain[n] + in_bias[n]).astype(low)

        in_slabs(rows, body)

    for n in range(2):

        @at(6 + n)
        def _(n=n):
            arrived(w_down.at[n], ws.at[n])
            out = mm(inner[n], w_down[n], NT)
            if n == 0:
                acc[...] = out
            else:
                acc[...] += out
            d_in[n] = mm(grad[...], w_down[n], NN)

    @at(7)
    def _():
        def first(s):
            mixed[s] = (resid[s] + acc[s] + b_down[...]).astype(low)
            grad_out[s] = grad[s]
            thin_acc[0] += fold(grad[s].astype(f32))

        in_slabs(rows, first)

        def second(s):
            mean, cross = 0.0, 0.0
            kept = []
            for n in range(2):
                value, normed = d_in[n, s], act[n, s]
                wide_acc[n, 0] += fold(value * normed)
                wide_acc[n, 1] += fold(value)
                scaled = value * in_gain[n]
                mean = mean + across(scaled)
                cross = cross + across(scaled * normed)
            mean, cross = mean / hidden, cross / hidden
            for n in range(2):
                normed, value, other = act[n, s], gate[n, s], up[n, s]
                d_act = stats[1, s] * (d_in[n, s] * in_gain[n] - mean - normed * cross)
                sigma = jax.nn.sigmoid(value)
                d_gate = (d_act * other * sigma * (1.0 + value * (1.0 - sigma))).astype(low)
                d_up = (d_act * value * sigma).astype(low)
                wide_acc[n, 2] += fold(d_gate.astype(f32))
                wide_acc[n, 3] += fold(d_up.astype(f32))
                d_gu[n, s, :wide] = d_gate
                d_gu[n, s, wide:] = d_up

        in_slabs(rows, second)
        for n in range(2):
            for k in range(4):
                wide_sums[n, k : k + 1] = down_rows(wide_acc[n, k])

    for n in range(4):

        @at(8 + n)
        def _(n=n):
            out = mm(d_gu[n // 2, :, (n % 2) * wide : (n % 2 + 1) * wide], w_gu[0], NT)
            if n == 0:
                acc[...] = out
            else:
                acc[...] += out

    @at(11)
    def _():
        def body(s):
            value = acc[s]
            normed, inverse = normalise(resid[s], width)
            thin_acc[1] += fold(value * normed)
            thin_acc[2] += fold(value)
            scaled = value * gain2[...]
            mean, cross = across(scaled) / width, across(scaled * normed) / width
            out = grad[s].astype(f32) + inverse * (scaled - mean - normed * cross)
            d_resid[s] = out
            rounded = out.astype(low)
            g_attn[s] = rounded
            thin_acc[3] += fold(rounded.astype(f32))

        in_slabs(rows, body)
        for k in range(4):
            thin_sums[k : k + 1] = down_rows(thin_acc[k])

    for n in range(2):

        @at(12 + n)
        def _(n=n):
            d_att[:, n * half : (n + 1) * half] = mm(g_attn[...], w_out[0], NN).astype(low)


def ffn(
    count, hidden, part, att, tok, w_out, w_gu, gu_bias, in_gain, in_bias, gain2, shift2, b_out,
    b_down, cot, own,
):
    rows, width = tok.shape
    half, wide = w_out.shape[2], w_gu.shape[2] // 2
    whole = lambda *s: pl.BlockSpec(s, lambda i: (0,) * len(s), pipeline_mode=pl.Buffered(1))
    out_at = lambda i: (jnp.where(i < 1, 0, jnp.where(i < 12, 1, jnp.where(i < 13, 0, 1))), 0, 0)
    any_spec = pl.BlockSpec(memory_space=pl.ANY)

    def gu_at(i):
        n = jnp.where(i < 8, jnp.clip(i - 2, 0, 3), jnp.clip(i - 8, 0, 3))
        return n // 2, n % 2

    sds, vm, dma = jax.ShapeDtypeStruct, pltpu.VMEM, pltpu.SemaphoreType.DMA
    shapes = [
        sds((rows, width), low), sds((2, rows, wide), low), sds((2, rows, 2 * wide), low),
        sds((rows, width), low), sds((rows, width), f32), sds((rows, width), low),
        sds((rows, width), low), sds((2, 4, wide), f32), sds((4, width), f32),
        sds((rows, width), low),
    ]
    return pl.pallas_call(
        functools.partial(ffn_kernel, count, hidden, part),
        grid=(14,),
        out_shape=shapes + full_shapes(count, [own]),
        in_specs=[
            whole(rows, width), whole(rows, width),
            pl.BlockSpec((1, width, half), out_at),
            pl.BlockSpec((1, width, wide), lambda i: (gu_at(i)[0], 0, gu_at(i)[1])),
            pl.BlockSpec((1, 1, wide), lambda i: (gu_at(i)[0], 0, gu_at(i)[1])),
            whole(2, 1, wide), whole(2, 1, wide), whole(1, width), whole(1, width),
            whole(1, width), whole(1, width), any_spec, any_spec,
        ],
        out_specs=[whole(*s.shape) for s in shapes] + [any_spec],
        scratch_shapes=[
            vm((rows, width), f32), vm((2, rows, wide), f32), vm((2, rows, wide), f32),
            vm((2, rows, wide), f32), vm((rows, width), f32), vm((2, rows, wide), f32),
            vm((2, rows, 1), f32), vm((2, 4, 8, wide), f32), vm((4, 8, width), f32),
            vm((rows, width), low), vm((2, width, wide), low), dma((2,)), dma(()), dma(()), dma(()),
        ]
        + gather_scratch(
            count, [(own.shape[0], wide // 256 * 128), (own.shape[0], wide - wide // 256 * 128)]
        ),
        compiler_params=pltpu.CompilerParams(
            vmem_limit_bytes=67000000, collective_id=6, has_side_effects=True
        ),
        name="ffn",
    )(att, tok, w_out, w_gu, gu_bias, in_gain, in_bias, gain2, shift2, b_out, b_down, cot, own)


def outer_kernel(left, right, out, flipped):
    @pl.when(pl.program_id(0) == 0)
    def _():
        flipped[...] = left[...].T

    right = right[...] if len(right.shape) == 2 else right[0]
    result = mm(flipped[...], right, NN).astype(low)
    if len(out.shape) == 4:
        out[0, 0] = result
    else:
        out[0] = result


def outer(left, right, steps, right_spec, out_spec, out_shape):
    rows, width = left.shape
    return pl.pallas_call(
        outer_kernel,
        grid=(steps,),
        out_shape=jax.ShapeDtypeStruct(out_shape, low),
        in_specs=[pl.BlockSpec((rows, width), lambda i: (0, 0)), right_spec],
        out_specs=out_spec,
        scratch_shapes=[pltpu.VMEM((width, rows), low)],
        compiler_params=pltpu.CompilerParams(vmem_limit_bytes=VMEM_LIMIT),
        name="outer",
    )(left, right)


def on_device(
    count, tokens, positions, key_mask, norm1_gain, norm1_bias, qkv_weight, qv_bias, out_weight,
    out_bias, norm2_gain, norm2_bias, gate_up_weight, gate_up_bias, inner_gain, inner_bias,
    down_weight, down_bias, cotangent,
):
    b, x, c, y = (lax.axis_index(a) for a in FAR)
    image = 2 * x + y
    local, images, width = tokens.shape
    shard = qkv_weight.shape[0]
    half = qkv_weight.shape[2]
    part = gate_up_weight.shape[2]
    hidden = gate_up_bias.shape[1]
    wide = -(-part // 128) * 128
    more = wide - part
    rows = 4 * PAD

    shards = [
        jnp.swapaxes(qkv_weight.astype(low), 0, 1),
        out_weight.astype(low).T,
        jnp.pad(gate_up_weight.astype(low), ((0, 0), (0, 0), (0, more))).reshape(shard, 2 * wide),
        jnp.pad(down_weight.astype(low).T, ((0, 0), (0, more))),
    ]
    chunks = jnp.pad(jnp.swapaxes(tokens, 0, 1), ((0, 0), (0, PAD - local), (0, 0)))
    cot = jnp.transpose(cotangent.reshape(2, local, images, width), (2, 0, 1, 3))
    cot = jnp.pad(cot, ((0, 0), (0, 0), (0, PAD - local), (0, 0))).reshape(images, 2 * PAD, width)
    spots = jnp.transpose(positions.reshape(2, 2, local, images), (3, 1, 2, 0)).astype(low)
    spots = jnp.pad(spots, ((0, 0), (0, 0), (0, PAD - local), (0, 0)))
    pick = (jnp.arange(128) // 32) % 2
    spots = jnp.where(pick == 0, spots[..., 0:1], spots[..., 1:2])
    join = lambda f: f.reshape(2, width, f.shape[-1])
    w_qkv, tok, spot = gather_first(count, shards[0], chunks, spots)
    w_qkv = w_qkv.reshape(3, 2, width, half)
    tok, spot = tok.reshape(rows, width), spot.reshape(rows, 128)

    live = lax.dynamic_index_in_dim(key_mask, image, 1, keepdims=False)
    live = jnp.pad(live.reshape(2, 2, 2, local), ((0, 0), (0, 0), (0, 0), (0, PAD - local)))
    live = jnp.stack(
        [lax.dynamic_index_in_dim(live, n, 1, keepdims=False).reshape(rows) for n in (c, 1 - c)]
    )
    bias = jnp.where(live > 0, 0.0, masked_score).astype(f32).reshape(1, 2 * rows)

    freqs = jnp.tile(10000.0 ** (-jnp.arange(16).astype(f32) / 16), 8).reshape(1, 128)
    row = lambda a: a.reshape(1, -1)
    qkv_bias = jnp.stack([qv_bias[0], jnp.zeros_like(qv_bias[0]), qv_bias[1]])[:, None]
    swap = ((0, 1), (1, 0))
    qkv, h1, attended, lse, far, *full = forward(
        count, tok, row(norm1_gain), row(norm1_bias), w_qkv, qkv_bias, spot, freqs, bias, shards[1:3]
    )
    w_out, w_gu = (join(f) for f in full)

    split = lambda a: jnp.pad(a.reshape(a.shape[:-1] + (2, part)), ((0, 0),) * a.ndim + ((0, more),))
    gu_bias = jnp.swapaxes(split(gate_up_bias), 0, 1).reshape(2, 1, 2 * wide)
    mixed, inner, d_gu, h2, d_resid, g_attn, d_attended, wide_sums, thin_sums, grad, _ = ffn(
        count, hidden, part, attended, tok, w_out, w_gu, gu_bias, split(inner_gain)[:, None],
        split(inner_bias)[:, None], row(norm2_gain), row(norm2_bias), row(out_bias), row(down_bias),
        cot, shards[3],
    )
    by_owner = lambda a: a.reshape(a.shape[:-2] + (count, 2, 2, shard, a.shape[-1]))
    p_down = by_owner(
        outer(
            grad, inner, 2, pl.BlockSpec((1, rows, wide), lambda i: (i, 0, 0)),
            pl.BlockSpec((1, width, wide), lambda i: (i, 0, 0)), (2, width, wide),
        )
    )
    p_out = by_owner(
        outer(
            g_attn, attended, 2, pl.BlockSpec((rows, half), lambda i: (0, i)),
            pl.BlockSpec((1, width, half), lambda i: (i, 0, 0)), (2, width, half),
        )
    )
    p_gu = by_owner(
        outer(
            h2, d_gu, 4, pl.BlockSpec((1, rows, wide), lambda i: (i % 2, 0, i // 2)),
            pl.BlockSpec((1, 1, width, wide), lambda i: (i // 2, i % 2, 0, 0)),
            (2, 2, width, wide),
        )
    )
    dq, dkv, dfar, r_down, r_out, mixed_home = unattend(
        count, qkv, far, bias, lse, d_attended, [p_down, p_out], mixed.reshape(4, PAD, width)
    )
    got = lax.ppermute(dfar, "core", swap)
    p_qkv, sums1, col, r_gu, d_tok_home = unproject(
        count, dq, dkv, got, w_qkv, spot, freqs, tok, row(norm1_gain), d_resid, h1, p_gu
    )

    merge = lambda a: a[..., :part].reshape(a.shape[:-2] + (hidden,))
    d_gu_bias = merge(jnp.swapaxes(wide_sums[:, 2:], 0, 1))
    d_in_gain, d_in_bias = wide_sums[:, 0], wide_sums[:, 1]
    d_down_bias, d_gain2, d_bias2, d_out_bias = (thin_sums[n] for n in range(4))
    vectors = [
        sums1[0], sums1[1], jnp.stack([col[0, 0], col[2, 0]]), d_out_bias, d_gain2, d_bias2,
        d_gu_bias, merge(d_in_gain), merge(d_in_bias), d_down_bias,
    ]
    flat = jnp.concatenate([v.reshape(-1) for v in vectors])
    size = flat.shape[0]
    lines = -(-size // 2048) * 16
    flat = jnp.pad(flat, (0, lines * 128 - size)).reshape(lines, 128)
    r_qkv, summed = last(count, by_owner(p_qkv), flat, 1)
    summed = summed.reshape(-1)
    pieces, at = [], 0
    for v in vectors:
        pieces.append(summed[at : at + v.size].reshape(v.shape))
        at += v.size

    home = lambda landed: jnp.swapaxes(landed[:, :local], 0, 1)

    return (
        home(mixed_home), home(d_tok_home), pieces[0], pieces[1], jnp.swapaxes(r_qkv, 0, 1), pieces[2],
        r_out.T, pieces[3], pieces[4], pieces[5], jnp.swapaxes(r_gu[:, :, :part], 0, 1),
        pieces[6], pieces[7], pieces[8], r_down[:, :part].T, pieces[9],
    )


def solution(mesh):
    count, ctx, tensor = (mesh.shape[a] for a in ("batch", "ctx", "tensor"))
    fine = jax.sharding.Mesh(mesh.devices.reshape(count, ctx // 2, 2, tensor), FAR)
    ctx, wide = ("x", "core"), ("batch", "x", "core")
    return jax.shard_map(
        functools.partial(on_device, count),
        mesh=fine,
        in_specs=(
            P(("x", "core", "tensor"), "batch", None), P(None, ctx, "batch"), P(None, "batch"),
            P(), P(), P(wide, None, "tensor"), P(), P("tensor", wide), P(), P(), P(),
            P(wide, None, "tensor"), P(), P(), P(), P("tensor", wide), P(), P(ctx, "batch", None),
        ),
        out_specs=(
            P(("x", "core", "tensor"), "batch", None), P(("x", "core", "tensor"), "batch", None),
            P(), P(), P(wide, None, "tensor"), P(), P("tensor", wide), P(), P(), P(),
            P(wide, None, "tensor"), P(), P(), P(), P("tensor", wide), P(),
        ),
        check_vma=False,
    )
```

```python
import functools

import jax
import jax.numpy as jnp
from jax import lax
from jax.experimental import pallas as pl
from jax.experimental.pallas import tpu as pltpu

from jax.sharding import PartitionSpec as P
MESH = pl.DeviceIdType.MESH
FAR = ("batch", "x", "core", "tensor")


def place(b, x, c, y):
    return {"batch": b, "x": x, "core": c, "tensor": y}


def ring_offsets(count):
    order = [0]
    for step in range(1, count // 2 + 1):
        for off in (step, count - step):
            if off not in order:
                order.append(off)
    return order


def greet(count, corner=False):
    b, x, c, y = (lax.axis_index(a) for a in FAR)
    barrier = pltpu.get_barrier_semaphore()
    for off in range(1, count):
        pl.semaphore_signal(
            barrier, inc=1, device_id=place(lax.rem(b + off, count), x, c, y), device_id_type=MESH
        )
    near = [place(b, 1 - x, c, y), place(b, x, c, 1 - y), place(b, x, 1 - c, y)]
    if corner:
        near.append(place(b, 1 - x, c, 1 - y))
    for there in near:
        pl.semaphore_signal(barrier, inc=1, device_id=there, device_id_type=MESH)
    pl.semaphore_wait(barrier, count - 1 + len(near))


def push(src, dst, s, r, there):
    pltpu.make_async_remote_copy(
        src_ref=src, dst_ref=dst, send_sem=s, recv_sem=r, device_id=there, device_id_type=MESH
    ).start()


def arrived(dst, sem):
    pltpu.make_async_copy(dst, dst, sem).wait()


def bounce(src, via, dst, sems):
    inward = pltpu.make_async_copy(src, via, sems.at[0])
    outward = pltpu.make_async_copy(via, dst, sems.at[1])

    def turn_round():
        inward.wait()
        outward.start()

    return inward.start, turn_round, outward.wait


def gather_scratch(count, shapes):
    groups = len(shapes)
    dma = pltpu.SemaphoreType.DMA
    many, one = dma((groups, count)), dma((groups,))
    sems = [one, many, one, many, one, many, one, one, many, one, one, dma((groups, 2))]
    return sems + [pltpu.VMEM(s, jnp.bfloat16) for s in shapes]


def gather_job(count, own, full, sems, by_x=lambda j: j % 2 == 1):
    groups = len(own)
    zs, zr, xs, xr, ys, yr, xds, yds, dr, cs, cr, ls, *vias = sems
    b, x, c, y = (lax.axis_index(a) for a in FAR)
    xn, yn, cn = place(b, 1 - x, c, y), place(b, x, c, 1 - y), place(b, x, 1 - c, y)
    offsets = ring_offsets(count)

    def block(g, yy, item, xx, cc):
        return full[g].at[yy, lax.rem(b + offsets[item], count), xx, cc]

    copies = [
        bounce(own[g], vias[g], full[g].at[y, b, x, c], ls.at[g]) for g in range(groups)
    ]

    def begin():
        for g in range(groups):
            for j in range(1, count):
                there = place(lax.rem(b + count - offsets[j], count), x, c, y)
                push(own[g], full[g].at[y, b, x, c], zs.at[g], zr.at[g, j], there)
            copies[g][0]()

    def column(g, j):
        dst = block(g, y, j, x, c)
        if j > 0:
            arrived(dst, zr.at[g, j])
        src = own[g] if j == 0 else dst
        push(src, dst, xs.at[g], xr.at[g, j], xn)
        push(src, dst, ys.at[g], yr.at[g, j], yn)
        push(src, dst, cs.at[g], cr.at[g], cn)

    def plane(g, j):
        from_x, from_y = block(g, y, j, 1 - x, c), block(g, 1 - y, j, x, c)
        arrived(from_x, xr.at[g, j])
        if not by_x(j):
            push(from_x, from_x, yds.at[g], dr.at[g, j], yn)
        push(from_x, from_x, cs.at[g], cr.at[g], cn)
        arrived(from_y, yr.at[g, j])
        if by_x(j):
            push(from_y, from_y, xds.at[g], dr.at[g, j], xn)
        push(from_y, from_y, cs.at[g], cr.at[g], cn)

    def corner(g, j):
        there = block(g, 1 - y, j, 1 - x, c)
        arrived(there, dr.at[g, j])
        push(there, there, cs.at[g], cr.at[g], cn)

    items = [(g, 0) for g in range(groups)]
    items += [(g, j) for g in range(groups) for j in range(1, count)]
    lag = min(3, max(1, len(items) // 4))

    def stage(t):
        if t < len(items):
            column(*items[t])
        if 0 <= t - lag < len(items):
            plane(*items[t - lag])
        if t - 2 * lag >= 0:
            corner(*items[t - 2 * lag])
        if t == 1:
            for copy in copies:
                copy[1]()

    def end():
        for g in range(groups):
            copies[g][2]()
            arrived(full[g].at[:, :, :, 1 - c], cr.at[g])
            arrived(full[g].at[:, :, :, 0], cs.at[g])
            arrived(full[g].at[0, : count - 1, 0, 0], zs.at[g])
            arrived(full[g].at[0, :, 0, 0], xs.at[g])
            arrived(full[g].at[0, :, 0, 0], ys.at[g])
            xd = sum(1 for j in range(count) if by_x(j))
            if xd:
                arrived(full[g].at[0, :xd, 0, 0], xds.at[g])
            if xd < count:
                arrived(full[g].at[0, : count - xd, 0, 0], yds.at[g])

    return begin, [functools.partial(stage, t) for t in range(len(items) + 2 * lag)], end


def full_shapes(count, shards):
    return [jax.ShapeDtypeStruct((2, count, 2, 2) + s.shape, s.dtype) for s in shards]


def gather_kernel(count, groups, *refs):
    own = [refs[0].at[n] for n in range(groups)]
    tokens, spots = refs[1:3]
    full = [refs[3].at[n] for n in range(groups)]
    landed = refs[4:6]
    *sems, ts, tr, tl, via_t, via_s = refs[6:]
    b, x, c, y = (lax.axis_index(a) for a in FAR)
    begin, steps, end = gather_job(count, own, full, sems)
    image = 2 * x + y
    far = 2 * (1 - x) + y
    corners = ((1, 0), (0, 1), (1, 1))
    greet(count, corner=True)
    for n, (ox, oy) in enumerate(corners):
        px, py = (1 - x if ox else x), (1 - y if oy else y)
        push(
            tokens.at[2 * px + py], landed[0].at[image], ts.at[n], tr.at[n], place(b, px, c, py)
        )
    begin()
    xn = place(b, 1 - x, c, y)
    push(spots.at[far], landed[1].at[x], ts.at[3], tr.at[3], xn)
    homes = [
        bounce(tokens.at[image], via_t, landed[0].at[image], tl.at[0]),
        bounce(spots.at[image], via_s, landed[1].at[x], tl.at[1]),
    ]
    for copy in homes:
        copy[0]()
    for n, step in enumerate(steps):
        step()
        if n == 1:
            for copy in homes:
                copy[1]()
    end()
    for n, (ox, oy) in enumerate(corners):
        px, py = (1 - x if ox else x), (1 - y if oy else y)
        arrived(landed[0].at[2 * px + py], tr.at[n])
        arrived(tokens.at[0], ts.at[n])
    arrived(landed[1].at[1 - x], tr.at[3])
    arrived(spots.at[0], ts.at[3])
    for copy in homes:
        copy[2]()


def gather_first(count, shards, tokens, spots):
    groups = shards.shape[0]
    any_spec = pl.BlockSpec(memory_space=pl.ANY)
    dma = pltpu.SemaphoreType.DMA
    outs = [
        jax.ShapeDtypeStruct((groups, 2, count, 2, 2) + shards.shape[1:], shards.dtype),
        jax.ShapeDtypeStruct(tokens.shape, tokens.dtype),
        jax.ShapeDtypeStruct((2,) + spots.shape[1:], spots.dtype),
    ]
    return pl.pallas_call(
        functools.partial(gather_kernel, count, groups),
        out_shape=outs,
        in_specs=[any_spec] * 3,
        out_specs=[any_spec] * 3,
        scratch_shapes=gather_scratch(count, [shards.shape[1:]] * groups)
        + [dma((4,)), dma((4,)), dma((2, 2))]
        + [pltpu.VMEM(a.shape[1:], a.dtype) for a in (tokens, spots)],
        compiler_params=pltpu.CompilerParams(collective_id=0, has_side_effects=True),
        name="gather_first",
    )(shards, tokens, spots)


def scatter_scratch(count, shapes):
    groups = len(shapes)
    dma = pltpu.SemaphoreType.DMA
    scratch = [pltpu.VMEM((2, count, 2) + s, jnp.bfloat16) for s in shapes] * 2
    scratch += [pltpu.VMEM((count,) + s, jnp.bfloat16) for s in shapes] * 4
    many, one = dma((groups, count)), dma((groups,))
    return scratch + [many, one, many, one, many, one, many, one, one, many, one, many]


def scatter_job(count, parts, outs, scratch):
    groups = len(parts)
    held, peer, from_x, from_y, from_d, from_z = (
        scratch[k * groups : (k + 1) * groups] for k in range(6)
    )
    ls, cs, cr, xs, xr, ys, yr, xds, yds, dr, zs, zr = scratch[6 * groups :]
    b, x, c, y = (lax.axis_index(a) for a in FAR)
    xn, yn, cn = place(b, 1 - x, c, y), place(b, x, c, 1 - y), place(b, x, 1 - c, y)
    offsets = ring_offsets(count)
    order = list(range(1, count)) + [0]
    rows = held[0].shape[3]
    chunk = min(rows, 16)

    def add_to(target, *others):
        def body(i, carry):
            at_rows = pl.ds(pl.multiple_of(i * chunk, chunk), chunk)
            total = target[at_rows]
            for other in others:
                total = total + other[at_rows]
            target[at_rows] = total
            return carry

        lax.fori_loop(0, rows // chunk, body, 0)

    def where_to(j):
        return lax.rem(b + offsets[j], count)

    items = [(g, j) for g in range(groups) for j in order]

    def begin(*which):
        for g, j in items:
            if which and g not in which:
                continue
            bb = where_to(j)
            push(parts[g].at[:, bb, :, 1 - c], peer[g].at[:, bb], cs.at[g], cr.at[g, j], cn)
            pltpu.make_async_copy(
                parts[g].at[:, bb, :, c], held[g].at[:, bb], ls.at[g, j]
            ).start()

    def merge_core(g, j):
        bb = where_to(j)
        arrived(held[g].at[:, bb], ls.at[g, j])
        arrived(peer[g].at[:, bb], cr.at[g, j])
        for yy, xx in ((1 - y, 1 - x), (y, 1 - x), (1 - y, x), (y, x)):
            add_to(held[g].at[yy, bb, xx], peer[g].at[yy, bb, xx])

    def send_corner(g, j):
        src = held[g].at[1 - y, where_to(j), 1 - x]
        if j % 2 == 0:
            push(src, from_d[g].at[j], xds.at[g], dr.at[g, j], xn)
        else:
            push(src, from_d[g].at[j], yds.at[g], dr.at[g, j], yn)

    def merge_corner(g, j):
        bb = where_to(j)
        arrived(from_d[g].at[j], dr.at[g, j])
        if j % 2 == 0:
            add_to(held[g].at[1 - y, bb, x], from_d[g].at[j])
        else:
            add_to(held[g].at[y, bb, 1 - x], from_d[g].at[j])

    def send_plane(g, j, by_x):
        bb = where_to(j)
        if by_x:
            push(held[g].at[y, bb, 1 - x], from_x[g].at[j], xs.at[g], xr.at[g, j], xn)
        else:
            push(held[g].at[1 - y, bb, x], from_y[g].at[j], ys.at[g], yr.at[g, j], yn)

    def merge_plane(g, j):
        arrived(from_x[g].at[j], xr.at[g, j])
        arrived(from_y[g].at[j], yr.at[g, j])
        add_to(held[g].at[y, where_to(j), x], from_x[g].at[j], from_y[g].at[j])

    def send_column(g, j):
        if j > 0:
            bb = where_to(j)
            push(
                held[g].at[y, bb, x], from_z[g].at[j], zs.at[g], zr.at[g, j], place(bb, x, c, y)
            )

    total = len(items)
    lag = min(3, max(1, total // 4))

    def stage(t):
        now = items[t] if t < total else None
        one = items[t - lag] if 0 <= t - lag < total else None
        two = items[t - 2 * lag] if t - 2 * lag >= 0 else None
        if two:
            merge_plane(*two)
        if one:
            merge_corner(*one)
        if now:
            merge_core(*now)
            send_corner(*now)
            send_plane(*now, now[1] % 2 == 0)
        if one:
            send_plane(*one, one[1] % 2 == 1)
        if two:
            send_column(*two)

    def end():
        for g in range(groups):
            for j in range(1, count):
                arrived(from_z[g].at[j], zr.at[g, j])

            def body(i, carry, g=g):
                at_rows = pl.ds(pl.multiple_of(i * chunk, chunk), chunk)
                result = held[g][y, b, x, at_rows].astype(jnp.float32)
                for j in range(1, count):
                    result = result + from_z[g][j, at_rows].astype(jnp.float32)
                outs[g][at_rows] = result
                return carry

            lax.fori_loop(0, rows // chunk, body, 0)
            arrived(peer[g], cs.at[g])
            arrived(from_x[g], xs.at[g])
            arrived(from_y[g], ys.at[g])
            arrived(from_d[g].at[: (count + 1) // 2], xds.at[g])
            arrived(from_d[g].at[: count // 2], yds.at[g])
            arrived(from_z[g].at[1:], zs.at[g])

    return begin, [functools.partial(stage, t) for t in range(total + 2 * lag)], end


CORNERS = ((1, 0), (0, 1), (1, 1))


def deliver_job(leaving, landed, ts, tr, tl, via):
    b, x, c, y = (lax.axis_index(a) for a in FAR)
    image = 2 * x + y
    copy = bounce(leaving.at[image], via, landed.at[image], tl)

    def begin():
        copy[0]()
        for n, (ox, oy) in enumerate(CORNERS):
            px, py = (1 - x if ox else x), (1 - y if oy else y)
            there = place(b, px, c, py)
            push(leaving.at[2 * px + py], landed.at[image], ts.at[n], tr.at[n], there)

    def end():
        copy[1]()
        copy[2]()
        for n, (ox, oy) in enumerate(CORNERS):
            px, py = (1 - x if ox else x), (1 - y if oy else y)
            arrived(landed.at[2 * px + py], tr.at[n])
            arrived(leaving.at[0], ts.at[n])

    return begin, end


def deliver_scratch(shape):
    dma = pltpu.SemaphoreType.DMA
    return [dma((3,)), dma((3,)), dma((2,)), pltpu.VMEM(shape, jnp.bfloat16)]


def share(todo, step, total):
    return todo[step * len(todo) // total : (step + 1) * len(todo) // total]


def sum_scratch(count, shape):
    half = (shape[0] // 2, shape[1])
    dma, vm = pltpu.SemaphoreType.DMA, pltpu.VMEM
    return [
        vm((3,) + half, jnp.float32), vm(half, jnp.float32), vm(half, jnp.float32),
        vm((count,) + half, jnp.float32), vm(shape, jnp.float32), dma((4,)), dma((4,)), dma(()),
        dma((count,)),
    ]


def sum_job(count, v_ref, o_ref, scratch):
    got, lane, plane, slots, final, ss, rs, zs, zr = scratch
    b, x, c, y = (lax.axis_index(a) for a in FAR)
    xn, yn, cn = place(b, 1 - x, c, y), place(b, x, c, 1 - y), place(b, x, 1 - c, y)
    half = v_ref.shape[0] // 2
    mine = pl.ds(pl.multiple_of(c * half, 8), half)
    theirs = pl.ds(pl.multiple_of((1 - c) * half, 8), half)

    def swap(src, dst, n, there):
        return pltpu.make_async_remote_copy(
            src_ref=src, dst_ref=dst, send_sem=ss.at[n], recv_sem=rs.at[n], device_id=there,
            device_id_type=MESH,
        )

    swaps = (
        lambda: swap(v_ref.at[theirs], got.at[0], 0, cn),
        lambda: swap(lane, got.at[1], 1, xn),
        lambda: swap(plane, got.at[2], 2, yn),
        lambda: swap(final.at[mine], final.at[mine], 3, cn),
    )

    def one():
        swaps[0]().start()

    def two():
        swaps[0]().wait()
        lane[...] = v_ref[mine] + got[0]
        swaps[1]().start()

    def three():
        swaps[1]().wait()
        plane[...] = lane[...] + got[1]
        swaps[2]().start()

    def four():
        swaps[2]().wait()
        slots[b] = plane[...] + got[2]
        for off in range(1, count):
            pltpu.make_async_remote_copy(
                src_ref=slots.at[b], dst_ref=slots.at[b], send_sem=zs, recv_sem=zr.at[off],
                device_id=place(lax.rem(b + off, count), x, c, y), device_id_type=MESH,
            ).start()

    def five():
        for off in range(1, count):
            there = slots.at[lax.rem(b + count - off, count)]
            pltpu.make_async_copy(there, there, zr.at[off]).wait()
        total = slots[0]
        for n in range(1, count):
            total = total + slots[n]
        final[mine] = total
        swaps[3]().start()

    def six():
        swaps[3]().wait()
        o_ref[...] = final[...]
        rest = slots.at[: count - 1]
        pltpu.make_async_copy(rest, rest, zs).wait()

    return [one, two, three, four, five, six]


PAD = 136
WIDTH_TILE = 128
HEAD_DIM = 64
epsilon = 1e-06
masked_score = -1e30
f32, low = jnp.float32, jnp.bfloat16
VMEM_LIMIT = 60000000


def mm(a, b, dims):
    return lax.dot_general(a, b, (dims, ((), ())), preferred_element_type=f32)


NN = ((1,), (0,))
NT = ((1,), (1,))
TN = ((0,), (0,))


def normalise(values, width):
    centre = jnp.sum(values, axis=-1, keepdims=True) / width
    shifted = values - centre
    spread = jnp.sum(jnp.square(shifted), axis=-1, keepdims=True) / width
    inverse = lax.rsqrt(spread + epsilon)
    return shifted * inverse, inverse


def turn(values, cosine, sine):
    lane = lax.broadcasted_iota(jnp.int32, values.shape, 1)
    other = jnp.where((lane // 16) % 2 == 0, pltpu.roll(values, 112, 1), pltpu.roll(values, 16, 1))
    return values * cosine + other * sine


def tables(spots, freqs):
    angles = spots.astype(f32) * freqs
    lane = lax.broadcasted_iota(jnp.int32, angles.shape, 1)
    sine = jnp.sin(angles)
    return jnp.cos(angles), jnp.where((lane // 16) % 2 == 0, -sine, sine)


def head_lanes(rows):
    return lax.broadcasted_iota(jnp.int32, (rows, 128), 1) // HEAD_DIM


def forward_kernel(count, groups, pairs, *refs):
    tok, gain, shift, w, w_bias, spots, freqs, mask = refs[:8]
    own = refs[8 : 8 + groups]
    out, h1, att, lse, far_out = refs[8 + groups : 13 + groups]
    full = refs[13 + groups : 13 + 2 * groups]
    hid, cos, sin, kept, far, keys, vals, ks, kr, fs = refs[13 + 2 * groups : 23 + 2 * groups]
    begin, steps, end = gather_job(count, own, full, refs[23 + 2 * groups :])
    step = pl.program_id(0)
    rows = tok.shape[0]
    half = w.shape[3]
    b, x, c, y = (lax.axis_index(a) for a in FAR)
    cn = place(b, x, 1 - c, y)
    total = 6 + pairs

    def kv(n):
        t, side = n % 2, n // 2
        return t, slice(side * half, (side + 1) * half)

    @pl.when(step == 0)
    def _():
        greet(count)
        begin()
        normed, _ = normalise(tok[...].astype(f32), tok.shape[1])
        hid[...] = (normed * gain[...] + shift[...]).astype(low)
        h1[...] = hid[...]
        lse[...] = jnp.zeros_like(lse)
        cosine, sine = tables(spots[...], freqs[...])
        cos[...] = cosine
        sin[...] = sine

    for s in range(total):
        todo = steps[s * len(steps) // total : (s + 1) * len(steps) // total]
        done = s - 1
        sent = 2 * (done // 3) + done % 3 - 1 if 0 <= done < 6 and done % 3 > 0 else None

        @pl.when(step == s)
        def _(s=s, todo=todo, sent=sent):
            if sent is not None:
                t, lanes = kv(sent)
                push(kept.at[1 + t, :, lanes], far.at[t, :, lanes], ks.at[sent], kr.at[sent], cn)
            for one in todo:
                one()
            if s in (6, 6 + pairs // 2):
                for n in range(2) if s == 6 else range(2, 4):
                    t, lanes = kv(n)
                    arrived(far.at[t, :, lanes], kr.at[n])
            if s == total - 1:
                pltpu.make_async_copy(far, far_out, fs).start()

    for n in range(6):

        @pl.when(step == n)
        def _(n=n):
            t, lanes = n % 3, slice((n // 3) * half, (n // 3 + 1) * half)
            acc = mm(hid[...], w[0, 0], NN) + w_bias[0]
            if t < 2:
                parts = [
                    turn(acc[:, k : k + 128], cos[...], sin[...]).astype(low)
                    for k in range(0, half, 128)
                ]
                result = jnp.concatenate(parts, axis=1)
            else:
                result = acc.astype(low)
            out[0] = result
            kept[t, :, lanes] = result

    @pl.when(step >= 6)
    def _():
        pair = step - 6
        mine_lanes = pl.ds(pl.multiple_of(pair * 128, 128), 128)
        keys[:rows], keys[rows:] = kept[1, :, mine_lanes], far[0, :, mine_lanes]
        vals[:rows], vals[rows:] = kept[2, :, mine_lanes], far[1, :, mine_lanes]
        chunk = rows // 2
        lanes = head_lanes(chunk)
        spot = lax.broadcasted_iota(jnp.int32, (chunk, 128), 1)
        for n in range(rows // chunk):
            here = slice(n * chunk, (n + 1) * chunk)
            query = kept[0, here, mine_lanes] * low(HEAD_DIM**-0.5)
            result = None
            marks = lse[here]
            for h in range(2):
                mine = jnp.where(lanes == h, query, low(0))
                scores = mm(mine, keys[...], NT) + mask[...]
                top = jnp.max(scores, axis=-1, keepdims=True)
                weight = jnp.exp(scores - top)
                sums = jnp.sum(weight, axis=-1, keepdims=True)
                probs = (weight * (1.0 / sums)).astype(low)
                got = mm(probs, vals[...], NN)
                result = got if h == 0 else jnp.where(lanes == 0, result, got)
                marks = jnp.where(spot == 2 * pair + h, top + jnp.log(sums), marks)
            lse[here] = marks
            att[here] = result.astype(low)

    @pl.when(step == total - 1)
    def _():
        end()
        for n in range(4):
            t, lanes = kv(n)
            arrived(kept.at[1 + t, :, lanes], ks.at[n])
        pltpu.make_async_copy(far, far_out, fs).wait()


def forward(count, tok, gain, shift, w, bias, spots, freqs, mask, shards):
    rows, width = tok.shape
    half = w.shape[3]
    groups, pairs = len(shards), width // 128
    whole = lambda *s: pl.BlockSpec(s, lambda i: (0,) * len(s))
    at = lambda i: jnp.minimum(i, 5)
    any_spec = pl.BlockSpec(memory_space=pl.ANY)
    sds, vm, dma = jax.ShapeDtypeStruct, pltpu.VMEM, pltpu.SemaphoreType.DMA
    return pl.pallas_call(
        functools.partial(forward_kernel, count, groups, pairs),
        grid=(6 + pairs,),
        out_shape=[
            sds((3, rows, width), low), sds((rows, width), low), sds((rows, width), low),
            sds((rows, 128), f32), sds((2, rows, width), low),
        ]
        + full_shapes(count, shards),
        in_specs=[
            whole(rows, width), whole(1, width), whole(1, width),
            pl.BlockSpec((1, 1, width, half), lambda i: (at(i) % 3, at(i) // 3, 0, 0)),
            pl.BlockSpec((1, 1, half), lambda i: (at(i) % 3, 0, at(i) // 3)),
            whole(rows, 128), whole(1, 128), whole(1, 2 * rows),
        ]
        + [any_spec] * groups,
        out_specs=[
            pl.BlockSpec((1, rows, half), lambda i: (at(i) % 3, 0, at(i) // 3)),
            whole(rows, width),
            pl.BlockSpec((rows, 128), lambda i: (0, jnp.maximum(i - 6, 0))),
            whole(rows, 128), any_spec,
        ]
        + [any_spec] * groups,
        scratch_shapes=[
            vm((rows, width), low), vm((rows, 128), f32), vm((rows, 128), f32),
            vm((3, rows, width), low), vm((2, rows, width), low), vm((2 * rows, 128), low),
            vm((2 * rows, 128), low), dma((4,)), dma((4,)), dma(()),
        ]
        + gather_scratch(count, [a.shape for a in shards]),
        compiler_params=pltpu.CompilerParams(
            vmem_limit_bytes=VMEM_LIMIT, collective_id=3, has_side_effects=True
        ),
        name="forward",
    )(tok, gain, shift, w, bias, spots, freqs, mask, *shards)


def unattend_kernel(count, pairs, *refs):
    q, k, v, kp, vp, mask, lse, grad, down_left, out_left, gu_left = refs[:11]
    inner, att, d_gu, mixed, early = refs[11:16]
    dq, dkv, dfar, r_down, r_out, r_gate, summed = refs[16:23]
    home, p_down, p_out, p_gate, p_up = refs[23:28]
    keys, vals, dk, dv, flipped, stage, stored, *moving = refs[28:39]
    parts, outs = [p_down, p_out, p_gate], [r_down, r_out, r_gate]
    begin, steps, end = scatter_job(count, parts, outs, refs[39:-11])
    early_here, early_sem = refs[-11:-9]
    adds = sum_job(count, early_here, summed, refs[-9:])
    fetch = pltpu.make_async_copy(early, early_here, early_sem)
    deliver, delivered = deliver_job(mixed, home, *moving)
    step = pl.program_id(0)
    rows = q.shape[1]
    chunk = rows // 2
    half = att.shape[1]
    shard = r_down.shape[0]
    outers = 8
    targets = [(p, y) for p in (p_down, p_out, p_gate, p_up) for y in range(2)]

    def store(n):
        target, side = targets[n]
        columns = target.shape[-1]
        for block in range(4 * count):
            pltpu.make_async_copy(
                stage.at[n % 2, block * shard : (block + 1) * shard, :columns],
                target.at[side, block // 4, (block // 2) % 2, block % 2],
                stored.at[n],
            ).start()

    def settle(n):
        arrived(targets[n][0].at[0], stored.at[n])

    for n in range(outers + pairs):

        @pl.when(step == n)
        def _(n=n):
            if n == 0:
                greet(count, corner=True)
                deliver()
                fetch.start()
            if n == 4:
                fetch.wait()
            if 2 <= n < outers + 2:
                settle(n - 2)
            if n in (3, 5, 7):
                begin((n - 3) // 2)
            for one in share(steps, n - 4, outers + pairs - 4) if n >= 4 else ():
                one()
            for one in share(adds, n - 4, outers + pairs - 4) if n >= 4 else ():
                one()
            if n < outers:
                if n % 2 == 0 and n < 6:
                    flipped[...] = (down_left, out_left, gu_left)[n // 2][...].T
                right = inner[0] if n < 2 else att[...] if n < 4 else d_gu[0]
                result = mm(flipped[...], right, NN).astype(low)
                stage[n % 2, :, : result.shape[1]] = result
                store(n)

    @pl.when(step >= outers)
    def _():
        pair = step - outers
        keys[:rows], keys[rows:] = k[0], kp[0]
        vals[:rows], vals[rows:] = v[0], vp[0]
        lanes = head_lanes(chunk)
        spot = lax.broadcasted_iota(jnp.int32, (chunk, 128), 1)
        for n in range(rows // chunk):
            here = slice(n * chunk, (n + 1) * chunk)
            query = q[0, here] * low(HEAD_DIM**-0.5)
            out_grad = grad[here]
            result = None
            for h in range(2):
                mine = jnp.where(lanes == h, query, low(0))
                mine_grad = jnp.where(lanes == h, out_grad, low(0))
                shift = jnp.sum(
                    jnp.where(spot == 2 * pair + h, lse[here], 0.0), axis=-1, keepdims=True
                )
                probs = jnp.exp(mm(mine, keys[...], NT) + mask[...] - shift)
                d_probs = mm(mine_grad, vals[...], NT)
                both = probs * d_probs
                inside = jnp.sum(both, axis=-1, keepdims=True)
                d_scores = (both - probs * inside).astype(low)
                got = mm(d_scores, keys[...], NN)
                result = got if h == 0 else jnp.where(lanes == 0, result, got)
                key_part = mm(d_scores, mine, TN)
                value_part = mm(probs.astype(low), mine_grad, TN)
                if n == 0 and h == 0:
                    dk[...], dv[...] = key_part, value_part
                else:
                    dk[...] += key_part
                    dv[...] += value_part
            dq[here] = result * HEAD_DIM**-0.5
        dkv[0], dkv[1] = dk[:rows], dv[:rows]
        dfar[0], dfar[1] = dk[rows:].astype(low), dv[rows:].astype(low)

    @pl.when(step == outers + pairs - 1)
    def _():
        end()
        delivered()


def unattend(count, shard, qkv, far, mask, lse, grad, lefts, inner, attended, d_gu, mixed, early):
    _, rows, width = qkv.shape
    keys, pairs = 2 * rows, width // 128
    wide, half = inner.shape[2], width // 2
    any_spec = pl.BlockSpec(memory_space=pl.ANY)
    pair = lambda i: jnp.maximum(i - 8, 0)
    at = lambda t: pl.BlockSpec((1, rows, 128), lambda i: (t, 0, pair(i)))
    both = pl.BlockSpec((2, rows, 128), lambda i: (0, 0, pair(i)))
    column = pl.BlockSpec((rows, 128), lambda i: (0, pair(i)))
    once = lambda *s: pl.BlockSpec(s, lambda i: (0,) * len(s), pipeline_mode=pl.Buffered(1))
    gu = lambda i: jnp.clip(i - 4, 0, 3)
    sds, vm, dma = jax.ShapeDtypeStruct, pltpu.VMEM, pltpu.SemaphoreType.DMA
    shapes = [(shard, wide), (shard, half), (shard, wide)]
    owners = (2, count, 2, 2)
    return pl.pallas_call(
        functools.partial(unattend_kernel, count, pairs),
        grid=(8 + pairs,),
        out_shape=[
            sds((rows, width), f32), sds((2, rows, width), f32), sds((2, rows, width), low),
        ]
        + [sds(s, f32) for s in shapes + [early.shape]]
        + [sds(mixed.shape, low)]
        + [sds(owners + s, low) for s in shapes + shapes[:1]],
        in_specs=[
            at(0), at(1), at(2), at(0), at(1), once(1, keys), once(rows, 128), column,
            once(rows, width), once(rows, width), once(rows, width),
            pl.BlockSpec((1, rows, wide), lambda i: (jnp.minimum(i, 1), 0, 0)),
            pl.BlockSpec((rows, half), lambda i: (0, jnp.clip(i - 2, 0, 1))),
            pl.BlockSpec((1, rows, wide), lambda i: (gu(i) % 2, 0, gu(i) // 2)),
            any_spec, any_spec,
        ],
        out_specs=[column, both, both]
        + [once(*s) for s in shapes + [early.shape]]
        + [any_spec] * 5,
        scratch_shapes=[vm((keys, 128), low)] * 2
        + [vm((keys, 128), f32)] * 2
        + [vm((width, rows), low), vm((2, width, wide), low), dma((8,))]
        + deliver_scratch(mixed.shape[1:])
        + scatter_scratch(count, shapes)
        + [vm(early.shape, f32), dma(())]
        + sum_scratch(count, early.shape),
        compiler_params=pltpu.CompilerParams(
            vmem_limit_bytes=67000000, collective_id=4, has_side_effects=True
        ),
        name="unattend",
    )(qkv, qkv, qkv, far, far, mask, lse, grad, *lefts, inner, attended, d_gu, mixed, early)


def unproject_kernel(count, *refs):
    dq, dkv, got, w, spots, freqs, tok, gain, d_resid, h1, p_up = refs[:11]
    summed, r_up, r_qkv, p_qkv, home = refs[11:16]
    acc, cos, sin, flipped, late, stage, stored, leaving, *moving = refs[16:28]
    wide, half = r_up.shape[1], w.shape[3]
    shard = r_up.shape[0]
    sides = (slice(0, wide // 256 * 128), slice(wide // 256 * 128, wide))
    parts, outs = [p_up.at[:, :, :, :, :, k] for k in sides], [r_up.at[:, k] for k in sides]
    parts += [p_qkv.at[n] for n in range(3)]
    outs += [r_qkv.at[n] for n in range(3)]
    begin, steps, end = scatter_job(count, parts, outs, refs[28:-9])
    adds = sum_job(count, late, summed, refs[-9:])
    deliver, delivered = deliver_job(leaving, home, *moving)
    step = pl.program_id(0)
    t, side = step // 2, lax.rem(step, 2)
    cuts = [k * count // 4 for k in (0, 2, 5, 8, 10, 13, 16)]

    def store(n):
        for block in range(4 * count):
            pltpu.make_async_copy(
                stage.at[n % 2, block * shard : (block + 1) * shard],
                p_qkv.at[n // 2, n % 2, block // 4, (block // 2) % 2, block % 2],
                stored.at[n],
            ).start()

    def settle(n):
        arrived(p_qkv.at[n // 2, n % 2], stored.at[n])

    for n in range(6):

        @pl.when(step == n)
        def _(n=n):
            if n == 0:
                greet(count, corner=True)
                begin(0, 1)
                cosine, sine = tables(spots[...], freqs[...])
                cos[...] = cosine
                sin[...] = -sine
                flipped[...] = h1[...].T
                late[...] = jnp.zeros_like(late)
            if n in (2, 4):
                settle(n - 2)
                settle(n - 1)
                begin(n // 2 + 1)
            for one in steps[cuts[n] : cuts[n + 1]]:
                one()

    def turned(value):
        parts = [
            turn(value[:, n * 128 : (n + 1) * 128], cos[...], sin[...])
            for n in range(value.shape[1] // 128)
        ]
        return jnp.concatenate(parts, axis=1)

    def use(value, line):
        rounded = value.astype(low)
        if line:
            lanes = pl.ds(pl.multiple_of(side * half, 128), half)
            late[line : line + 1, lanes] = jnp.sum(rounded.astype(f32), axis=0, keepdims=True)
        stage[side] = mm(flipped[...], rounded, NN).astype(low)
        part = mm(rounded, w[0, 0], NT)

        @pl.when(step == 0)
        def _():
            acc[...] = part

        @pl.when(step > 0)
        def _():
            acc[...] += part

    @pl.when(t == 0)
    def _():
        use(turned(dq[...]), 8)

    @pl.when(t == 1)
    def _():
        use(turned(dkv[0] + got[0].astype(f32)), 0)

    @pl.when(t == 2)
    def _():
        use(dkv[0] + got[0].astype(f32), 9)

    for n in range(6):

        @pl.when(step == n)
        def _(n=n):
            store(n)

    @pl.when(step == 5)
    def _():
        width = tok.shape[1]
        normed, inverse = normalise(tok[...].astype(f32), width)
        up = acc[...]
        late[0:1] = jnp.sum(up * normed, axis=0, keepdims=True)
        late[1:2] = jnp.sum(up, axis=0, keepdims=True)
        scaled = up * gain[...]
        mean = jnp.sum(scaled, axis=-1, keepdims=True) / width
        cross = jnp.sum(scaled * normed, axis=-1, keepdims=True) / width
        result = d_resid[...] + inverse * (scaled - mean - normed * cross)
        for n in range(4):
            leaving[n] = result[n * PAD : (n + 1) * PAD].astype(low)
        settle(4)
        settle(5)
        begin(4)
        deliver()
        rest = steps[cuts[6] :]
        for n, one in enumerate(rest):
            one()
            for add in share(adds, n, len(rest)):
                add()
        end()
        delivered()


def unproject(count, dq, dkv, got, w, spots, freqs, tok, gain, d_resid, h1, p_up):
    rows, width = tok.shape
    half = w.shape[3]
    once = lambda *s: pl.BlockSpec(s, lambda i: (0,) * len(s), pipeline_mode=pl.Buffered(1))
    pick = lambda i: (jnp.maximum(i // 2 - 1, 0), 0, i % 2)
    any_spec = pl.BlockSpec(memory_space=pl.ANY)
    shape = p_up.shape[4:]
    cut = shape[1] // 256 * 128
    thin = (shape[0], half)
    sds, vm = jax.ShapeDtypeStruct, pltpu.VMEM
    return pl.pallas_call(
        functools.partial(unproject_kernel, count),
        grid=(6,),
        out_shape=[
            sds((16, width), f32), sds(shape, f32), sds((3,) + thin, f32),
            sds((3,) + p_up.shape[:4] + thin, low), sds((4, PAD, width), low),
        ],
        in_specs=[
            pl.BlockSpec((rows, half), lambda i: (0, i % 2)),
            pl.BlockSpec((1, rows, half), pick), pl.BlockSpec((1, rows, half), pick),
            pl.BlockSpec((1, 1, width, half), lambda i: (i // 2, i % 2, 0, 0)),
            once(rows, 128), once(1, 128), once(rows, width), once(1, width),
            once(rows, width), once(rows, width), any_spec,
        ],
        out_specs=[once(16, width), once(*shape), once(3, *thin), any_spec, any_spec],
        scratch_shapes=[
            vm((rows, width), f32), vm((rows, 128), f32), vm((rows, 128), f32),
            vm((width, rows), low), vm((16, width), f32), vm((2, width, half), low),
            pltpu.SemaphoreType.DMA((6,)), vm((4, PAD, width), low),
        ]
        + deliver_scratch((PAD, width))
        + scatter_scratch(count, [(shape[0], cut), (shape[0], shape[1] - cut)] + [thin] * 3)
        + sum_scratch(count, (16, width)),
        compiler_params=pltpu.CompilerParams(
            vmem_limit_bytes=67000000, collective_id=5, has_side_effects=True
        ),
        name="unproject",
    )(dq, dkv, got, w, spots, freqs, tok, gain, d_resid, h1, p_up)


SLAB = 32


def in_slabs(rows, body):
    def step(i, carry):
        body(pl.ds(pl.multiple_of(i * SLAB, SLAB), SLAB))
        return carry

    lax.fori_loop(0, rows // SLAB, step, 0)


def fold(values):
    return values[:8] + values[8:16] + values[16:24] + values[24:]


def across(values):
    return jnp.sum(values, axis=-1, keepdims=True)


def down_rows(acc):
    return jnp.sum(acc, axis=0, keepdims=True)


def ffn_kernel(
    count, hidden, part, att, tok, w_out, w_gu, gu_bias, in_gain, in_bias, gain2, shift2, b_out,
    b_down, cot, own, mixed, inner, d_gu, h2, d_resid, g_attn, d_att, wide_sums, thin_sums, grad_out,
    full, resid, gate, up, act, acc, d_in, stats, wide_acc, thin_acc, grad, w_down, ws, gs, gr, gl,
    *scratch,
):
    step = pl.program_id(0)
    rows, width = tok.shape
    wide = in_gain.shape[2]
    half = w_out.shape[2]
    shard = own.shape[0]
    edge = lax.broadcasted_iota(jnp.int32, (SLAB, wide), 1) < part
    cut = wide // 256 * 128
    sides = (slice(0, cut), slice(cut, wide))
    begin, steps, end = gather_job(
        count, [own.at[:, k] for k in sides], [full.at[:, :, :, :, :, k] for k in sides], scratch,
        lambda j: j % 4 == 3,
    )
    b, x, c, y = (lax.axis_index(a) for a in FAR)
    band = rows // 2
    mine = pl.ds(pl.multiple_of(x * band, 16), band)
    theirs = pl.ds(pl.multiple_of((1 - x) * band, 16), band)
    local = pltpu.make_async_copy(cot.at[2 * x + y], grad.at[mine], gl)

    for n in range(7):

        @pl.when(step == n)
        def _(n=n):
            if n == 0:
                greet(count)
                local.start()
                begin()
            for one in share(steps, n, 6) if n < 6 else ():
                one()
            if n == 3:
                push(cot.at[2 * (1 - x) + y], grad.at[mine], gs, gr, place(b, 1 - x, c, y))
            if n == 6:
                end()
                for side in range(2):
                    for k in range(4 * count):
                        block = full.at[side, k // 4, (k // 2) % 2, k % 2]
                        there = w_down.at[side, k * shard : (k + 1) * shard]
                        pltpu.make_async_copy(block, there, ws.at[side]).start()
                local.wait()
                arrived(grad.at[theirs], gr)
                arrived(cot.at[0], gs)

    def at(n):
        return pl.when(step == n)

    @at(0)
    def _():
        acc[...] = mm(att[:, :half], w_out[0], NT)
        wide_acc[...] = jnp.zeros_like(wide_acc)
        thin_acc[...] = jnp.zeros_like(thin_acc)

    @at(1)
    def _():
        acc[...] += mm(att[:, half:], w_out[0], NT)

        def body(s):
            value = tok[s].astype(f32) + acc[s] + b_out[...]
            resid[s] = value
            normed, _ = normalise(value, width)
            h2[s] = (normed * gain2[...] + shift2[...]).astype(low)

        in_slabs(rows, body)

    for n in range(2):

        @at(2 + 2 * n)
        def _(n=n):
            gate[n] = mm(h2[...], w_gu[0], NN) + gu_bias[0]

        @at(3 + 2 * n)
        def _(n=n):
            up[n] = mm(h2[...], w_gu[0], NN) + gu_bias[0]

            def body(s):
                value = gate[n, s]
                out = value * jax.nn.sigmoid(value) * up[n, s]
                act[n, s] = out
                total = across(out)
                stats[0, s] = total if n == 0 else stats[0, s] + total

            in_slabs(rows, body)

    @at(6)
    def _():
        def body(s):
            centre = stats[0, s] / hidden
            total = 0.0
            moved = []
            for n in range(2):
                shifted = jnp.where(edge, act[n, s] - centre, 0.0)
                moved.append(shifted)
                total = total + across(jnp.square(shifted))
            inverse = lax.rsqrt(total / hidden + epsilon)
            stats[1, s] = inverse
            for n in range(2):
                normed = moved[n] * inverse
                act[n, s] = normed
                inner[n, s] = (normed * in_gain[n] + in_bias[n]).astype(low)

        in_slabs(rows, body)

    for n in range(2):

        @at(6 + n)
        def _(n=n):
            arrived(w_down.at[n], ws.at[n])
            out = mm(inner[n], w_down[n], NT)
            if n == 0:
                acc[...] = out
            else:
                acc[...] += out
            d_in[n] = mm(grad[...], w_down[n], NN)

    @at(7)
    def _():
        def first(s):
            mixed[s] = (resid[s] + acc[s] + b_down[...]).astype(low)
            grad_out[s] = grad[s]
            thin_acc[0] += fold(grad[s].astype(f32))

        in_slabs(rows, first)

        def second(s):
            mean, cross = 0.0, 0.0
            kept = []
            for n in range(2):
                value, normed = d_in[n, s], act[n, s]
                wide_acc[n, 0] += fold(value * normed)
                wide_acc[n, 1] += fold(value)
                scaled = value * in_gain[n]
                mean = mean + across(scaled)
                cross = cross + across(scaled * normed)
            mean, cross = mean / hidden, cross / hidden
            for n in range(2):
                normed, value, other = act[n, s], gate[n, s], up[n, s]
                d_act = stats[1, s] * (d_in[n, s] * in_gain[n] - mean - normed * cross)
                sigma = jax.nn.sigmoid(value)
                d_gate = (d_act * other * sigma * (1.0 + value * (1.0 - sigma))).astype(low)
                d_up = (d_act * value * sigma).astype(low)
                wide_acc[n, 2] += fold(d_gate.astype(f32))
                wide_acc[n, 3] += fold(d_up.astype(f32))
                d_gu[n, s, :wide] = d_gate
                d_gu[n, s, wide:] = d_up

        in_slabs(rows, second)
        for n in range(2):
            for k in range(4):
                wide_sums[n, k : k + 1] = down_rows(wide_acc[n, k])

    for n in range(4):

        @at(8 + n)
        def _(n=n):
            out = mm(d_gu[n // 2, :, (n % 2) * wide : (n % 2 + 1) * wide], w_gu[0], NT)
            if n == 0:
                acc[...] = out
            else:
                acc[...] += out

    @at(11)
    def _():
        def body(s):
            value = acc[s]
            normed, inverse = normalise(resid[s], width)
            thin_acc[1] += fold(value * normed)
            thin_acc[2] += fold(value)
            scaled = value * gain2[...]
            mean, cross = across(scaled) / width, across(scaled * normed) / width
            out = grad[s].astype(f32) + inverse * (scaled - mean - normed * cross)
            d_resid[s] = out
            rounded = out.astype(low)
            g_attn[s] = rounded
            thin_acc[3] += fold(rounded.astype(f32))

        in_slabs(rows, body)
        for k in range(4):
            thin_sums[k : k + 1] = down_rows(thin_acc[k])

    for n in range(2):

        @at(12 + n)
        def _(n=n):
            d_att[:, n * half : (n + 1) * half] = mm(g_attn[...], w_out[0], NN).astype(low)


def ffn(
    count, hidden, part, att, tok, w_out, w_gu, gu_bias, in_gain, in_bias, gain2, shift2, b_out,
    b_down, cot, own,
):
    rows, width = tok.shape
    half, wide = w_out.shape[2], w_gu.shape[2] // 2
    whole = lambda *s: pl.BlockSpec(s, lambda i: (0,) * len(s), pipeline_mode=pl.Buffered(1))
    out_at = lambda i: (jnp.where(i < 1, 0, jnp.where(i < 12, 1, jnp.where(i < 13, 0, 1))), 0, 0)
    any_spec = pl.BlockSpec(memory_space=pl.ANY)

    def gu_at(i):
        n = jnp.where(i < 8, jnp.clip(i - 2, 0, 3), jnp.clip(i - 8, 0, 3))
        return n // 2, n % 2

    sds, vm, dma = jax.ShapeDtypeStruct, pltpu.VMEM, pltpu.SemaphoreType.DMA
    shapes = [
        sds((rows, width), low), sds((2, rows, wide), low), sds((2, rows, 2 * wide), low),
        sds((rows, width), low), sds((rows, width), f32), sds((rows, width), low),
        sds((rows, width), low), sds((2, 4, wide), f32), sds((4, width), f32),
        sds((rows, width), low),
    ]
    return pl.pallas_call(
        functools.partial(ffn_kernel, count, hidden, part),
        grid=(14,),
        out_shape=shapes + full_shapes(count, [own]),
        in_specs=[
            whole(rows, width), whole(rows, width),
            pl.BlockSpec((1, width, half), out_at),
            pl.BlockSpec((1, width, wide), lambda i: (gu_at(i)[0], 0, gu_at(i)[1])),
            pl.BlockSpec((1, 1, wide), lambda i: (gu_at(i)[0], 0, gu_at(i)[1])),
            whole(2, 1, wide), whole(2, 1, wide), whole(1, width), whole(1, width),
            whole(1, width), whole(1, width), any_spec, any_spec,
        ],
        out_specs=[whole(*s.shape) for s in shapes] + [any_spec],
        scratch_shapes=[
            vm((rows, width), f32), vm((2, rows, wide), f32), vm((2, rows, wide), f32),
            vm((2, rows, wide), f32), vm((rows, width), f32), vm((2, rows, wide), f32),
            vm((2, rows, 1), f32), vm((2, 4, 8, wide), f32), vm((4, 8, width), f32),
            vm((rows, width), low), vm((2, width, wide), low), dma((2,)), dma(()), dma(()), dma(()),
        ]
        + gather_scratch(
            count, [(own.shape[0], wide // 256 * 128), (own.shape[0], wide - wide // 256 * 128)]
        ),
        compiler_params=pltpu.CompilerParams(
            vmem_limit_bytes=67000000, collective_id=6, has_side_effects=True
        ),
        name="ffn",
    )(att, tok, w_out, w_gu, gu_bias, in_gain, in_bias, gain2, shift2, b_out, b_down, cot, own)


def on_device(
    count, tokens, positions, key_mask, norm1_gain, norm1_bias, qkv_weight, qv_bias, out_weight,
    out_bias, norm2_gain, norm2_bias, gate_up_weight, gate_up_bias, inner_gain, inner_bias,
    down_weight, down_bias, cotangent,
):
    b, x, c, y = (lax.axis_index(a) for a in FAR)
    image = 2 * x + y
    local, images, width = tokens.shape
    shard = qkv_weight.shape[0]
    half = qkv_weight.shape[2]
    part = gate_up_weight.shape[2]
    hidden = gate_up_bias.shape[1]
    wide = -(-part // 128) * 128
    more = wide - part
    rows = 4 * PAD

    shards = [
        jnp.swapaxes(qkv_weight.astype(low), 0, 1),
        out_weight.astype(low).T,
        jnp.pad(gate_up_weight.astype(low), ((0, 0), (0, 0), (0, more))).reshape(shard, 2 * wide),
        jnp.pad(down_weight.astype(low).T, ((0, 0), (0, more))),
    ]
    chunks = jnp.pad(jnp.swapaxes(tokens, 0, 1), ((0, 0), (0, PAD - local), (0, 0)))
    cot = jnp.transpose(cotangent.reshape(2, local, images, width), (2, 0, 1, 3))
    cot = jnp.pad(cot, ((0, 0), (0, 0), (0, PAD - local), (0, 0))).reshape(images, 2 * PAD, width)
    spots = jnp.transpose(positions.reshape(2, 2, local, images), (3, 1, 2, 0)).astype(low)
    spots = jnp.pad(spots, ((0, 0), (0, 0), (0, PAD - local), (0, 0)))
    pick = (jnp.arange(128) // 32) % 2
    spots = jnp.where(pick == 0, spots[..., 0:1], spots[..., 1:2])
    join = lambda f: f.reshape(2, width, f.shape[-1])
    w_qkv, tok, spot = gather_first(count, shards[0], chunks, spots)
    w_qkv = w_qkv.reshape(3, 2, width, half)
    tok, spot = tok.reshape(rows, width), spot.reshape(rows, 128)

    live = lax.dynamic_index_in_dim(key_mask, image, 1, keepdims=False)
    live = jnp.pad(live.reshape(2, 2, 2, local), ((0, 0), (0, 0), (0, 0), (0, PAD - local)))
    live = jnp.stack(
        [lax.dynamic_index_in_dim(live, n, 1, keepdims=False).reshape(rows) for n in (c, 1 - c)]
    )
    bias = jnp.where(live > 0, 0.0, masked_score).astype(f32).reshape(1, 2 * rows)

    freqs = jnp.tile(10000.0 ** (-jnp.arange(16).astype(f32) / 16), 8).reshape(1, 128)
    row = lambda a: a.reshape(1, -1)
    qkv_bias = jnp.stack([qv_bias[0], jnp.zeros_like(qv_bias[0]), qv_bias[1]])[:, None]
    swap = ((0, 1), (1, 0))
    qkv, h1, attended, lse, far, *full = forward(
        count, tok, row(norm1_gain), row(norm1_bias), w_qkv, qkv_bias, spot, freqs, bias, shards[1:3]
    )
    w_out, w_gu = (join(f) for f in full)

    split = lambda a: jnp.pad(a.reshape(a.shape[:-1] + (2, part)), ((0, 0),) * a.ndim + ((0, more),))
    gu_bias = jnp.swapaxes(split(gate_up_bias), 0, 1).reshape(2, 1, 2 * wide)
    mixed, inner, d_gu, h2, d_resid, g_attn, d_attended, wide_sums, thin_sums, grad, _ = ffn(
        count, hidden, part, attended, tok, w_out, w_gu, gu_bias, split(inner_gain)[:, None],
        split(inner_bias)[:, None], row(norm2_gain), row(norm2_bias), row(out_bias), row(down_bias),
        cot, shards[3],
    )
    merge = lambda a: a[..., :part].reshape(a.shape[:-2] + (hidden,))
    d_gu_bias = merge(jnp.swapaxes(wide_sums[:, 2:], 0, 1))
    d_down_bias, d_gain2, d_bias2, d_out_bias = (thin_sums[n] for n in range(4))
    vectors = [
        d_out_bias, d_gain2, d_bias2, d_down_bias, d_gu_bias, merge(wide_sums[:, 0]),
        merge(wide_sums[:, 1]),
    ]
    flat = jnp.concatenate([v.reshape(-1) for v in vectors])
    size = flat.shape[0]
    lines = -(-size // 2048) * 16
    flat = jnp.pad(flat, (0, lines * 128 - size)).reshape(lines, 128)
    dq, dkv, dfar, r_down, r_out, r_gate, summed, mixed_home, _, _, _, p_up = unattend(
        count, shard, qkv, far, bias, lse, d_attended, (grad, g_attn, h2), inner, attended, d_gu,
        mixed.reshape(4, PAD, width), flat,
    )
    got = lax.ppermute(dfar, "core", swap)
    late, r_up, r_qkv, _, d_tok_home = unproject(
        count, dq, dkv, got, w_qkv, spot, freqs, tok, row(norm1_gain), d_resid, h1, p_up
    )
    summed = summed.reshape(-1)
    pieces, at = [], 0
    for v in vectors:
        pieces.append(summed[at : at + v.size].reshape(v.shape))
        at += v.size

    home = lambda landed: jnp.swapaxes(landed[:, :local], 0, 1)

    return (
        home(mixed_home), home(d_tok_home), late[0], late[1], jnp.swapaxes(r_qkv, 0, 1), late[8:10],
        r_out.T, pieces[0], pieces[1], pieces[2],
        jnp.stack([r_gate[:, :part], r_up[:, :part]], axis=1), pieces[4], pieces[5], pieces[6],
        r_down[:, :part].T, pieces[3],
    )


def solution(mesh):
    count, ctx, tensor = (mesh.shape[a] for a in ("batch", "ctx", "tensor"))
    fine = jax.sharding.Mesh(mesh.devices.reshape(count, ctx // 2, 2, tensor), FAR)
    ctx, wide = ("x", "core"), ("batch", "x", "core")
    return jax.shard_map(
        functools.partial(on_device, count),
        mesh=fine,
        in_specs=(
            P(("x", "core", "tensor"), "batch", None), P(None, ctx, "batch"), P(None, "batch"),
            P(), P(), P(wide, None, "tensor"), P(), P("tensor", wide), P(), P(), P(),
            P(wide, None, "tensor"), P(), P(), P(), P("tensor", wide), P(), P(ctx, "batch", None),
        ),
        out_specs=(
            P(("x", "core", "tensor"), "batch", None), P(("x", "core", "tensor"), "batch", None),
            P(), P(), P(wide, None, "tensor"), P(), P("tensor", wide), P(), P(), P(),
            P(wide, None, "tensor"), P(), P(), P(), P("tensor", wide), P(),
        ),
        check_vma=False,
    )
```
